8 devices in a mesh: frag: 1 (over z), dev2: 2 (over y), dev: 4 (over x, core).
Axes of the slice: x: 2, y: 2, z: 1, core: 2. Of those that a mesh axis runs over, the one named last changes fastest.
Arguments:
- ao_ints: bfloat16 [116, 116, 116, 116], P(('frag', 'dev'), 'dev2')
- c_occ: bfloat16 [116, 15], P('frag')
- c_vir: bfloat16 [116, 96], P('frag')
Outputs:
- output: float32 [15, 96, 1440], P(None, None, ('frag', 'dev2', 'dev'))
All inputs are finite; a program needn't handle non-finite values.
Results may differ from the reference program's by a relative error of at most 0.001.
Values are sent between devices in bfloat16 or wider.
A program may use at most 1 GiB of HBM per device.

```python
import jax
import jax.numpy as jnp
from jax import lax

N_BASIS = 116
N_OCC = 15
N_VIRT = 96


def setup_inputs(seed: int = 0, part: int = 0) -> dict:
    base_key = jax.random.fold_in(jax.random.key(seed), part)
    key_ints, key_occ, key_vir = jax.random.split(base_key, 3)
    coef_scale = N_BASIS ** -0.5
    ao_ints = jax.random.normal(key_ints, (N_BASIS, N_BASIS, N_BASIS, N_BASIS), jnp.float32).astype(jnp.bfloat16)
    c_occ = (jax.random.normal(key_occ, (N_BASIS, N_OCC), jnp.float32) * coef_scale).astype(jnp.bfloat16)
    c_vir = (jax.random.normal(key_vir, (N_BASIS, N_VIRT), jnp.float32) * coef_scale).astype(jnp.bfloat16)
    return {'ao_ints': ao_ints, 'c_occ': c_occ, 'c_vir': c_vir}


def reference(ao_ints, c_occ, c_vir):
    occ_f32 = c_occ.astype(jnp.float32)
    vir_f32 = c_vir.astype(jnp.float32)
    n_pairs = c_occ.shape[1] * c_vir.shape[1]

    def first_half(ao_row):
        t_one = jnp.einsum('qrs,rj->qsj', ao_row.astype(jnp.float32), occ_f32).astype(jnp.bfloat16)
        half_ints = jnp.einsum('qsj,sb->qjb', t_one.astype(jnp.float32), vir_f32).astype(jnp.bfloat16)
        return half_ints.reshape(ao_row.shape[0], n_pairs)

    half_all = lax.map(first_half, ao_ints)
    g_mid = jnp.einsum('qa,pqc->apc', vir_f32, half_all.astype(jnp.float32))
    return jnp.einsum('pi,apc->iac', occ_f32, g_mid)
```

```python
import functools

import jax
import jax.numpy as jnp
from jax import lax
from jax.experimental import pallas as pl
from jax.experimental.pallas import tpu as pltpu
from jax.sharding import PartitionSpec as P

MESH = pl.DeviceIdType.MESH
F32, BF16, I32 = jnp.float32, jnp.bfloat16, jnp.int32

NP, NQ, NB = 29, 58, 116
NO, NV = 15, 96
QC = 8
NM = NQ // QC
QT = NQ - NM * QC
PG = 4
LW = 384
JR = [((360 * d) // 96, (360 * d + 359) // 96) for d in range(4)]
JO = [sum(hi - lo + 1 for lo, hi in JR[:d]) for d in range(5)]
KF = 144


def iota(shape, dim):
    return lax.broadcasted_iota(I32, shape, dim)


def dot(a, b):
    return jnp.dot(a, b, preferred_element_type=F32)


def kernel(a_hbm, cot_ref, cvt_ref, out_ref, abuf, atail, cot, cvt, s_mat, b_mat, l_mat, lt_mat, g_mat, x_buf,
           own_m, own_t, ps_m, ps_t, pr_m, pr_t, rb_m, rb_t, vsend,
           a_sem, at_sem, d_send, d_recv, r_send, r_recv, v_send, v_recv):
    y = lax.axis_index('dev2')
    dev = lax.axis_index('dev')
    core = lax.rem(dev, 2)
    x = dev // 2
    partner = (0, y, x * 2 + (1 - core))
    peers = [(0, y, (1 - x) * 2 + core), (0, 1 - y, x * 2 + core), (0, 1 - y, (1 - x) * 2 + core)]
    chip = [2 * y + (1 - x), 2 * (1 - y) + x, 2 * (1 - y) + (1 - x)]
    me = 2 * y + x

    def a_copy(n, slot):
        return pltpu.make_async_copy(a_hbm.at[:, pl.ds(n * QC, QC)], abuf.at[slot], a_sem.at[slot])

    tail_copy = pltpu.make_async_copy(a_hbm.at[:, pl.ds(NM * QC, QT)], atail, at_sem)
    tail_copy.start()
    a_copy(0, 0).start()
    a_copy(1, 1).start()

    barrier = pltpu.get_barrier_semaphore()
    for other in [partner] + peers:
        pl.semaphore_signal(barrier, inc=1, device_id=other, device_id_type=MESH)

    cot[...] = jnp.zeros_like(cot)
    cot[0:NO, 0:NB] = cot_ref[...].astype(F32)
    cvt[...] = jnp.zeros_like(cvt)
    cvt[0:NV, 0:NB] = cvt_ref[...].astype(F32)
    sub = iota((8, 128), 0)
    zero = jnp.zeros((8, 128), F32)
    for jj in range(8):
        for p in range(8):
            two = [jnp.where(sub == p, cot[j:j + 1, :], zero) for j in (2 * jj, 2 * jj + 1)]
            s_mat[16 * jj:16 * jj + 16, 128 * p:128 * p + 128] = jnp.concatenate(two, axis=0).astype(BF16)
    cv = cvt[...].T.astype(BF16)
    lane = iota((128, LW), 1)
    rel = jnp.where(lane < 180, lane, jnp.where(lane >= 256, lane - 76, lane + 116))
    bad = ((lane >= 180) & (lane < 192)) | ((lane >= 244) & (lane < 256))
    want = jnp.where(bad, -100000, rel) - iota((128, LW), 0)
    for d in range(4):
        for j in range(JR[d][0], JR[d][1] + 1):
            place = jnp.where(want == 96 * j - 360 * d, 1.0, 0.0).astype(BF16)
            k = JO[d] + j - JR[d][0]
            b_mat[128 * k:128 * k + 128, :] = dot(cv, place).astype(BF16)
    low, high = cot[0:8, :], cot[8:16, :]
    mine = jnp.concatenate([jnp.where(core == 0, low, high), jnp.where(core == 0, high, low)], axis=0)
    kk = iota((128, 256), 1)
    ploc = ((kk >> 4) & 3) * 8 + (kk & 7)
    pick = (iota((128, 256), 0) == ploc + NP * dev) & (ploc < NP)
    l0 = dot(mine.astype(BF16), jnp.where(pick, 1.0, 0.0).astype(BF16)).astype(BF16)
    row, k2 = iota((128, 256), 0), iota((128, 256), 1)
    e8 = jnp.where((iota((128, 16), 0) >> 3) == iota((128, 16), 1), 1.0, 0.0).astype(BF16)
    l_mat[...] = jnp.where((k2 >> 6) * 2 + ((k2 >> 3) & 1) == (row & 7), dot(e8, l0), 0.0).astype(BF16)
    e2 = jnp.where((iota((32, 16), 0) >> 1) == iota((32, 16), 1), 1.0, 0.0).astype(BF16)
    rowt, kt = iota((32, 256), 0), iota((32, 256), 1)
    lt_mat[...] = jnp.where(((kt >> 3) & 1) == (rowt & 1), dot(e2, l0), 0.0).astype(BF16)
    kf = iota((128, 3 * KF), 1)
    kf = jnp.where(kf >= 2 * KF, kf - 2 * KF, jnp.where(kf >= KF, kf - KF, kf))
    base, other_base = NQ * y, NQ * (1 - y)
    want_q = jnp.where(kf < 56, base + kf, jnp.where(kf < 112, other_base + kf - 56,
                       jnp.where(kf < 128, base + 56 + (kf & 1), other_base + 56 + (kf & 1))))
    sel = jnp.where(iota((128, 3 * KF), 0) == want_q, 1.0, 0.0).astype(BF16)
    g_mat[...] = dot(cvt[0:NV, :].astype(BF16), sel)

    pl.semaphore_wait(barrier, 4)

    def step1(a, q0, qps):
        zl = jnp.zeros((NB, 128 - NB), BF16)
        zs = jnp.zeros((128 - NB, 128), BF16)

        def tile(p, q):
            t = jnp.concatenate([a[p, q], zl], axis=1)
            return jnp.concatenate([t, zs], axis=0)

        for qp in qps:
            for pg in range(PG):
                ps = range(8 * pg, min(NP, 8 * pg + 8))
                rhs = jnp.concatenate(
                    [jnp.concatenate([tile(p, 2 * qp), tile(p, 2 * qp + 1)], axis=1) for p in ps], axis=0)
                t = dot(s_mat[0:8 * NO, 0:128 * len(ps)], rhs)
                r = 64 * qp + 16 * pg
                for j in range(NO):
                    two = jnp.concatenate([t[8 * j:8 * j + 8, 0:128], t[8 * j:8 * j + 8, 128:256]], axis=0)
                    x_buf[r:r + 16, 128 * j:128 * j + 128] = two.astype(BF16)

    def step2(rows, lhs, half, own, send):
        for d in range(4):
            lo, hi = JR[d]
            h = dot(x_buf[0:rows, 128 * lo:128 * hi + 128], b_mat[128 * JO[d]:128 * JO[d + 1], :]).astype(BF16)
            w = dot(lhs, h)
            own[d] = w[0:half]
            send[d] = w[half:2 * half]

    def d2d(n):
        return pltpu.make_async_remote_copy(
            src_ref=ps_m.at[n], dst_ref=pr_m.at[n], send_sem=d_send.at[n], recv_sem=d_recv.at[n],
            device_id=partner, device_id_type=MESH)

    d2d_t = pltpu.make_async_remote_copy(
        src_ref=ps_t, dst_ref=pr_t, send_sem=d_send.at[NM], recv_sem=d_recv.at[NM],
        device_id=partner, device_id_type=MESH)

    def out_m(n, k):
        return pltpu.make_async_remote_copy(
            src_ref=own_m.at[n, chip[k]], dst_ref=rb_m.at[k, n], send_sem=r_send.at[n, k], recv_sem=r_recv.at[n, k],
            device_id=peers[k], device_id_type=MESH)

    def out_t(k):
        return pltpu.make_async_remote_copy(
            src_ref=own_t.at[chip[k]], dst_ref=rb_t.at[k], send_sem=r_send.at[NM, k], recv_sem=r_recv.at[NM, k],
            device_id=peers[k], device_id_type=MESH)

    def finish_m(n):
        d2d(n).wait_recv()
        own_m[n] = own_m[n] + pr_m[n]
        for k in (2, 0, 1):
            out_m(n, k).start()

    def finish_t():
        d2d_t.wait_recv()
        own_t[...] = own_t[...] + pr_t[...]
        for k in (2, 0, 1):
            out_t(k).start()

    tail_copy.wait()
    step1(atail, 0, range(QT // 2))
    step2(64, lt_mat[:, 0:64], 16, own_t, ps_t)
    d2d_t.start()

    def body(n, carry):
        slot = lax.rem(n, 2)
        a_copy(n, slot).wait()
        a = abuf.at[slot]
        step1(a, 0, range(2))

        @pl.when(n == 0)
        def _():
            finish_t()

        @pl.when(n > 0)
        def _():
            finish_m(n - 1)

        step1(a, 0, range(2, 4))

        @pl.when(n + 2 < NM)
        def _():
            a_copy(n + 2, slot).start()

        step2(256, l_mat[...], 64, own_m.at[n], ps_m.at[n])
        d2d(n).start()
        return carry

    lax.fori_loop(0, NM, body, 0)
    finish_m(NM - 1)

    for k in range(3):
        out_t(k).wait_recv()

    def arrive(n, carry):
        for k in range(3):
            out_m(n, k).wait_recv()
        return carry

    lax.fori_loop(0, NM, arrive, 0)

    kg = iota((NV, 3 * KF), 1)
    kg = jnp.where(kg >= 2 * KF, kg - 2 * KF, jnp.where(kg >= KF, kg - KF, kg))
    which = jnp.where(kg < 112, -1, ((kg - 112) & 15) >> 1)

    def back(i):
        return pltpu.make_async_remote_copy(
            src_ref=vsend.at[i], dst_ref=out_ref.at[core * 8 + i], send_sem=v_send.at[i], recv_sem=v_recv.at[i],
            device_id=partner, device_id_type=MESH)

    def back_in(i):
        return pltpu.make_async_remote_copy(
            src_ref=vsend.at[i], dst_ref=out_ref.at[(1 - core) * 8 + i], send_sem=v_send.at[i], recv_sem=v_recv.at[i],
            device_id=partner, device_id_type=MESH)

    tails = [own_t[me] + rb_t[0], rb_t[1] + rb_t[2]]

    def last(i, carry):
        rows = pl.ds(pl.multiple_of(8 * i, 8), 8)
        near = [own_m[n, me, rows, :] + rb_m[0, n, rows, :] for n in range(NM)]
        far = [rb_m[1, n, rows, :] + rb_m[2, n, rows, :] for n in range(NM)]
        w = jnp.concatenate(near + far + tails, axis=0)
        hi = w.astype(BF16)
        r1 = w - hi.astype(F32)
        mid = r1.astype(BF16)
        lo = (r1 - mid.astype(F32)).astype(BF16)
        lhs = jnp.where((which < 0) | (which == i), g_mat[...], 0.0).astype(BF16)
        v = dot(lhs, jnp.concatenate([hi, mid, lo], axis=0))
        c0, c1, c2 = v[:, 0:128], v[:, 128:256], v[:, 256:384]
        c3 = pltpu.roll(c1, 64, 1)
        mine_v = jnp.concatenate([jnp.where(core == 0, c0, c2), jnp.where(core == 0, c1, c3)], axis=1)
        theirs = jnp.concatenate([jnp.where(core == 0, c2, c0), jnp.where(core == 0, c3, c1)], axis=1)
        out_ref[core * 8 + i] = mine_v[:, 0:180]
        vsend[i] = theirs[:, 0:180]
        back(i).start()
        return carry

    lax.fori_loop(0, 8, last, 0)

    def drain_v(i, carry):
        back_in(i).wait_recv()
        back(i).wait_send()
        return carry

    lax.fori_loop(0, 8, drain_v, 0)
    d2d_t.wait_send()
    for k in range(3):
        out_t(k).wait_send()

    def drain(n, carry):
        d2d(n).wait_send()
        for k in range(3):
            out_m(n, k).wait_send()
        return carry

    lax.fori_loop(0, NM, drain, 0)


def solution(mesh):
    def local_program(ints_blk, c_occ, c_vir):
        v = pl.pallas_call(
            kernel,
            out_shape=jax.ShapeDtypeStruct((16, NV, 180), F32),
            in_specs=[pl.BlockSpec(memory_space=pl.ANY),
                      pl.BlockSpec(memory_space=pltpu.VMEM), pl.BlockSpec(memory_space=pltpu.VMEM)],
            out_specs=pl.BlockSpec(memory_space=pltpu.VMEM),
            scratch_shapes=[
                pltpu.VMEM((2, NP, QC, NB, NB), BF16),
                pltpu.VMEM((NP, QT, NB, NB), BF16),
                pltpu.VMEM((16, 128), F32),
                pltpu.VMEM((128, 128), F32),
                pltpu.VMEM((128, 1024), BF16),
                pltpu.VMEM((128 * JO[4], LW), BF16),
                pltpu.VMEM((128, 256), BF16),
                pltpu.VMEM((32, 256), BF16),
                pltpu.VMEM((NV, 3 * KF), F32),
                pltpu.VMEM((256, 128 * NO), BF16),
                pltpu.VMEM((NM, 4, 64, LW), F32),
                pltpu.VMEM((4, 16, LW), F32),
                pltpu.VMEM((NM, 4, 64, LW), F32),
                pltpu.VMEM((4, 16, LW), F32),
                pltpu.VMEM((NM, 4, 64, LW), F32),
                pltpu.VMEM((4, 16, LW), F32),
                pltpu.VMEM((3, NM, 64, LW), F32),
                pltpu.VMEM((3, 16, LW), F32),
                pltpu.VMEM((8, NV, 180), F32),
                pltpu.SemaphoreType.DMA((2,)),
                pltpu.SemaphoreType.DMA,
                pltpu.SemaphoreType.DMA((NM + 1,)),
                pltpu.SemaphoreType.DMA((NM + 1,)),
                pltpu.SemaphoreType.DMA((NM + 1, 3)),
                pltpu.SemaphoreType.DMA((NM + 1, 3)),
                pltpu.SemaphoreType.DMA((8,)),
                pltpu.SemaphoreType.DMA((8,)),
            ],
            compiler_params=pltpu.CompilerParams(
                collective_id=0, has_side_effects=True, vmem_limit_bytes=60 * 1024 * 1024),
            name='four_index',
        )(ints_blk, c_occ.T, c_vir.T)
        return v[0:NO]

    return jax.shard_map(
        local_program,
        mesh=mesh,
        in_specs=(P(('frag', 'dev'), 'dev2', None, None), P('frag', None), P('frag', None)),
        out_specs=P(None, None, ('frag', 'dev2', 'dev')),
        check_vma=False,
    )
```

```python
import jax
import jax.numpy as jnp
from jax import lax
from jax.experimental import pallas as pl
from jax.experimental.pallas import tpu as pltpu
from jax.sharding import PartitionSpec as P

MESH = pl.DeviceIdType.MESH
F32, BF16, I32 = jnp.float32, jnp.bfloat16, jnp.int32

NP, NQ, NB = 29, 58, 116
NO, NV = 15, 96
QC = 8
NM = NQ // QC
QT = NQ - NM * QC
PG = 4
LW = 384
NJ = 5
RW = 184
ROWS = (RW, RW - 24)
N1 = 4
K1, K2 = 16 * N1 + 32, 16 * (NM - N1)


def iota(shape, dim):
    return lax.broadcasted_iota(I32, shape, dim)


def dot(a, b):
    return jnp.dot(a, b, preferred_element_type=F32)


def parts(w):
    hi = w.astype(BF16)
    rest = w - hi.astype(F32)
    mid = rest.astype(BF16)
    lo = (rest - mid.astype(F32)).astype(BF16)
    return jnp.concatenate([hi, mid, lo], axis=0)


def kernel(a_hbm, cot_hbm, cvt_hbm, out_hbm, abuf, atail, cot_in, cvt_in, cot, cvt, s_mat, b_mat, l_mat, lt_mat,
           g1_mat, g2_mat, x_buf, own_m, own_t, ps_m, ps_t, pr_m, pr_t, rb_m, rb_t, v_acc, v_own, v_other,
           a_sem, at_sem, c_sem, d_send, d_recv, r_send, r_recv, v_send, v_recv, o_sem):
    y = lax.axis_index('dev2')
    dev = lax.axis_index('dev')
    core = lax.rem(dev, 2)
    x = dev // 2
    partner = (0, y, x * 2 + (1 - core))
    peers = [(0, 1 - y, (1 - x) * 2 + core), (0, y, (1 - x) * 2 + core), (0, 1 - y, x * 2 + core)]
    chip = [2 * (1 - y) + (1 - x), 2 * y + (1 - x), 2 * (1 - y) + x, 2 * y + x]

    def a_copy(n, qp, slot):
        return pltpu.make_async_copy(
            a_hbm.at[:, pl.ds(n * QC + 2 * qp, 2)], abuf.at[slot, qp], a_sem.at[slot, qp])

    small = [pltpu.make_async_copy(cot_hbm, cot_in, c_sem.at[0]), pltpu.make_async_copy(cvt_hbm, cvt_in, c_sem.at[1])]
    tail_copy = pltpu.make_async_copy(a_hbm.at[:, pl.ds(NM * QC, QT)], atail, at_sem)
    for c in small:
        c.start()
    tail_copy.start()

    barrier = pltpu.get_barrier_semaphore()
    for other in [partner] + peers:
        pl.semaphore_signal(barrier, inc=1, device_id=other, device_id_type=MESH)

    cot[...] = jnp.zeros_like(cot)
    cvt[...] = jnp.zeros_like(cvt)
    for c in small:
        c.wait()
    cot[0:NO, 0:NB] = cot_in[...].astype(F32)
    cvt[0:NV, 0:NB] = cvt_in[...].astype(F32)
    for qp in range(4):
        a_copy(0, qp, 0).start()
    sub = iota((8, 128), 0)
    zero = jnp.zeros((8, 128), F32)
    for jj in range(8):
        for p in range(8):
            two = [jnp.where(sub == p, cot[j:j + 1, :], zero) for j in (2 * jj, 2 * jj + 1)]
            s_mat[16 * jj:16 * jj + 16, 128 * p:128 * p + 128] = jnp.concatenate(two, axis=0).astype(BF16)
    cv = cvt[...].T.astype(BF16)
    lane = iota((128, LW), 1)
    rel = jnp.where(lane < 128, lane, jnp.where(lane < 256, lane + 52, jnp.where(lane < 308, lane - 128, lane)))
    want = jnp.where(lane >= 360, -100000, rel) - iota((128, LW), 0)
    for d in range(4):
        for j in range(NJ):
            place = jnp.where(want == 96 * ((7 * d) // 2 + j) - 360 * d, 1.0, 0.0).astype(BF16)
            b_mat[d, 128 * j:128 * j + 128, :] = dot(cv, place).astype(BF16)
    low, high = cot[0:8, :], cot[8:16, :]
    mine = jnp.concatenate([jnp.where(core == 0, low, high), jnp.where(core == 0, high, low)], axis=0)
    kk = iota((128, 256), 1)
    ploc = ((kk >> 4) & 3) * 8 + (kk & 7)
    pick = (iota((128, 256), 0) == ploc + NP * dev) & (ploc < NP)
    l0 = dot(mine.astype(BF16), jnp.where(pick, 1.0, 0.0).astype(BF16)).astype(BF16)
    row, k2 = iota((128, 256), 0), iota((128, 256), 1)
    e8 = jnp.where((iota((128, 16), 0) >> 3) == iota((128, 16), 1), 1.0, 0.0).astype(BF16)
    l_mat[...] = jnp.where((k2 >> 6) * 2 + ((k2 >> 3) & 1) == (row & 7), dot(e8, l0), 0.0).astype(BF16)
    e2 = jnp.where((iota((32, 16), 0) >> 1) == iota((32, 16), 1), 1.0, 0.0).astype(BF16)
    rowt, kt = iota((32, 256), 0), iota((32, 256), 1)
    lt_mat[...] = jnp.where(((kt >> 3) & 1) == (rowt & 1), dot(e2, l0), 0.0).astype(BF16)

    base, other_base = NQ * y, NQ * (1 - y)

    def fold(k, period):
        return jnp.where(k >= 2 * period, k - 2 * period, jnp.where(k >= period, k - period, k))

    def g_of(k, want_q):
        sel = jnp.where(iota((128, k), 0) == want_q, 1.0, 0.0).astype(BF16)
        return dot(cvt[0:NV, :].astype(BF16), sel)

    k1 = fold(iota((128, 3 * K1), 1), K1)
    h1 = 8 * N1
    want1 = jnp.where(k1 < h1, base + k1, jnp.where(k1 < 2 * h1, other_base + k1 - h1,
                      jnp.where(k1 < 2 * h1 + 16, base, other_base) + NM * QC + (k1 & 1)))
    g1_mat[...] = g_of(3 * K1, want1)
    k2f = fold(iota((128, 3 * K2), 1), K2)
    h2 = 8 * (NM - N1)
    g2_mat[...] = g_of(3 * K2, jnp.where(k2f < h2, base + h1 + k2f, other_base + h1 + k2f - h2)).astype(BF16)

    def step1(tile_of, qp):
        zl = jnp.zeros((NB, 128 - NB), BF16)
        zs = jnp.zeros((128 - NB, 128), BF16)

        def tile(p, q):
            t = jnp.concatenate([tile_of(p, q), zl], axis=1)
            return jnp.concatenate([t, zs], axis=0)

        for pg in range(PG):
            ps = range(8 * pg, min(NP, 8 * pg + 8))
            rhs = jnp.concatenate([jnp.concatenate([tile(p, 0), tile(p, 1)], axis=1) for p in ps], axis=0)
            t = dot(s_mat[0:8 * NO, 0:128 * len(ps)], rhs)
            r = 64 * qp + 16 * pg
            for j in range(NO):
                two = jnp.concatenate([t[8 * j:8 * j + 8, 0:128], t[8 * j:8 * j + 8, 128:256]], axis=0)
                x_buf[j, r:r + 16, :] = two.astype(BF16)

    def step2(rows, lhs, r):
        first = (7 * chip[r]) // 2
        t = jnp.concatenate([x_buf[first + j, 0:rows, :] for j in range(NJ)], axis=1)
        return dot(lhs, dot(t, b_mat[chip[r]]).astype(BF16))

    spare = iota((8, 128), 1) >= 104

    def pack(ref, w):
        col = [[w[8 * i:8 * i + 8, 128 * c:128 * c + 128] for c in range(3)] for i in range(8)]
        ref[0:8, :] = col[0][0]
        ref[8:16, :] = col[0][1]
        for i in range(1, 8):
            third = col[i][2]
            if i <= 5:
                third = jnp.where(spare, pltpu.roll(col[0][2], 104 - 24 * (i - 1), 1), third)
            b = 24 * i - 8
            ref[b:b + 8, :] = col[i][0]
            ref[b + 8:b + 16, :] = col[i][1]
            ref[b + 16:b + 24, :] = third

    def d2d(n, r):
        return pltpu.make_async_remote_copy(
            src_ref=ps_m.at[n, r], dst_ref=pr_m.at[n, r], send_sem=d_send.at[n, r], recv_sem=d_recv.at[n, r],
            device_id=partner, device_id_type=MESH)

    def d2d_t(r):
        return pltpu.make_async_remote_copy(
            src_ref=ps_t.at[r], dst_ref=pr_t.at[r], send_sem=d_send.at[NM, r], recv_sem=d_recv.at[NM, r],
            device_id=partner, device_id_type=MESH)

    def out_m(n, r, rows):
        return pltpu.make_async_remote_copy(
            src_ref=own_m.at[n, r, pl.ds(0, rows)], dst_ref=rb_m.at[r, n, pl.ds(0, rows)],
            send_sem=r_send.at[n, r], recv_sem=r_recv.at[n, r], device_id=peers[r], device_id_type=MESH)

    def out_t(r):
        return pltpu.make_async_remote_copy(
            src_ref=own_t.at[r], dst_ref=rb_t.at[r], send_sem=r_send.at[NM, r], recv_sem=r_recv.at[NM, r],
            device_id=peers[r], device_id_type=MESH)

    def by_core(f):
        for k in range(2):
            @pl.when(core == k)
            def _(k=k):
                f(ROWS[k])

    def finish_m(n, rs):
        for r in rs:
            d2d(n, r).wait_recv()
            own_m[n, r] = own_m[n, r] + pr_m[n, r]

        def go(rows):
            for r in rs:
                if r < 3:
                    out_m(n, r, rows).start()

        by_core(go)

    def finish_t():
        for r in range(4):
            d2d_t(r).wait_recv()
            own_t[r] = own_t[r] + pr_t[r]
            if r < 3:
                out_t(r).start()

    tail_copy.wait()
    step1(lambda p, q: atail[p, q], 0)
    pl.semaphore_wait(barrier, 4)
    for r in range(4):
        w = step2(64, lt_mat[:, 0:64], r)
        for c in range(3):
            own_t[r, 16 * c:16 * c + 16, :] = w[0:16, 128 * c:128 * c + 128]
            ps_t[r, 16 * c:16 * c + 16, :] = w[16:32, 128 * c:128 * c + 128]
        d2d_t(r).start()
    for qp in range(4):
        a_copy(1, qp, 1).start()

    def body(n, carry):
        slot = lax.rem(n, 2)
        for qp in range(4):
            a_copy(n, qp, slot).wait()
            step1(lambda p, q: abuf[slot, qp, p, q], qp)

            @pl.when(n + 2 < NM)
            def _():
                a_copy(n + 2, qp, slot).start()

            if qp == 1:
                @pl.when(n == 0)
                def _():
                    finish_t()

                @pl.when(n > 0)
                def _():
                    finish_m(n - 1, (2, 3))

        for r in range(4):
            w = step2(256, l_mat[...], r)
            pack(own_m.at[n, r], w[0:64])
            pack(ps_m.at[n, r], w[64:128])
            d2d(n, r).start()
        finish_m(n, (0, 1))
        return carry

    lax.fori_loop(0, NM, body, 0)
    finish_m(NM - 1, (2, 3))

    def arrive(n, carry):
        def wait(rows):
            for r in range(3):
                out_m(n, r, rows).wait_recv()

        by_core(wait)
        return carry

    lane8 = iota((8, 128), 1)

    def w_rows(i, ns):
        def block(n, b):
            near = own_m[n, 3, b:b + 8, :] + rb_m[1, n, b:b + 8, :]
            far = rb_m[2, n, b:b + 8, :] + rb_m[0, n, b:b + 8, :]
            return near, far

        near, far = [], []
        for n in ns:
            b = 24 * i - 8 if i else 0
            cols = [block(n, b), block(n, b + 8)]
            if i:
                s = block(n, b + 16)
            else:
                s = [jnp.zeros((8, 128), F32)] * 2
                for m in range(5):
                    piece = block(n, 24 * (m + 1) + 8)
                    here = (lane8 >= 24 * m) & (lane8 < min(104, 24 * m + 24))
                    s = [jnp.where(here, pltpu.roll(v, 24 * m + 24, 1), o) for v, o in zip(piece, s)]
            cols.append(s)
            near.append(jnp.concatenate([c[0] for c in cols], axis=1))
            far.append(jnp.concatenate([c[1] for c in cols], axis=1))
        return near + far

    for r in range(3):
        out_t(r).wait_recv()
    lax.fori_loop(0, N1, arrive, 0)
    tails = [jnp.concatenate([own_t[3, 16 * c:16 * c + 16, :] + rb_t[1, 16 * c:16 * c + 16, :] for c in range(3)], axis=1),
             jnp.concatenate([rb_t[2, 16 * c:16 * c + 16, :] + rb_t[0, 16 * c:16 * c + 16, :] for c in range(3)], axis=1)]
    kg = fold(iota((NV, 3 * K1), 1), K1)
    which = jnp.where(kg < 2 * h1, -1, ((kg - 2 * h1) & 15) >> 1)
    for i in range(8):
        w = jnp.concatenate(w_rows(i, range(N1)) + tails, axis=0)
        lhs = jnp.where((which < 0) | (which == i), g1_mat[...], 0.0).astype(BF16)
        v_acc[i] = dot(lhs, parts(w))

    lax.fori_loop(N1, NM, arrive, 0)

    def home(i):
        return pltpu.make_async_copy(v_own.at[i], out_hbm.at[core * 8 + i], o_sem.at[i])

    def back(i):
        return pltpu.make_async_remote_copy(
            src_ref=v_other.at[i], dst_ref=out_hbm.at[core * 8 + i], send_sem=v_send.at[i], recv_sem=v_recv.at[i],
            device_id=partner, device_id_type=MESH)

    def back_in(i):
        return pltpu.make_async_remote_copy(
            src_ref=v_other.at[i], dst_ref=out_hbm.at[(1 - core) * 8 + i], send_sem=v_send.at[i], recv_sem=v_recv.at[i],
            device_id=partner, device_id_type=MESH)

    for i in range(8):
        w = jnp.concatenate(w_rows(i, range(N1, NM)), axis=0)
        v = v_acc[i] + dot(g2_mat[...], parts(w))
        c0, c1, c2 = v[:, 0:128], v[:, 128:256], v[:, 256:384]
        c3 = pltpu.roll(c2, 76, 1)
        mine_v = jnp.concatenate([jnp.where(core == 0, c0, c1), jnp.where(core == 0, c2, c3)], axis=1)
        theirs = jnp.concatenate([jnp.where(core == 0, c1, c0), jnp.where(core == 0, c3, c2)], axis=1)
        v_own[i] = mine_v[:, 0:180]
        v_other[i] = theirs[:, 0:180]
        if i < 7:
            back(i).start()
            home(i).start()
        else:
            @pl.when(core == 0)
            def _():
                back(7).start()
                home(7).start()

    for i in range(7):
        home(i).wait()
        back(i).wait_send()
        back_in(i).wait_recv()

    @pl.when(core == 0)
    def _():
        home(7).wait()
        back(7).wait_send()

    @pl.when(core == 1)
    def _():
        back_in(7).wait_recv()

    for r in range(4):
        d2d_t(r).wait_send()
    for r in range(3):
        out_t(r).wait_send()

    def drain(n, carry):
        for r in range(4):
            d2d(n, r).wait_send()

        def wait(rows):
            for r in range(3):
                out_m(n, r, rows).wait_send()

        by_core(wait)
        return carry

    lax.fori_loop(0, NM, drain, 0)


def solution(mesh):
    def local_program(ints_blk, c_occ, c_vir):
        return pl.pallas_call(
            kernel,
            out_shape=jax.ShapeDtypeStruct((NO, NV, 180), F32),
            in_specs=[pl.BlockSpec(memory_space=pl.ANY)] * 3,
            out_specs=pl.BlockSpec(memory_space=pl.ANY),
            scratch_shapes=[
                pltpu.VMEM((2, 4, NP, 2, NB, NB), BF16),
                pltpu.VMEM((NP, QT, NB, NB), BF16),
                pltpu.VMEM((NO, NB), BF16),
                pltpu.VMEM((NV, NB), BF16),
                pltpu.VMEM((16, 128), F32),
                pltpu.VMEM((128, 128), F32),
                pltpu.VMEM((128, 1024), BF16),
                pltpu.VMEM((4, 128 * NJ, LW), BF16),
                pltpu.VMEM((128, 256), BF16),
                pltpu.VMEM((32, 256), BF16),
                pltpu.VMEM((NV, 3 * K1), F32),
                pltpu.VMEM((NV, 3 * K2), BF16),
                pltpu.VMEM((NO, 256, 128), BF16),
                pltpu.VMEM((NM, 4, RW, 128), F32),
                pltpu.VMEM((4, 48, 128), F32),
                pltpu.VMEM((NM, 4, RW, 128), F32),
                pltpu.VMEM((4, 48, 128), F32),
                pltpu.VMEM((NM, 4, RW, 128), F32),
                pltpu.VMEM((4, 48, 128), F32),
                pltpu.VMEM((3, NM, RW, 128), F32),
                pltpu.VMEM((3, 48, 128), F32),
                pltpu.VMEM((8, NV, LW), F32),
                pltpu.VMEM((8, NV, 180), F32),
                pltpu.VMEM((8, NV, 180), F32),
                pltpu.SemaphoreType.DMA((2, 4)),
                pltpu.SemaphoreType.DMA,
                pltpu.SemaphoreType.DMA((2,)),
                pltpu.SemaphoreType.DMA((NM + 1, 4)),
                pltpu.SemaphoreType.DMA((NM + 1, 4)),
                pltpu.SemaphoreType.DMA((NM + 1, 3)),
                pltpu.SemaphoreType.DMA((NM + 1, 3)),
                pltpu.SemaphoreType.DMA((8,)),
                pltpu.SemaphoreType.DMA((8,)),
                pltpu.SemaphoreType.DMA((8,)),
            ],
            compiler_params=pltpu.CompilerParams(
                collective_id=0, has_side_effects=True, vmem_limit_bytes=60 * 1024 * 1024),
            name='four_index',
        )(ints_blk, c_occ.T, c_vir.T)

    return jax.shard_map(
        local_program,
        mesh=mesh,
        in_specs=(P(('frag', 'dev'), 'dev2', None, None), P('frag', None), P('frag', None)),
        out_specs=P(None, None, ('frag', 'dev2', 'dev')),
        check_vma=False,
    )
```

```python
import jax
import jax.numpy as jnp
from jax import lax
from jax.experimental import pallas as pl
from jax.experimental.pallas import tpu as pltpu
from jax.sharding import PartitionSpec as P

MESH = pl.DeviceIdType.MESH
F32, BF16, I32 = jnp.float32, jnp.bfloat16, jnp.int32

NP, NQ, NB = 29, 58, 116
NO, NV = 15, 96
QC = 8
NM = NQ // QC
QT = NQ - NM * QC
PG = 4
L = 128
LW = 3 * L
SP = 108
PW, NS = L - SP, 6
NC, CH = 180, 184
RW = 184
ROWS = (RW, RW - 24)
N1 = NM - 1


def place_of(i, c):
    return 3 * i - 1 + c if i else c


def cols(k, n=1):
    return slice(L * k, L * (k + n))


def rows8(k, n=1):
    return slice(8 * k, 8 * (k + n))


def iota(shape, dim):
    return lax.broadcasted_iota(I32, shape, dim)


def dot(a, b):
    return jnp.dot(a, b, preferred_element_type=F32)


def parts(w):
    hi = w.astype(BF16)
    rest = w - hi.astype(F32)
    mid = rest.astype(BF16)
    lo = (rest - mid.astype(F32)).astype(BF16)
    return jnp.concatenate([hi, mid, lo], axis=1)


def kernel(a_hbm, cot_hbm, cvt_hbm, out_hbm, abuf, atail, cot_in, cvt_in, cot, cvt, s_mat, b_mat, bs_mat, l_mat, lt_mat,
           f1_mat, f2_mat, x_buf, own_m, own_t, ps_m, ps_t, pr_m, pr_t, rb_m, rb_t, v_acc, v_fin,
           a_sem, at_sem, c_sem, d_send, d_recv, r_send, r_recv, v_send, v_recv, o_sem):
    y = lax.axis_index('dev2')
    dev = lax.axis_index('dev')
    core = lax.rem(dev, 2)
    x = dev // 2
    partner = (0, y, x * 2 + (1 - core))
    peers = [(0, 1 - y, (1 - x) * 2 + core), (0, y, (1 - x) * 2 + core), (0, 1 - y, x * 2 + core)]
    chip = [2 * (1 - y) + (1 - x), 2 * y + (1 - x), 2 * (1 - y) + x, 2 * y + x]

    def a_copy(n, qp, slot):
        return pltpu.make_async_copy(
            a_hbm.at[:, pl.ds(n * QC + 2 * qp, 2)], abuf.at[slot, qp], a_sem.at[slot, qp])

    small = [pltpu.make_async_copy(cot_hbm, cot_in, c_sem.at[0]), pltpu.make_async_copy(cvt_hbm, cvt_in, c_sem.at[1])]
    tail_copy = pltpu.make_async_copy(a_hbm.at[:, pl.ds(NM * QC, QT)], atail, at_sem)
    for c in small:
        c.start()
    tail_copy.start()

    barrier = pltpu.get_barrier_semaphore()
    for other in [partner] + peers:
        pl.semaphore_signal(barrier, inc=1, device_id=other, device_id_type=MESH)

    cot[...] = jnp.zeros_like(cot)
    cvt[...] = jnp.zeros_like(cvt)
    for c in small:
        c.wait()
    cot[0:NO, 0:NB] = cot_in[...].astype(F32)
    cvt[0:NV, 0:NB] = cvt_in[...].astype(F32)
    for qp in range(4):
        a_copy(0, qp, 0).start()
    sub = iota((8, L), 0)
    zero = jnp.zeros((8, L), F32)
    for jj in range(8):
        for p in range(8):
            two = [jnp.where(sub == p, cot[j:j + 1, :], zero) for j in (2 * jj, 2 * jj + 1)]
            s_mat[rows8(2 * jj, 2), cols(p)] = jnp.concatenate(two, axis=0).astype(BF16)
    cv = cvt[...].T.astype(BF16)
    first = [(15 * c) // 4 for c in chip]
    first_s = [4 * c + 2 - c // 3 for c in chip]
    lane, row = iota((L, 256), 1), iota((L, 256), 0)
    want = jnp.where(lane < NC, lane, jnp.where(lane < CH, -100000, lane - 4)) - row
    lane_s, row_s = iota((L, L), 1), iota((L, L), 0)
    want_s = jnp.where(lane_s < SP, lane_s + 252, -100000) - row_s
    bs_mat[...] = jnp.zeros_like(bs_mat)
    for r in range(4):
        for j in range(4):
            place = jnp.where(want == 96 * (first[r] + j) - 360 * chip[r], 1.0, 0.0).astype(BF16)
            b_mat[r, cols(j), :] = dot(cv, place).astype(BF16)
        for j in range(2):
            place = jnp.where(want_s == 96 * (first_s[r] + j) - 360 * chip[r], 1.0, 0.0).astype(BF16)
            h = r % 2
            bs_mat[r // 2, cols(2 * h + j), cols(h)] = dot(cv, place).astype(BF16)
    low, high = cot[0:8, :], cot[8:16, :]
    mine = jnp.concatenate([jnp.where(core == 0, low, high), jnp.where(core == 0, high, low)], axis=0)
    kk = iota((L, 256), 1)
    ploc = ((kk >> 4) & 3) * 8 + (kk & 7)
    pick = (iota((L, 256), 0) == ploc + NP * dev) & (ploc < NP)
    l0 = dot(mine.astype(BF16), jnp.where(pick, 1.0, 0.0).astype(BF16)).astype(BF16)
    row, k2 = iota((L, 256), 0), iota((L, 256), 1)
    e8 = jnp.where((iota((L, 16), 0) >> 3) == iota((L, 16), 1), 1.0, 0.0).astype(BF16)
    l_mat[...] = jnp.where((k2 >> 6) * 2 + ((k2 >> 3) & 1) == (row & 7), dot(e8, l0), 0.0).astype(BF16)
    e2 = jnp.where((iota((32, 16), 0) >> 1) == iota((32, 16), 1), 1.0, 0.0).astype(BF16)
    rowt, kt = iota((32, 256), 0), iota((32, 256), 1)
    lt_mat[...] = jnp.where(((kt >> 3) & 1) == (rowt & 1), dot(e2, l0), 0.0).astype(BF16)

    base, other_base = NQ * y, NQ * (1 - y)

    def f_of(want_q):
        sel = jnp.where(iota((L, L), 1) == want_q, 1.0, 0.0).astype(BF16)
        return dot(sel, cv)

    kf = iota((L, L), 0)
    h1 = QC * N1
    f1_mat[...] = f_of(jnp.where(kf < h1, base + kf, jnp.where(kf < 2 * h1, other_base + kf - h1,
                       jnp.where(kf < 2 * h1 + 16, base, other_base) + NM * QC + (kf & 1))))
    f2 = f_of(jnp.where((kf & 8) == 0, base, other_base) + h1 + (kf & 7))
    for i in range(8):
        mine_f = jnp.where((kf >> 4) == i, f2, 0.0).astype(BF16)
        for k in range(3):
            f2_mat[cols(k), cols(i)] = mine_f

    def step1(tile_of, qp):
        zl = jnp.zeros((NB, L - NB), BF16)
        zs = jnp.zeros((L - NB, L), BF16)

        def tile(p, q):
            t = jnp.concatenate([tile_of(p, q), zl], axis=1)
            return jnp.concatenate([t, zs], axis=0)

        for pg in range(PG):
            ps = range(8 * pg, min(NP, 8 * pg + 8))
            rhs = jnp.concatenate([jnp.concatenate([tile(p, 0), tile(p, 1)], axis=1) for p in ps], axis=0)
            t = dot(s_mat[rows8(0, NO), cols(0, len(ps))], rhs)
            r = rows8(8 * qp + 2 * pg, 2)
            for j in range(NO):
                two = jnp.concatenate([t[rows8(j), cols(k)] for k in range(2)], axis=0)
                x_buf[j, r, :] = two.astype(BF16)

    def step2(rows, lhs, pair):
        def w_of(js, weights):
            t = jnp.concatenate([x_buf[j, 0:rows, :] for j in js], axis=1)
            return dot(lhs, dot(t, weights).astype(BF16))

        w = [w_of([first[r] + j for j in range(4)], b_mat[r]) for r in pair]
        third = w_of([first_s[r] + j for r in pair for j in range(2)], bs_mat[pair[0] // 2])
        return [jnp.concatenate([w[k], third[:, cols(k)]], axis=1) for k in range(2)]

    lane8 = iota((8, L), 1)
    spare = lane8 >= SP

    def pack(ref, w):
        col = [[w[rows8(i), cols(c)] for c in range(3)] for i in range(8)]
        for i in range(8):
            for c in range(3 if i else 2):
                v = col[i][c]
                if c == 2 and i <= NS:
                    v = jnp.where(spare, pltpu.roll(col[0][c], SP - PW * (i - 1), 1), v)
                ref[rows8(place_of(i, c)), :] = v

    def d2d(n, r):
        return pltpu.make_async_remote_copy(
            src_ref=ps_m.at[n, r], dst_ref=pr_m.at[n, r], send_sem=d_send.at[n, r], recv_sem=d_recv.at[n, r],
            device_id=partner, device_id_type=MESH)

    def d2d_t(r):
        return pltpu.make_async_remote_copy(
            src_ref=ps_t.at[r], dst_ref=pr_t.at[r], send_sem=d_send.at[NM, r], recv_sem=d_recv.at[NM, r],
            device_id=partner, device_id_type=MESH)

    def out_m(n, r, rows):
        return pltpu.make_async_remote_copy(
            src_ref=own_m.at[n, r, pl.ds(0, rows)], dst_ref=rb_m.at[r, n, pl.ds(0, rows)],
            send_sem=r_send.at[n, r], recv_sem=r_recv.at[n, r], device_id=peers[r], device_id_type=MESH)

    def out_t(r):
        return pltpu.make_async_remote_copy(
            src_ref=own_t.at[r], dst_ref=rb_t.at[r], send_sem=r_send.at[NM, r], recv_sem=r_recv.at[NM, r],
            device_id=peers[r], device_id_type=MESH)

    def by_core(f):
        for k in range(2):
            @pl.when(core == k)
            def _(k=k):
                f(ROWS[k])

    def finish_m(n, rs):
        for r in rs:
            d2d(n, r).wait_recv()
            own_m[n, r] = own_m[n, r] + pr_m[n, r]

        def go(rows):
            for r in rs:
                if r < 3:
                    out_m(n, r, rows).start()

        by_core(go)

    def finish_t():
        for r in range(4):
            d2d_t(r).wait_recv()
            own_t[r] = own_t[r] + pr_t[r]
            if r < 3:
                out_t(r).start()

    tail_copy.wait()
    step1(lambda p, q: atail[p, q], 0)
    pl.semaphore_wait(barrier, 4)
    for pair in ((0, 1), (2, 3)):
        for r, w in zip(pair, step2(64, lt_mat[:, 0:64], pair)):
            for c in range(3):
                own_t[r, rows8(2 * c, 2), :] = w[rows8(0, 2), cols(c)]
                ps_t[r, rows8(2 * c, 2), :] = w[rows8(2, 2), cols(c)]
        for r in pair:
            d2d_t(r).start()
    for qp in range(4):
        a_copy(1, qp, 1).start()

    def body(n, carry):
        slot = lax.rem(n, 2)
        for half in range(2):
            qps = (2 * half, 2 * half + 1)
            for qp in qps:
                a_copy(n, qp, slot).wait()
            for qp in qps:
                step1(lambda p, q: abuf[slot, qp, p, q], qp)

            @pl.when(n + 2 < NM)
            def _():
                for qp in qps:
                    a_copy(n + 2, qp, slot).start()

            if half == 0:
                @pl.when(n == 0)
                def _():
                    finish_t()

            @pl.when(n > 0)
            def _():
                finish_m(n - 1, qps)

        for pair in ((0, 1), (2, 3)):
            for r, w in zip(pair, step2(256, l_mat[...], pair)):
                pack(own_m.at[n, r], w[rows8(0, 8)])
                pack(ps_m.at[n, r], w[rows8(8, 8)])
            for r in pair:
                d2d(n, r).start()
        return carry

    lax.fori_loop(0, NM, body, 0)
    finish_m(NM - 1, (0, 1))
    finish_m(NM - 1, (2, 3))

    def arrive(n, carry):
        def wait(rows):
            for r in range(3):
                out_m(n, r, rows).wait_recv()

        by_core(wait)
        return carry


    def w_rows(i, ns):
        def block(n, b):
            near = own_m[n, 3, rows8(b), :] + rb_m[1, n, rows8(b), :]
            far = rb_m[2, n, rows8(b), :] + rb_m[0, n, rows8(b), :]
            return near, far

        both = []
        for n in ns:
            parts_of = [block(n, place_of(i, c)) for c in range(3 if i else 2)]
            if not i:
                s = [jnp.zeros((8, L), F32)] * 2
                for m in range(NS):
                    piece = block(n, place_of(m + 1, 2))
                    here = (lane8 >= PW * m) & (lane8 < min(SP, PW * m + PW))
                    s = [jnp.where(here, pltpu.roll(v, PW * m + PW, 1), o) for v, o in zip(piece, s)]
                parts_of.append(s)
            both.append([jnp.concatenate(list(c), axis=1) for c in zip(*parts_of)])
        return [b[0] for b in both] + [b[1] for b in both]

    for r in range(3):
        out_t(r).wait_recv()
    lax.fori_loop(0, N1, arrive, 0)
    two = [rows8(2 * c, 2) for c in range(3)]
    tails = [jnp.concatenate([own_t[3, t, :] + rb_t[1, t, :] for t in two], axis=1),
             jnp.concatenate([rb_t[2, t, :] + rb_t[0, t, :] for t in two], axis=1)]
    which = jnp.where(kf < 2 * h1, -1, ((kf - 2 * h1) & 15) >> 1)

    def turned(w):
        return parts(jnp.concatenate([w[:, cols(c)].T for c in range(3)], axis=0))

    for i in range(8):
        w = jnp.concatenate(w_rows(i, range(N1)) + tails, axis=0)
        f1 = jnp.where((which < 0) | (which == i), f1_mat[...], 0.0).astype(BF16)
        v_acc[i] = dot(turned(w), jnp.concatenate([f1] * 3, axis=0))

    lax.fori_loop(N1, NM, arrive, 0)

    def home(i):
        return pltpu.make_async_copy(v_fin.at[i, core], out_hbm.at[core * 8 + i], o_sem.at[i])

    def back(i):
        return pltpu.make_async_remote_copy(
            src_ref=v_fin.at[i, 1 - core], dst_ref=out_hbm.at[core * 8 + i], send_sem=v_send.at[i],
            recv_sem=v_recv.at[i], device_id=partner, device_id_type=MESH)

    def back_in(i):
        return pltpu.make_async_remote_copy(
            src_ref=v_fin.at[i, 1 - core], dst_ref=out_hbm.at[(1 - core) * 8 + i], send_sem=v_send.at[i],
            recv_sem=v_recv.at[i], device_id=partner, device_id_type=MESH)

    rows = [v for i in range(7) for v in w_rows(i, range(N1, NM))]
    rows += [jnp.where(core == 0, v, 0.0) for v in w_rows(7, range(N1, NM))]
    w = turned(jnp.concatenate(rows, axis=0))
    for g in range(4):
        v = dot(w, f2_mat[:, cols(2 * g, 2)])
        for i in (2 * g, 2 * g + 1):
            vi = v_acc[i] + v[:, cols(i % 2)]
            for h in range(2):
                v_fin[i, h] = vi[CH * h:CH * h + NC, 0:NV]
        for i in (2 * g, 2 * g + 1):
            if i < 7:
                back(i).start()
                home(i).start()
            else:
                @pl.when(core == 0)
                def _():
                    back(7).start()
                    home(7).start()

    for i in range(7):
        home(i).wait()
        back(i).wait_send()
        back_in(i).wait_recv()

    @pl.when(core == 0)
    def _():
        home(7).wait()
        back(7).wait_send()

    @pl.when(core == 1)
    def _():
        back_in(7).wait_recv()

    for r in range(4):
        d2d_t(r).wait_send()
    for r in range(3):
        out_t(r).wait_send()

    def drain(n, carry):
        for r in range(4):
            d2d(n, r).wait_send()

        def wait(rows):
            for r in range(3):
                out_m(n, r, rows).wait_send()

        by_core(wait)
        return carry

    lax.fori_loop(0, NM, drain, 0)


def solution(mesh):
    def local_program(ints_blk, c_occ, c_vir):
        v = pl.pallas_call(
            kernel,
            out_shape=jax.ShapeDtypeStruct((NO, NC, NV), F32),
            in_specs=[pl.BlockSpec(memory_space=pl.ANY)] * 3,
            out_specs=pl.BlockSpec(memory_space=pl.ANY),
            scratch_shapes=[
                pltpu.VMEM((2, 4, NP, 2, NB, NB), BF16),
                pltpu.VMEM((NP, QT, NB, NB), BF16),
                pltpu.VMEM((NO, NB), BF16),
                pltpu.VMEM((NV, NB), BF16),
                pltpu.VMEM((16, L), F32),
                pltpu.VMEM((L, L), F32),
                pltpu.VMEM((L, 1024), BF16),
                pltpu.VMEM((4, 512, 256), BF16),
                pltpu.VMEM((2, 512, 256), BF16),
                pltpu.VMEM((L, 256), BF16),
                pltpu.VMEM((32, 256), BF16),
                pltpu.VMEM((L, L), F32),
                pltpu.VMEM((384, 1024), BF16),
                pltpu.VMEM((NO, 256, L), BF16),
                pltpu.VMEM((NM, 4, RW, L), F32),
                pltpu.VMEM((4, 48, L), F32),
                pltpu.VMEM((NM, 4, RW, L), F32),
                pltpu.VMEM((4, 48, L), F32),
                pltpu.VMEM((NM, 4, RW, L), F32),
                pltpu.VMEM((4, 48, L), F32),
                pltpu.VMEM((3, NM, RW, L), F32),
                pltpu.VMEM((3, 48, L), F32),
                pltpu.VMEM((8, LW, L), F32),
                pltpu.VMEM((8, 2, NC, NV), F32),
                pltpu.SemaphoreType.DMA((2, 4)),
                pltpu.SemaphoreType.DMA,
                pltpu.SemaphoreType.DMA((2,)),
                pltpu.SemaphoreType.DMA((NM + 1, 4)),
                pltpu.SemaphoreType.DMA((NM + 1, 4)),
                pltpu.SemaphoreType.DMA((NM + 1, 3)),
                pltpu.SemaphoreType.DMA((NM + 1, 3)),
                pltpu.SemaphoreType.DMA((8,)),
                pltpu.SemaphoreType.DMA((8,)),
                pltpu.SemaphoreType.DMA((8,)),
            ],
            compiler_params=pltpu.CompilerParams(
                collective_id=0, has_side_effects=True, vmem_limit_bytes=60 * 1024 * 1024),
            name='four_index',
        )(ints_blk, c_occ.T, c_vir.T)
        return v.transpose(0, 2, 1)

    return jax.shard_map(
        local_program,
        mesh=mesh,
        in_specs=(P(('frag', 'dev'), 'dev2', None, None), P('frag', None), P('frag', None)),
        out_specs=P(None, None, ('frag', 'dev2', 'dev')),
        check_vma=False,
    )
```

```python
import jax
import jax.numpy as jnp
from jax import lax
from jax.experimental import pallas as pl
from jax.experimental.pallas import tpu as pltpu
from jax.sharding import PartitionSpec as P

MESH = pl.DeviceIdType.MESH
F32, BF16, I32 = jnp.float32, jnp.bfloat16, jnp.int32

NP, NQ, NB = 29, 58, 116
NO, NV = 15, 96
QC = 8
NM = NQ // QC
QT = NQ - NM * QC
PG = 4
L = 128
LW = 3 * L
SP = 108
PW, NS = L - SP, 6
NC, CH = 180, 184
RW = 184
ROWS = (RW, RW - 24)
N1 = NM - 1


def place_of(i, c):
    return 3 * i - 1 + c if i else c


def cols(k, n=1):
    return slice(L * k, L * (k + n))


def rows8(k, n=1):
    return slice(8 * k, 8 * (k + n))


def iota(shape, dim):
    return lax.broadcasted_iota(I32, shape, dim)


def dot(a, b):
    return jnp.dot(a, b, preferred_element_type=F32)


def parts(w):
    hi = w.astype(BF16)
    rest = w - hi.astype(F32)
    mid = rest.astype(BF16)
    lo = (rest - mid.astype(F32)).astype(BF16)
    return jnp.concatenate([hi, mid, lo], axis=1)


def kernel(a_hbm, cot_hbm, cvt_hbm, out_hbm, abuf, atail, cot_in, cvt_in, cot, cvt, s_mat, b_mat, bs_mat, l_mat, lt_mat,
           f1_mat, f2_mat, x_buf, h_buf, own_m, own_t, ps_m, ps_t, pr_m, pr_t, rb_m, rb_t, v_acc, v_fin,
           a_sem, at_sem, c_sem, d_send, d_recv, r_send, r_recv, v_send, v_recv, o_sem):
    y = lax.axis_index('dev2')
    dev = lax.axis_index('dev')
    core = lax.rem(dev, 2)
    x = dev // 2
    partner = (0, y, x * 2 + (1 - core))
    peers = [(0, 1 - y, (1 - x) * 2 + core), (0, y, (1 - x) * 2 + core), (0, 1 - y, x * 2 + core)]
    chip = [2 * (1 - y) + (1 - x), 2 * y + (1 - x), 2 * (1 - y) + x, 2 * y + x]

    def a_copy(n, qp, slot):
        return pltpu.make_async_copy(
            a_hbm.at[:, pl.ds(n * QC + 2 * qp, 2)], abuf.at[slot, qp], a_sem.at[slot, qp])

    small = [pltpu.make_async_copy(cot_hbm, cot_in, c_sem.at[0]), pltpu.make_async_copy(cvt_hbm, cvt_in, c_sem.at[1])]
    tail_copy = pltpu.make_async_copy(a_hbm.at[:, pl.ds(NM * QC, QT)], atail, at_sem)
    for c in small:
        c.start()
    tail_copy.start()

    barrier = pltpu.get_barrier_semaphore()
    for other in [partner] + peers:
        pl.semaphore_signal(barrier, inc=1, device_id=other, device_id_type=MESH)

    cot[...] = jnp.zeros_like(cot)
    cvt[...] = jnp.zeros_like(cvt)
    for c in small:
        c.wait()
    cot[0:NO, 0:NB] = cot_in[...].astype(F32)
    cvt[0:NV, 0:NB] = cvt_in[...].astype(F32)
    for qp in range(4):
        a_copy(0, qp, 0).start()
    sub = iota((8, L), 0)
    zero = jnp.zeros((8, L), F32)
    for jj in range(8):
        for p in range(8):
            two = [jnp.where(sub == p, cot[j:j + 1, :], zero) for j in (2 * jj, 2 * jj + 1)]
            s_mat[rows8(2 * jj, 2), cols(p)] = jnp.concatenate(two, axis=0).astype(BF16)
    cv = cvt[...].T.astype(BF16)
    first = [(15 * c) // 4 for c in chip]
    first_s = [4 * c + 2 - c // 3 for c in chip]
    lane, row = iota((L, 256), 1), iota((L, 256), 0)
    want = jnp.where(lane < NC, lane, jnp.where(lane < CH, -100000, lane - 4)) - row
    lane_s, row_s = iota((L, L), 1), iota((L, L), 0)
    want_s = jnp.where(lane_s < SP, lane_s + 252, -100000) - row_s
    bs_mat[...] = jnp.zeros_like(bs_mat)
    for r in range(4):
        for j in range(4):
            place = jnp.where(want == 96 * (first[r] + j) - 360 * chip[r], 1.0, 0.0).astype(BF16)
            b_mat[r, cols(j), :] = dot(cv, place).astype(BF16)
        for j in range(2):
            place = jnp.where(want_s == 96 * (first_s[r] + j) - 360 * chip[r], 1.0, 0.0).astype(BF16)
            h = r % 2
            bs_mat[r // 2, cols(2 * h + j), cols(h)] = dot(cv, place).astype(BF16)
    low, high = cot[0:8, :], cot[8:16, :]
    mine = jnp.concatenate([jnp.where(core == 0, low, high), jnp.where(core == 0, high, low)], axis=0)
    kk = iota((L, 256), 1)
    ploc = ((kk >> 4) & 3) * 8 + (kk & 7)
    pick = (iota((L, 256), 0) == ploc + NP * dev) & (ploc < NP)
    l0 = dot(mine.astype(BF16), jnp.where(pick, 1.0, 0.0).astype(BF16)).astype(BF16)
    row, k2 = iota((L, 256), 0), iota((L, 256), 1)
    e8 = jnp.where((iota((L, 16), 0) >> 3) == iota((L, 16), 1), 1.0, 0.0).astype(BF16)
    l_mat[...] = jnp.where((k2 >> 6) * 2 + ((k2 >> 3) & 1) == (row & 7), dot(e8, l0), 0.0).astype(BF16)
    e2 = jnp.where((iota((32, 16), 0) >> 1) == iota((32, 16), 1), 1.0, 0.0).astype(BF16)
    rowt, kt = iota((32, 256), 0), iota((32, 256), 1)
    lt_mat[...] = jnp.where(((kt >> 3) & 1) == (rowt & 1), dot(e2, l0), 0.0).astype(BF16)

    base, other_base = NQ * y, NQ * (1 - y)

    def f_of(want_q):
        sel = jnp.where(iota((L, L), 1) == want_q, 1.0, 0.0).astype(BF16)
        return dot(sel, cv)

    kf = iota((L, L), 0)
    h1 = QC * N1
    f1_mat[...] = f_of(jnp.where(kf < h1, base + kf, jnp.where(kf < 2 * h1, other_base + kf - h1,
                       jnp.where(kf < 2 * h1 + 16, base, other_base) + NM * QC + (kf & 1))))
    f2 = f_of(jnp.where((kf & 8) == 0, base, other_base) + h1 + (kf & 7))
    for i in range(8):
        mine_f = jnp.where((kf >> 4) == i, f2, 0.0).astype(BF16)
        for k in range(3):
            f2_mat[cols(k), cols(i)] = mine_f

    def step1(tile_of, qp):
        zl = jnp.zeros((NB, L - NB), BF16)
        zs = jnp.zeros((L - NB, L), BF16)

        def tile(p, q):
            t = jnp.concatenate([tile_of(p, q), zl], axis=1)
            return jnp.concatenate([t, zs], axis=0)

        for pg in range(PG):
            ps = range(8 * pg, min(NP, 8 * pg + 8))
            rhs = jnp.concatenate([jnp.concatenate([tile(p, 0), tile(p, 1)], axis=1) for p in ps], axis=0)
            t = dot(s_mat[rows8(0, NO), cols(0, len(ps))], rhs)
            r = rows8(8 * qp + 2 * pg, 2)
            for j in range(NO):
                two = jnp.concatenate([t[rows8(j), cols(k)] for k in range(2)], axis=0)
                x_buf[j, r, :] = two.astype(BF16)

    def stage_h(rows, k):
        p, t = k // 3, k % 3
        if t < 2:
            js, weights = [first[2 * p + t] + j for j in range(4)], b_mat[2 * p + t]
        else:
            js, weights = [first_s[r] + j for r in (2 * p, 2 * p + 1) for j in range(2)], bs_mat[p]
        lhs = jnp.concatenate([x_buf[j, 0:rows, :] for j in js], axis=1)
        h_buf[k, 0:rows, :] = dot(lhs, weights).astype(BF16)

    def stage_w(rows, lhs, p):
        w = [dot(lhs, h_buf[3 * p + t, 0:rows, :]) for t in range(3)]
        return [jnp.concatenate([w[k], w[2][:, cols(k)]], axis=1) for k in range(2)]

    lane8 = iota((8, L), 1)
    spare = lane8 >= SP

    def pack(ref, w):
        col = [[w[rows8(i), cols(c)] for c in range(3)] for i in range(8)]
        for i in range(8):
            for c in range(3 if i else 2):
                v = col[i][c]
                if c == 2 and i <= NS:
                    v = jnp.where(spare, pltpu.roll(col[0][c], SP - PW * (i - 1), 1), v)
                ref[rows8(place_of(i, c)), :] = v

    def d2d(n, r):
        return pltpu.make_async_remote_copy(
            src_ref=ps_m.at[n, r], dst_ref=pr_m.at[n, r], send_sem=d_send.at[n, r], recv_sem=d_recv.at[n, r],
            device_id=partner, device_id_type=MESH)

    def d2d_t(r):
        return pltpu.make_async_remote_copy(
            src_ref=ps_t.at[r], dst_ref=pr_t.at[r], send_sem=d_send.at[NM, r], recv_sem=d_recv.at[NM, r],
            device_id=partner, device_id_type=MESH)

    def out_m(n, r, rows):
        return pltpu.make_async_remote_copy(
            src_ref=own_m.at[n, r, pl.ds(0, rows)], dst_ref=rb_m.at[r, n, pl.ds(0, rows)],
            send_sem=r_send.at[n, r], recv_sem=r_recv.at[n, r], device_id=peers[r], device_id_type=MESH)

    def out_t(r):
        return pltpu.make_async_remote_copy(
            src_ref=own_t.at[r], dst_ref=rb_t.at[r], send_sem=r_send.at[NM, r], recv_sem=r_recv.at[NM, r],
            device_id=peers[r], device_id_type=MESH)

    def by_core(f):
        for k in range(2):
            @pl.when(core == k)
            def _(k=k):
                f(ROWS[k])

    def finish_m(n, rs):
        for r in rs:
            d2d(n, r).wait_recv()
            own_m[n, r] = own_m[n, r] + pr_m[n, r]

        def go(rows):
            for r in rs:
                if r < 3:
                    out_m(n, r, rows).start()

        by_core(go)

    def finish_t():
        for r in range(4):
            d2d_t(r).wait_recv()
            own_t[r] = own_t[r] + pr_t[r]
            if r < 3:
                out_t(r).start()

    tail_copy.wait()
    step1(lambda p, q: atail[p, q], 0)
    pl.semaphore_wait(barrier, 4)
    for k in range(6):
        stage_h(64, k)
    for p in range(2):
        pair = (2 * p, 2 * p + 1)
        for r, w in zip(pair, stage_w(64, lt_mat[:, 0:64], p)):
            for c in range(3):
                own_t[r, rows8(2 * c, 2), :] = w[rows8(0, 2), cols(c)]
                ps_t[r, rows8(2 * c, 2), :] = w[rows8(2, 2), cols(c)]
        for r in pair:
            d2d_t(r).start()
    for qp in range(4):
        a_copy(1, qp, 1).start()

    def body(n, carry):
        slot = lax.rem(n, 2)
        for half in range(2):
            qps = (2 * half, 2 * half + 1)
            for qp in qps:
                a_copy(n, qp, slot).wait()
            for qp in qps:
                step1(lambda p, q: abuf[slot, qp, p, q], qp)

            @pl.when(n + 2 < NM)
            def _():
                for qp in qps:
                    a_copy(n + 2, qp, slot).start()

            if half == 0:
                @pl.when(n == 0)
                def _():
                    finish_t()

            @pl.when(n > 0)
            def _():
                finish_m(n - 1, qps)

        for k in range(6):
            stage_h(256, k)
        for p in range(2):
            pair = (2 * p, 2 * p + 1)
            for r, w in zip(pair, stage_w(256, l_mat[...], p)):
                pack(own_m.at[n, r], w[rows8(0, 8)])
                pack(ps_m.at[n, r], w[rows8(8, 8)])
            for r in pair:
                d2d(n, r).start()
        return carry

    lax.fori_loop(0, NM, body, 0)
    finish_m(NM - 1, (0, 1))
    finish_m(NM - 1, (2, 3))

    def arrive(n, carry):
        def wait(rows):
            for r in range(3):
                out_m(n, r, rows).wait_recv()

        by_core(wait)
        return carry


    def w_rows(i, ns):
        def block(n, b):
            near = own_m[n, 3, rows8(b), :] + rb_m[1, n, rows8(b), :]
            far = rb_m[2, n, rows8(b), :] + rb_m[0, n, rows8(b), :]
            return near, far

        both = []
        for n in ns:
            parts_of = [block(n, place_of(i, c)) for c in range(3 if i else 2)]
            if not i:
                s = [jnp.zeros((8, L), F32)] * 2
                for m in range(NS):
                    piece = block(n, place_of(m + 1, 2))
                    here = (lane8 >= PW * m) & (lane8 < min(SP, PW * m + PW))
                    s = [jnp.where(here, pltpu.roll(v, PW * m + PW, 1), o) for v, o in zip(piece, s)]
                parts_of.append(s)
            both.append([jnp.concatenate(list(c), axis=1) for c in zip(*parts_of)])
        return [b[0] for b in both] + [b[1] for b in both]

    for r in range(3):
        out_t(r).wait_recv()
    lax.fori_loop(0, N1, arrive, 0)
    two = [rows8(2 * c, 2) for c in range(3)]
    tails = [jnp.concatenate([own_t[3, t, :] + rb_t[1, t, :] for t in two], axis=1),
             jnp.concatenate([rb_t[2, t, :] + rb_t[0, t, :] for t in two], axis=1)]
    which = jnp.where(kf < 2 * h1, -1, ((kf - 2 * h1) & 15) >> 1)

    def turned(w):
        return parts(jnp.concatenate([w[:, cols(c)].T for c in range(3)], axis=0))

    for i in range(8):
        w = jnp.concatenate(w_rows(i, range(N1)) + tails, axis=0)
        f1 = jnp.where((which < 0) | (which == i), f1_mat[...], 0.0).astype(BF16)
        v_acc[i] = dot(turned(w), jnp.concatenate([f1] * 3, axis=0))

    for r in range(4):
        d2d_t(r).wait_send()
    for r in range(3):
        out_t(r).wait_send()

    def drain(n, carry):
        for r in range(4):
            d2d(n, r).wait_send()

        def wait(rows):
            for r in range(3):
                out_m(n, r, rows).wait_send()

        by_core(wait)
        return carry

    lax.fori_loop(0, N1, drain, 0)
    arrive(N1, 0)

    def home(i):
        return pltpu.make_async_copy(v_fin.at[i, core], out_hbm.at[core * 8 + i], o_sem.at[i])

    def back(i):
        return pltpu.make_async_remote_copy(
            src_ref=v_fin.at[i, 1 - core], dst_ref=out_hbm.at[core * 8 + i], send_sem=v_send.at[i],
            recv_sem=v_recv.at[i], device_id=partner, device_id_type=MESH)

    def back_in(i):
        return pltpu.make_async_remote_copy(
            src_ref=v_fin.at[i, 1 - core], dst_ref=out_hbm.at[(1 - core) * 8 + i], send_sem=v_send.at[i],
            recv_sem=v_recv.at[i], device_id=partner, device_id_type=MESH)

    rows = [v for i in range(7) for v in w_rows(i, range(N1, NM))]
    rows += [jnp.where(core == 0, v, 0.0) for v in w_rows(7, range(N1, NM))]
    w = turned(jnp.concatenate(rows, axis=0))
    vs = [dot(w, f2_mat[:, cols(2 * g, 2)]) for g in range(4)]
    for g, v in enumerate(vs):
        for i in (2 * g, 2 * g + 1):
            vi = v_acc[i] + v[:, cols(i % 2)]
            for h in range(2):
                v_fin[i, h] = vi[CH * h:CH * h + NC, 0:NV]
        if g % 2:
            for i in range(2 * g - 2, 2 * g + 2):
                if i < 7:
                    back(i).start()
                    home(i).start()
                else:
                    @pl.when(core == 0)
                    def _():
                        back(7).start()
                        home(7).start()

    for i in range(7):
        home(i).wait()
        back(i).wait_send()
        back_in(i).wait_recv()

    @pl.when(core == 0)
    def _():
        home(7).wait()
        back(7).wait_send()

    @pl.when(core == 1)
    def _():
        back_in(7).wait_recv()
    drain(NM - 1, 0)


def solution(mesh):
    def local_program(ints_blk, c_occ, c_vir):
        v = pl.pallas_call(
            kernel,
            out_shape=jax.ShapeDtypeStruct((NO, NC, NV), F32),
            in_specs=[pl.BlockSpec(memory_space=pl.ANY)] * 3,
            out_specs=pl.BlockSpec(memory_space=pl.ANY),
            scratch_shapes=[
                pltpu.VMEM((2, 4, NP, 2, NB, NB), BF16),
                pltpu.VMEM((NP, QT, NB, NB), BF16),
                pltpu.VMEM((NO, NB), BF16),
                pltpu.VMEM((NV, NB), BF16),
                pltpu.VMEM((16, L), F32),
                pltpu.VMEM((L, L), F32),
                pltpu.VMEM((L, 1024), BF16),
                pltpu.VMEM((4, 512, 256), BF16),
                pltpu.VMEM((2, 512, 256), BF16),
                pltpu.VMEM((L, 256), BF16),
                pltpu.VMEM((32, 256), BF16),
                pltpu.VMEM((L, L), F32),
                pltpu.VMEM((384, 1024), BF16),
                pltpu.VMEM((NO, 256, L), BF16),
                pltpu.VMEM((6, 256, 256), BF16),
                pltpu.VMEM((NM, 4, RW, L), F32),
                pltpu.VMEM((4, 48, L), F32),
                pltpu.VMEM((NM, 4, RW, L), F32),
                pltpu.VMEM((4, 48, L), F32),
                pltpu.VMEM((NM, 4, RW, L), F32),
                pltpu.VMEM((4, 48, L), F32),
                pltpu.VMEM((3, NM, RW, L), F32),
                pltpu.VMEM((3, 48, L), F32),
                pltpu.VMEM((8, LW, L), F32),
                pltpu.VMEM((8, 2, NC, NV), F32),
                pltpu.SemaphoreType.DMA((2, 4)),
                pltpu.SemaphoreType.DMA,
                pltpu.SemaphoreType.DMA((2,)),
                pltpu.SemaphoreType.DMA((NM + 1, 4)),
                pltpu.SemaphoreType.DMA((NM + 1, 4)),
                pltpu.SemaphoreType.DMA((NM + 1, 3)),
                pltpu.SemaphoreType.DMA((NM + 1, 3)),
                pltpu.SemaphoreType.DMA((8,)),
                pltpu.SemaphoreType.DMA((8,)),
                pltpu.SemaphoreType.DMA((8,)),
            ],
            compiler_params=pltpu.CompilerParams(
                collective_id=0, has_side_effects=True, vmem_limit_bytes=60 * 1024 * 1024),
            name='four_index',
        )(ints_blk, c_occ.T, c_vir.T)
        return v.transpose(0, 2, 1)

    return jax.shard_map(
        local_program,
        mesh=mesh,
        in_specs=(P(('frag', 'dev'), 'dev2', None, None), P('frag', None), P('frag', None)),
        out_specs=P(None, None, ('frag', 'dev2', 'dev')),
        check_vma=False,
    )
```

```python
import jax
import jax.numpy as jnp
from jax import lax
from jax.experimental import pallas as pl
from jax.experimental.pallas import tpu as pltpu
from jax.sharding import PartitionSpec as P

MESH = pl.DeviceIdType.MESH
F32, BF16, I32 = jnp.float32, jnp.bfloat16, jnp.int32

NP, NQ, NB = 29, 58, 116
NO, NV = 15, 96
QC = 8
NM = 6
SMALL = ((48, 2), (50, 4), (54, 4))
PG = 4
L = 128
LW = 3 * L
SP = 108
PW, NS = L - SP, 6
NC, CH = 180, 184
RW = 184
ROWS = (RW, RW - 24)
N1 = NM - 1


def place_of(i, c):
    return 3 * i - 1 + c if i else c


def cols(k, n=1):
    return slice(L * k, L * (k + n))


def rows8(k, n=1):
    return slice(8 * k, 8 * (k + n))


def iota(shape, dim):
    return lax.broadcasted_iota(I32, shape, dim)


def dot(a, b):
    return jnp.dot(a, b, preferred_element_type=F32)


def parts(w):
    hi = w.astype(BF16)
    rest = w - hi.astype(F32)
    mid = rest.astype(BF16)
    lo = (rest - mid.astype(F32)).astype(BF16)
    return jnp.concatenate([hi, mid, lo], axis=1)


def kernel(a_hbm, cot_hbm, cvt_hbm, out_hbm, abuf, as0, as1, as2, cot_in, cvt_in, cot, cvt, s_mat, b_mat, bs_mat, l8, l4, l2,
           f1_mat, f2_mat, x_buf, h_buf, own_m, own_s, ps_m, ps_s, pr_m, pr_s, rb_m, rb_s, v_acc, v_fin,
           a_sem, as_sem, c_sem, d_send, d_recv, r_send, r_recv, v_send, v_recv, o_sem):
    y = lax.axis_index('dev2')
    dev = lax.axis_index('dev')
    core = lax.rem(dev, 2)
    x = dev // 2
    partner = (0, y, x * 2 + (1 - core))
    peers = [(0, 1 - y, (1 - x) * 2 + core), (0, y, (1 - x) * 2 + core), (0, 1 - y, x * 2 + core)]
    chip = [2 * (1 - y) + (1 - x), 2 * y + (1 - x), 2 * (1 - y) + x, 2 * y + x]

    def a_copy(n, qp, slot):
        return pltpu.make_async_copy(
            a_hbm.at[:, pl.ds(n * QC + 2 * qp, 2)], abuf.at[slot, qp], a_sem.at[slot, qp])

    small = [pltpu.make_async_copy(cot_hbm, cot_in, c_sem.at[0]), pltpu.make_async_copy(cvt_hbm, cvt_in, c_sem.at[1])]
    a_small = (as0, as1, as2)
    small_copy = [pltpu.make_async_copy(a_hbm.at[:, pl.ds(q, nq)], a_small[m], as_sem.at[m])
                  for m, (q, nq) in enumerate(SMALL)]
    for c in small:
        c.start()
    small_copy[0].start()
    small_copy[1].start()

    barrier = pltpu.get_barrier_semaphore()
    for other in [partner] + peers:
        pl.semaphore_signal(barrier, inc=1, device_id=other, device_id_type=MESH)

    cot[...] = jnp.zeros_like(cot)
    cvt[...] = jnp.zeros_like(cvt)
    for c in small:
        c.wait()
    cot[0:NO, 0:NB] = cot_in[...].astype(F32)
    cvt[0:NV, 0:NB] = cvt_in[...].astype(F32)
    sub = iota((8, L), 0)
    zero = jnp.zeros((8, L), F32)
    for jj in range(8):
        for p in range(8):
            two = [jnp.where(sub == p, cot[j:j + 1, :], zero) for j in (2 * jj, 2 * jj + 1)]
            s_mat[rows8(2 * jj, 2), cols(p)] = jnp.concatenate(two, axis=0).astype(BF16)
    cv = cvt[...].T.astype(BF16)
    first = [(15 * c) // 4 for c in chip]
    first_s = [4 * c + 2 - c // 3 for c in chip]
    lane, row = iota((L, 256), 1), iota((L, 256), 0)
    want = jnp.where(lane < NC, lane, jnp.where(lane < CH, -100000, lane - 4)) - row
    lane_s, row_s = iota((L, L), 1), iota((L, L), 0)
    want_s = jnp.where(lane_s < SP, lane_s + 252, -100000) - row_s
    bs_mat[...] = jnp.zeros_like(bs_mat)
    for r in range(4):
        for j in range(4):
            place = jnp.where(want == 96 * (first[r] + j) - 360 * chip[r], 1.0, 0.0).astype(BF16)
            b_mat[r, cols(j), :] = dot(cv, place).astype(BF16)
        for j in range(2):
            place = jnp.where(want_s == 96 * (first_s[r] + j) - 360 * chip[r], 1.0, 0.0).astype(BF16)
            h = r % 2
            bs_mat[r // 2, cols(2 * h + j), cols(h)] = dot(cv, place).astype(BF16)
    low, high = cot[0:8, :], cot[8:16, :]
    mine = jnp.concatenate([jnp.where(core == 0, low, high), jnp.where(core == 0, high, low)], axis=0)
    kk = iota((L, 256), 1)
    ploc = ((kk >> 4) & 3) * 8 + (kk & 7)
    pick = (iota((L, 256), 0) == ploc + NP * dev) & (ploc < NP)
    l0 = dot(mine.astype(BF16), jnp.where(pick, 1.0, 0.0).astype(BF16)).astype(BF16)
    for l_mat, sh in ((l8, 3), (l4, 2), (l2, 1)):
        nq = 1 << sh
        rows = 16 * nq
        e = jnp.where((iota((rows, 16), 0) >> sh) == iota((rows, 16), 1), 1.0, 0.0).astype(BF16)
        row, k2 = iota((rows, 256), 0), iota((rows, 256), 1)
        here = (k2 >> 6) * 2 + ((k2 >> 3) & 1) == (row & (nq - 1))
        l_mat[...] = jnp.where(here, dot(e, l0), 0.0).astype(BF16)

    base, other_base = NQ * y, NQ * (1 - y)

    def f_of(want_q):
        sel = jnp.where(iota((L, L), 1) == want_q, 1.0, 0.0).astype(BF16)
        return dot(sel, cv)

    kf = iota((L, L), 0)
    h1 = QC * N1
    kt = kf - 2 * h1
    ks, ku = kt >> 4, kt & 7
    kq = jnp.where(ks == 0, SMALL[0][0] + (ku & 1), jnp.where(ks == 1, SMALL[1][0], SMALL[2][0]) + (ku & 3))
    f1_mat[...] = f_of(jnp.where(kt < 0, jnp.where(kf < h1, base + kf, other_base + kf - h1),
                       jnp.where((kt & 8) == 0, base, other_base) + kq))
    f2 = f_of(jnp.where((kf & 8) == 0, base, other_base) + h1 + (kf & 7))
    for i in range(8):
        mine_f = jnp.where((kf >> 4) == i, f2, 0.0).astype(BF16)
        for k in range(3):
            f2_mat[cols(k), cols(i)] = mine_f

    def step1(tile_of, qp):
        zl = jnp.zeros((NB, L - NB), BF16)
        zs = jnp.zeros((L - NB, L), BF16)

        def tile(p, q):
            t = jnp.concatenate([tile_of(p, q), zl], axis=1)
            return jnp.concatenate([t, zs], axis=0)

        for pg in range(PG):
            ps = range(8 * pg, min(NP, 8 * pg + 8))
            rhs = jnp.concatenate([jnp.concatenate([tile(p, 0), tile(p, 1)], axis=1) for p in ps], axis=0)
            t = dot(s_mat[rows8(0, NO), cols(0, len(ps))], rhs)
            r = rows8(8 * qp + 2 * pg, 2)
            for j in range(NO):
                two = jnp.concatenate([t[rows8(j), cols(k)] for k in range(2)], axis=0)
                x_buf[j, r, :] = two.astype(BF16)

    def stage_h(rows, k):
        p, t = k // 3, k % 3
        if t < 2:
            js, weights = [first[2 * p + t] + j for j in range(4)], b_mat[2 * p + t]
        else:
            js, weights = [first_s[r] + j for r in (2 * p, 2 * p + 1) for j in range(2)], bs_mat[p]
        lhs = jnp.concatenate([x_buf[j, 0:rows, :] for j in js], axis=1)
        h_buf[k, 0:rows, :] = dot(lhs, weights).astype(BF16)

    def stage_w(rows, lhs, p):
        w = [dot(lhs, h_buf[3 * p + t, 0:rows, :]) for t in range(3)]
        return [jnp.concatenate([w[k], w[2][:, cols(k)]], axis=1) for k in range(2)]

    lane8 = iota((8, L), 1)
    spare = lane8 >= SP

    def pack(ref, w):
        col = [[w[rows8(i), cols(c)] for c in range(3)] for i in range(8)]
        for i in range(8):
            for c in range(3 if i else 2):
                v = col[i][c]
                if c == 2 and i <= NS:
                    v = jnp.where(spare, pltpu.roll(col[0][c], SP - PW * (i - 1), 1), v)
                ref[rows8(place_of(i, c)), :] = v

    def d2d(n, r):
        return pltpu.make_async_remote_copy(
            src_ref=ps_m.at[n, r], dst_ref=pr_m.at[n, r], send_sem=d_send.at[n, r], recv_sem=d_recv.at[n, r],
            device_id=partner, device_id_type=MESH)

    def d2d_s(m, r):
        part = pl.ds(0, 24 * SMALL[m][1])
        return pltpu.make_async_remote_copy(
            src_ref=ps_s.at[m, r, part], dst_ref=pr_s.at[m, r, part], send_sem=d_send.at[NM + m, r],
            recv_sem=d_recv.at[NM + m, r], device_id=partner, device_id_type=MESH)

    def out_m(n, r, rows):
        return pltpu.make_async_remote_copy(
            src_ref=own_m.at[n, r, pl.ds(0, rows)], dst_ref=rb_m.at[r, n, pl.ds(0, rows)],
            send_sem=r_send.at[n, r], recv_sem=r_recv.at[n, r], device_id=peers[r], device_id_type=MESH)

    def out_s(m, r):
        part = pl.ds(0, 24 * SMALL[m][1])
        return pltpu.make_async_remote_copy(
            src_ref=own_s.at[m, r, part], dst_ref=rb_s.at[r, m, part], send_sem=r_send.at[NM + m, r],
            recv_sem=r_recv.at[NM + m, r], device_id=peers[r], device_id_type=MESH)

    def by_core(f):
        for k in range(2):
            @pl.when(core == k)
            def _(k=k):
                f(ROWS[k])

    def finish_m(n, rs):
        for r in rs:
            d2d(n, r).wait_recv()
            own_m[n, r] = own_m[n, r] + pr_m[n, r]

        def go(rows):
            for r in rs:
                if r < 3:
                    out_m(n, r, rows).start()

        by_core(go)

    def finish_s(m):
        part = rows8(0, 3 * SMALL[m][1])
        for r in range(4):
            d2d_s(m, r).wait_recv()
            own_s[m, r, part, :] = own_s[m, r, part, :] + pr_s[m, r, part, :]
            if r < 3:
                out_s(m, r).start()

    small_copy[2].start()
    for m, (l_mat, a_ref) in enumerate(zip((l2, l4, l4), a_small)):
        nq = SMALL[m][1]
        small_copy[m].wait()
        for qp in range(nq // 2):
            step1(lambda p, q: a_ref[p, 2 * qp + q], qp)
        if m == 0:
            pl.semaphore_wait(barrier, 4)
        rows = 32 * nq
        for k in range(6):
            stage_h(rows, k)
        for p in range(2):
            pair = (2 * p, 2 * p + 1)
            for r, w in zip(pair, stage_w(rows, l_mat[:, 0:rows], p)):
                for c in range(3):
                    own_s[m, r, rows8(c * nq, nq), :] = w[rows8(0, nq), cols(c)]
                    ps_s[m, r, rows8(c * nq, nq), :] = w[rows8(nq, nq), cols(c)]
            for r in pair:
                d2d_s(m, r).start()
        if m < 2:
            for qp in range(4):
                a_copy(m, qp, m).start()
        if m > 0:
            finish_s(m - 1)

    def body(n, carry):
        slot = lax.rem(n, 2)
        for half in range(2):
            qps = (2 * half, 2 * half + 1)
            for qp in qps:
                a_copy(n, qp, slot).wait()
            for qp in qps:
                step1(lambda p, q: abuf[slot, qp, p, q], qp)

            @pl.when(n + 2 < NM)
            def _():
                for qp in qps:
                    a_copy(n + 2, qp, slot).start()

            if half == 1:
                @pl.when(n == 0)
                def _():
                    finish_s(2)

            @pl.when(n > 0)
            def _():
                finish_m(n - 1, qps)

        for k in range(6):
            stage_h(256, k)
        for p in range(2):
            pair = (2 * p, 2 * p + 1)
            for r, w in zip(pair, stage_w(256, l8[...], p)):
                pack(own_m.at[n, r], w[rows8(0, 8)])
                pack(ps_m.at[n, r], w[rows8(8, 8)])
            for r in pair:
                d2d(n, r).start()
        return carry

    lax.fori_loop(0, NM, body, 0)
    finish_m(NM - 1, (0, 1))
    finish_m(NM - 1, (2, 3))

    def arrive(n, carry):
        def wait(rows):
            for r in range(3):
                out_m(n, r, rows).wait_recv()

        by_core(wait)
        return carry


    def w_rows(i, ns):
        def block(n, b):
            near = own_m[n, 3, rows8(b), :] + rb_m[1, n, rows8(b), :]
            far = rb_m[2, n, rows8(b), :] + rb_m[0, n, rows8(b), :]
            return near, far

        both = []
        for n in ns:
            parts_of = [block(n, place_of(i, c)) for c in range(3 if i else 2)]
            if not i:
                s = [jnp.zeros((8, L), F32)] * 2
                for m in range(NS):
                    piece = block(n, place_of(m + 1, 2))
                    here = (lane8 >= PW * m) & (lane8 < min(SP, PW * m + PW))
                    s = [jnp.where(here, pltpu.roll(v, PW * m + PW, 1), o) for v, o in zip(piece, s)]
                parts_of.append(s)
            both.append([jnp.concatenate(list(c), axis=1) for c in zip(*parts_of)])
        return [b[0] for b in both] + [b[1] for b in both]

    def small_rows(i):
        out = []
        for m, (_, nq) in enumerate(SMALL):
            own, ins = [], []
            for c in range(3):
                t = rows8(c * nq + (i * nq) // 8)
                own.append(own_s[m, 3, t, :] + rb_s[1, m, t, :])
                ins.append(rb_s[2, m, t, :] + rb_s[0, m, t, :])
            out += [jnp.concatenate(own, axis=1), jnp.concatenate(ins, axis=1)]
        return out

    for m in range(3):
        for r in range(3):
            out_s(m, r).wait_recv()
    lax.fori_loop(0, N1, arrive, 0)

    def turned(w):
        return parts(jnp.concatenate([w[:, cols(c)].T for c in range(3)], axis=0))

    for i in range(8):
        w = jnp.concatenate(w_rows(i, range(N1)) + small_rows(i), axis=0)
        here = (kt < 0) | ((ks == 0) & (ku >> 1 == i % 4)) | ((ks > 0) & (ku >> 2 == i % 2))
        f1 = jnp.where(here, f1_mat[...], 0.0).astype(BF16)
        v_acc[i] = dot(turned(w), jnp.concatenate([f1] * 3, axis=0))

    for m in range(3):
        for r in range(4):
            d2d_s(m, r).wait_send()
        for r in range(3):
            out_s(m, r).wait_send()

    def drain(n, carry):
        for r in range(4):
            d2d(n, r).wait_send()

        def wait(rows):
            for r in range(3):
                out_m(n, r, rows).wait_send()

        by_core(wait)
        return carry

    lax.fori_loop(0, N1, drain, 0)
    arrive(N1, 0)

    def home(i):
        return pltpu.make_async_copy(v_fin.at[i, core], out_hbm.at[core * 8 + i], o_sem.at[i])

    def back(i):
        return pltpu.make_async_remote_copy(
            src_ref=v_fin.at[i, 1 - core], dst_ref=out_hbm.at[core * 8 + i], send_sem=v_send.at[i],
            recv_sem=v_recv.at[i], device_id=partner, device_id_type=MESH)

    def back_in(i):
        return pltpu.make_async_remote_copy(
            src_ref=v_fin.at[i, 1 - core], dst_ref=out_hbm.at[(1 - core) * 8 + i], send_sem=v_send.at[i],
            recv_sem=v_recv.at[i], device_id=partner, device_id_type=MESH)

    rows = [v for i in range(7) for v in w_rows(i, range(N1, NM))]
    rows += [jnp.where(core == 0, v, 0.0) for v in w_rows(7, range(N1, NM))]
    w = turned(jnp.concatenate(rows, axis=0))
    vs = [dot(w, f2_mat[:, cols(2 * g, 2)]) for g in range(4)]
    for g, v in enumerate(vs):
        for i in (2 * g, 2 * g + 1):
            vi = v_acc[i] + v[:, cols(i % 2)]
            for h in range(2):
                v_fin[i, h] = vi[CH * h:CH * h + NC, 0:NV]
        if g % 2:
            for i in range(2 * g - 2, 2 * g + 2):
                if i < 7:
                    back(i).start()
                    home(i).start()
                else:
                    @pl.when(core == 0)
                    def _():
                        back(7).start()
                        home(7).start()

    for i in range(7):
        home(i).wait()
        back(i).wait_send()
        back_in(i).wait_recv()

    @pl.when(core == 0)
    def _():
        home(7).wait()
        back(7).wait_send()

    @pl.when(core == 1)
    def _():
        back_in(7).wait_recv()
    drain(NM - 1, 0)


def solution(mesh):
    def local_program(ints_blk, c_occ, c_vir):
        v = pl.pallas_call(
            kernel,
            out_shape=jax.ShapeDtypeStruct((NO, NC, NV), F32),
            in_specs=[pl.BlockSpec(memory_space=pl.ANY)] * 3,
            out_specs=pl.BlockSpec(memory_space=pl.ANY),
            scratch_shapes=[
                pltpu.VMEM((2, 4, NP, 2, NB, NB), BF16),
                pltpu.VMEM((NP, 2, NB, NB), BF16),
                pltpu.VMEM((NP, 4, NB, NB), BF16),
                pltpu.VMEM((NP, 4, NB, NB), BF16),
                pltpu.VMEM((NO, NB), BF16),
                pltpu.VMEM((NV, NB), BF16),
                pltpu.VMEM((16, L), F32),
                pltpu.VMEM((L, L), F32),
                pltpu.VMEM((L, 1024), BF16),
                pltpu.VMEM((4, 512, 256), BF16),
                pltpu.VMEM((2, 512, 256), BF16),
                pltpu.VMEM((L, 256), BF16),
                pltpu.VMEM((64, 256), BF16),
                pltpu.VMEM((32, 256), BF16),
                pltpu.VMEM((L, L), F32),
                pltpu.VMEM((384, 1024), BF16),
                pltpu.VMEM((NO, 256, L), BF16),
                pltpu.VMEM((6, 256, 256), BF16),
                pltpu.VMEM((NM, 4, RW, L), F32),
                pltpu.VMEM((3, 4, 96, L), F32),
                pltpu.VMEM((NM, 4, RW, L), F32),
                pltpu.VMEM((3, 4, 96, L), F32),
                pltpu.VMEM((NM, 4, RW, L), F32),
                pltpu.VMEM((3, 4, 96, L), F32),
                pltpu.VMEM((3, NM, RW, L), F32),
                pltpu.VMEM((3, 3, 96, L), F32),
                pltpu.VMEM((8, LW, L), F32),
                pltpu.VMEM((8, 2, NC, NV), F32),
                pltpu.SemaphoreType.DMA((2, 4)),
                pltpu.SemaphoreType.DMA((3,)),
                pltpu.SemaphoreType.DMA((2,)),
                pltpu.SemaphoreType.DMA((NM + 3, 4)),
                pltpu.SemaphoreType.DMA((NM + 3, 4)),
                pltpu.SemaphoreType.DMA((NM + 3, 3)),
                pltpu.SemaphoreType.DMA((NM + 3, 3)),
                pltpu.SemaphoreType.DMA((8,)),
                pltpu.SemaphoreType.DMA((8,)),
                pltpu.SemaphoreType.DMA((8,)),
            ],
            compiler_params=pltpu.CompilerParams(
                collective_id=0, has_side_effects=True, vmem_limit_bytes=60 * 1024 * 1024),
            name='four_index',
        )(ints_blk, c_occ.T, c_vir.T)
        return v.transpose(0, 2, 1)

    return jax.shard_map(
        local_program,
        mesh=mesh,
        in_specs=(P(('frag', 'dev'), 'dev2', None, None), P('frag', None), P('frag', None)),
        out_specs=P(None, None, ('frag', 'dev2', 'dev')),
        check_vma=False,
    )
```

```python
import jax
import jax.numpy as jnp
from jax import lax
from jax.experimental import pallas as pl
from jax.experimental.pallas import tpu as pltpu
from jax.sharding import PartitionSpec as P

MESH = pl.DeviceIdType.MESH
F32, BF16, I32 = jnp.float32, jnp.bfloat16, jnp.int32

NP, NQ, NB = 29, 58, 116
NO, NV = 15, 96
QC = 8
NM = 6
SMALL = ((48, 2), (50, 4), (54, 4))
PG = 4
L = 128
LW = 3 * L
SP = 108
PW, NS = L - SP, 6
NC, CH = 180, 184
RW = 184
ROWS = (RW, RW - 24)
N1 = NM - 1


def place_of(i, c):
    return 3 * i - 1 + c if i else c


def cols(k, n=1):
    return slice(L * k, L * (k + n))


def rows8(k, n=1):
    return slice(8 * k, 8 * (k + n))


def iota(shape, dim):
    return lax.broadcasted_iota(I32, shape, dim)


def dot(a, b):
    return jnp.dot(a, b, preferred_element_type=F32)


def parts(w):
    hi = w.astype(BF16)
    rest = w - hi.astype(F32)
    mid = rest.astype(BF16)
    lo = (rest - mid.astype(F32)).astype(BF16)
    return jnp.concatenate([hi, mid, lo], axis=1)


def kernel(a_hbm, cot_hbm, cvt_hbm, out_ref, abuf, as0, as1, as2, cot_in, cvt_in, cot, cvt, s_mat, b_mat, bs_mat, l8, l4, l2,
           f1_mat, f2_mat, x_buf, h_buf, own_m, own_s, ps_m, ps_s, pr_m, pr_s, rb_m, rb_s, v_acc, v_fin,
           a_sem, as_sem, c_sem, d_send, d_recv, r_send, r_recv, v_send, v_recv):
    y = lax.axis_index('dev2')
    dev = lax.axis_index('dev')
    core = lax.rem(dev, 2)
    x = dev // 2
    partner = (0, y, x * 2 + (1 - core))
    peers = [(0, 1 - y, (1 - x) * 2 + core), (0, y, (1 - x) * 2 + core), (0, 1 - y, x * 2 + core)]
    chip = [2 * (1 - y) + (1 - x), 2 * y + (1 - x), 2 * (1 - y) + x, 2 * y + x]

    def a_copy(n, qp, slot):
        return pltpu.make_async_copy(
            a_hbm.at[:, pl.ds(n * QC + 2 * qp, 2)], abuf.at[slot, qp], a_sem.at[slot, qp])

    small = [pltpu.make_async_copy(cot_hbm, cot_in, c_sem.at[0]), pltpu.make_async_copy(cvt_hbm, cvt_in, c_sem.at[1])]
    a_small = (as0, as1, as2)
    small_copy = [pltpu.make_async_copy(a_hbm.at[:, pl.ds(q, nq)], a_small[m], as_sem.at[m])
                  for m, (q, nq) in enumerate(SMALL)]
    for c in small:
        c.start()
    small_copy[0].start()
    small_copy[1].start()

    barrier = pltpu.get_barrier_semaphore()
    for other in [partner] + peers:
        pl.semaphore_signal(barrier, inc=1, device_id=other, device_id_type=MESH)

    cot[...] = jnp.zeros_like(cot)
    cvt[...] = jnp.zeros_like(cvt)
    for c in small:
        c.wait()
    cot[0:NO, 0:NB] = cot_in[...].astype(F32)
    cvt[0:NV, 0:NB] = cvt_in[...].astype(F32)
    sub = iota((8, L), 0)
    zero = jnp.zeros((8, L), F32)
    for jj in range(8):
        for p in range(8):
            two = [jnp.where(sub == p, cot[j:j + 1, :], zero) for j in (2 * jj, 2 * jj + 1)]
            s_mat[rows8(2 * jj, 2), cols(p)] = jnp.concatenate(two, axis=0).astype(BF16)
    cv = cvt[...].T.astype(BF16)
    first = [(15 * c) // 4 for c in chip]
    first_s = [4 * c + 2 - c // 3 for c in chip]
    lane, row = iota((L, 256), 1), iota((L, 256), 0)
    want = jnp.where(lane < NC, lane, jnp.where(lane < CH, -100000, lane - 4)) - row
    lane_s, row_s = iota((L, L), 1), iota((L, L), 0)
    want_s = jnp.where(lane_s < SP, lane_s + 252, -100000) - row_s
    bs_mat[...] = jnp.zeros_like(bs_mat)
    for r in range(4):
        for j in range(4):
            place = jnp.where(want == 96 * (first[r] + j) - 360 * chip[r], 1.0, 0.0).astype(BF16)
            b_mat[r, cols(j), :] = dot(cv, place).astype(BF16)
        for j in range(2):
            place = jnp.where(want_s == 96 * (first_s[r] + j) - 360 * chip[r], 1.0, 0.0).astype(BF16)
            h = r % 2
            bs_mat[r // 2, cols(2 * h + j), cols(h)] = dot(cv, place).astype(BF16)
    low, high = cot[0:8, :], cot[8:16, :]
    mine = jnp.concatenate([jnp.where(core == 0, low, high), jnp.where(core == 0, high, low)], axis=0)
    kk = iota((L, 256), 1)
    ploc = ((kk >> 4) & 3) * 8 + (kk & 7)
    pick = (iota((L, 256), 0) == ploc + NP * dev) & (ploc < NP)
    l0 = dot(mine.astype(BF16), jnp.where(pick, 1.0, 0.0).astype(BF16)).astype(BF16)
    def build_l(l_mat, sh):
        nq = 1 << sh
        rows = 16 * nq
        e = jnp.where((iota((rows, 16), 0) >> sh) == iota((rows, 16), 1), 1.0, 0.0).astype(BF16)
        row, k2 = iota((rows, 256), 0), iota((rows, 256), 1)
        here = (k2 >> 6) * 2 + ((k2 >> 3) & 1) == (row & (nq - 1))
        l_mat[...] = jnp.where(here, dot(e, l0), 0.0).astype(BF16)

    build_l(l2, 1)

    def step1(tile_of, qp):
        zl = jnp.zeros((NB, L - NB), BF16)
        zs = jnp.zeros((L - NB, L), BF16)

        def tile(p, q):
            t = jnp.concatenate([tile_of(p, q), zl], axis=1)
            return jnp.concatenate([t, zs], axis=0)

        for pg in range(PG):
            ps = range(8 * pg, min(NP, 8 * pg + 8))
            rhs = jnp.concatenate([jnp.concatenate([tile(p, 0), tile(p, 1)], axis=1) for p in ps], axis=0)
            t = dot(s_mat[rows8(0, NO), cols(0, len(ps))], rhs)
            r = rows8(8 * qp + 2 * pg, 2)
            for j in range(NO):
                two = jnp.concatenate([t[rows8(j), cols(k)] for k in range(2)], axis=0)
                x_buf[j, r, :] = two.astype(BF16)

    def stage_h(rows, k):
        p, t = k // 3, k % 3
        if t < 2:
            js, weights = [first[2 * p + t] + j for j in range(4)], b_mat[2 * p + t]
        else:
            js, weights = [first_s[r] + j for r in (2 * p, 2 * p + 1) for j in range(2)], bs_mat[p]
        lhs = jnp.concatenate([x_buf[j, 0:rows, :] for j in js], axis=1)
        h_buf[k, 0:rows, :] = dot(lhs, weights).astype(BF16)

    def stage_w(rows, lhs, p):
        w = [dot(lhs, h_buf[3 * p + t, 0:rows, :]) for t in range(3)]
        return [jnp.concatenate([w[k], w[2][:, cols(k)]], axis=1) for k in range(2)]

    lane8 = iota((8, L), 1)
    spare = lane8 >= SP

    def pack(ref, w):
        col = [[w[rows8(i), cols(c)] for c in range(3)] for i in range(8)]
        for i in range(8):
            for c in range(3 if i else 2):
                v = col[i][c]
                if c == 2 and i <= NS:
                    v = jnp.where(spare, pltpu.roll(col[0][c], SP - PW * (i - 1), 1), v)
                ref[rows8(place_of(i, c)), :] = v

    def d2d(n, r):
        return pltpu.make_async_remote_copy(
            src_ref=ps_m.at[n, r], dst_ref=pr_m.at[n, r], send_sem=d_send.at[n, r], recv_sem=d_recv.at[n, r],
            device_id=partner, device_id_type=MESH)

    def d2d_s(m, r):
        part = pl.ds(0, 24 * SMALL[m][1])
        return pltpu.make_async_remote_copy(
            src_ref=ps_s.at[m, r, part], dst_ref=pr_s.at[m, r, part], send_sem=d_send.at[NM + m, r],
            recv_sem=d_recv.at[NM + m, r], device_id=partner, device_id_type=MESH)

    def out_m(n, r, rows):
        return pltpu.make_async_remote_copy(
            src_ref=own_m.at[n, r, pl.ds(0, rows)], dst_ref=rb_m.at[r, n, pl.ds(0, rows)],
            send_sem=r_send.at[n, r], recv_sem=r_recv.at[n, r], device_id=peers[r], device_id_type=MESH)

    def out_s(m, r):
        part = pl.ds(0, 24 * SMALL[m][1])
        return pltpu.make_async_remote_copy(
            src_ref=own_s.at[m, r, part], dst_ref=rb_s.at[r, m, part], send_sem=r_send.at[NM + m, r],
            recv_sem=r_recv.at[NM + m, r], device_id=peers[r], device_id_type=MESH)

    def by_core(f):
        for k in range(2):
            @pl.when(core == k)
            def _(k=k):
                f(ROWS[k])

    def finish_m(n, rs):
        for r in rs:
            d2d(n, r).wait_recv()
            own_m[n, r] = own_m[n, r] + pr_m[n, r]

        def go(rows):
            for r in rs:
                if r < 3:
                    out_m(n, r, rows).start()

        by_core(go)

    def finish_s(m):
        part = rows8(0, 3 * SMALL[m][1])
        for r in range(4):
            d2d_s(m, r).wait_recv()
            own_s[m, r, part, :] = own_s[m, r, part, :] + pr_s[m, r, part, :]
            if r < 3:
                out_s(m, r).start()

    small_copy[2].start()
    for m, (l_mat, a_ref) in enumerate(zip((l2, l4, l4), a_small)):
        nq = SMALL[m][1]
        small_copy[m].wait()
        for qp in range(nq // 2):
            step1(lambda p, q: a_ref[p, 2 * qp + q], qp)
        if m == 0:
            pl.semaphore_wait(barrier, 4)
        else:
            finish_s(m - 1)
        rows = 32 * nq
        for k in range(6):
            stage_h(rows, k)
        for p in range(2):
            pair = (2 * p, 2 * p + 1)
            for r, w in zip(pair, stage_w(rows, l_mat[:, 0:rows], p)):
                for c in range(3):
                    own_s[m, r, rows8(c * nq, nq), :] = w[rows8(0, nq), cols(c)]
                    ps_s[m, r, rows8(c * nq, nq), :] = w[rows8(nq, nq), cols(c)]
            for r in pair:
                d2d_s(m, r).start()
        if m < 2:
            for qp in range(4):
                a_copy(m, qp, m).start()
        if m == 0:
            build_l(l4, 2)
            build_l(l8, 3)

    def body(n, carry):
        slot = lax.rem(n, 2)
        for half in range(2):
            qps = (2 * half, 2 * half + 1)
            for qp in qps:
                a_copy(n, qp, slot).wait()
            for qp in qps:
                step1(lambda p, q: abuf[slot, qp, p, q], qp)

            @pl.when(n + 2 < NM)
            def _():
                for qp in qps:
                    a_copy(n + 2, qp, slot).start()

            if half == 0:
                @pl.when(n == 0)
                def _():
                    finish_s(2)

            @pl.when(n > 0)
            def _():
                finish_m(n - 1, qps)

        for k in range(6):
            stage_h(256, k)
        for p in range(2):
            pair = (2 * p, 2 * p + 1)
            for r, w in zip(pair, stage_w(256, l8[...], p)):
                pack(own_m.at[n, r], w[rows8(0, 8)])
                pack(ps_m.at[n, r], w[rows8(8, 8)])
            for r in pair:
                d2d(n, r).start()
        return carry

    lax.fori_loop(0, NM, body, 0)
    finish_m(NM - 1, (0, 1))
    finish_m(NM - 1, (2, 3))

    def arrive(n, carry):
        def wait(rows):
            for r in range(3):
                out_m(n, r, rows).wait_recv()

        by_core(wait)
        return carry


    def w_rows(i, ns):
        def block(n, b):
            near = own_m[n, 3, rows8(b), :] + rb_m[1, n, rows8(b), :]
            far = rb_m[2, n, rows8(b), :] + rb_m[0, n, rows8(b), :]
            return near, far

        both = []
        for n in ns:
            parts_of = [block(n, place_of(i, c)) for c in range(3 if i else 2)]
            if not i:
                s = [jnp.zeros((8, L), F32)] * 2
                for m in range(NS):
                    piece = block(n, place_of(m + 1, 2))
                    here = (lane8 >= PW * m) & (lane8 < min(SP, PW * m + PW))
                    s = [jnp.where(here, pltpu.roll(v, PW * m + PW, 1), o) for v, o in zip(piece, s)]
                parts_of.append(s)
            both.append([jnp.concatenate(list(c), axis=1) for c in zip(*parts_of)])
        return [b[0] for b in both] + [b[1] for b in both]

    def small_rows(i):
        out = []
        for m, (_, nq) in enumerate(SMALL):
            own, ins = [], []
            for c in range(3):
                t = rows8(c * nq + (i * nq) // 8)
                own.append(own_s[m, 3, t, :] + rb_s[1, m, t, :])
                ins.append(rb_s[2, m, t, :] + rb_s[0, m, t, :])
            out += [jnp.concatenate(own, axis=1), jnp.concatenate(ins, axis=1)]
        return out

    base, other_base = NQ * y, NQ * (1 - y)

    late_cv = cvt[...].T.astype(BF16)

    def f_of(want_q):
        sel = jnp.where(iota((L, L), 1) == want_q, 1.0, 0.0).astype(BF16)
        return dot(sel, late_cv)

    kf = iota((L, L), 0)
    h1 = QC * N1
    kt = kf - 2 * h1
    ks, ku = kt >> 4, kt & 7
    kq = jnp.where(ks == 0, SMALL[0][0] + (ku & 1), jnp.where(ks == 1, SMALL[1][0], SMALL[2][0]) + (ku & 3))
    f1_mat[...] = f_of(jnp.where(kt < 0, jnp.where(kf < h1, base + kf, other_base + kf - h1),
                       jnp.where((kt & 8) == 0, base, other_base) + kq))
    f2 = f_of(jnp.where((kf & 8) == 0, base, other_base) + h1 + (kf & 7))
    for i in range(8):
        mine_f = jnp.where((kf >> 4) == i, f2, 0.0).astype(BF16)
        for k in range(3):
            f2_mat[cols(k), cols(i)] = mine_f

    for m in range(3):
        for r in range(3):
            out_s(m, r).wait_recv()
    lax.fori_loop(0, N1, arrive, 0)

    def turned(w):
        return parts(jnp.concatenate([w[:, cols(c)].T for c in range(3)], axis=0))

    for i in range(8):
        w = jnp.concatenate(w_rows(i, range(N1)) + small_rows(i), axis=0)
        here = (kt < 0) | ((ks == 0) & (ku >> 1 == i % 4)) | ((ks > 0) & (ku >> 2 == i % 2))
        f1 = jnp.where(here, f1_mat[...], 0.0).astype(BF16)
        v_acc[i] = dot(turned(w), jnp.concatenate([f1] * 3, axis=0))

    for m in range(3):
        for r in range(4):
            d2d_s(m, r).wait_send()
        for r in range(3):
            out_s(m, r).wait_send()

    def drain(n, carry):
        for r in range(4):
            d2d(n, r).wait_send()

        def wait(rows):
            for r in range(3):
                out_m(n, r, rows).wait_send()

        by_core(wait)
        return carry

    lax.fori_loop(0, N1, drain, 0)
    arrive(N1, 0)

    def back(i):
        return pltpu.make_async_remote_copy(
            src_ref=v_fin.at[i], dst_ref=out_ref.at[core * 8 + i], send_sem=v_send.at[i],
            recv_sem=v_recv.at[i], device_id=partner, device_id_type=MESH)

    def back_in(i):
        return pltpu.make_async_remote_copy(
            src_ref=v_fin.at[i], dst_ref=out_ref.at[(1 - core) * 8 + i], send_sem=v_send.at[i],
            recv_sem=v_recv.at[i], device_id=partner, device_id_type=MESH)

    rows = [v for i in range(7) for v in w_rows(i, range(N1, NM))]
    rows += [jnp.where(core == 0, v, 0.0) for v in w_rows(7, range(N1, NM))]
    w = turned(jnp.concatenate(rows, axis=0))
    vs = [dot(w, f2_mat[:, cols(2 * g, 2)]) for g in range(4)]
    for g, v in enumerate(vs):
        for i in (2 * g, 2 * g + 1):
            vi = v_acc[i] + v[:, cols(i % 2)]
            low, high = vi[0:NC, 0:NV], vi[CH:CH + NC, 0:NV]
            v_fin[i] = jnp.where(core == 0, high, low)
            if i < 7:
                out_ref[core * 8 + i] = jnp.where(core == 0, low, high)
            else:
                @pl.when(core == 0)
                def _():
                    out_ref[7] = low
        if g % 2:
            for i in range(2 * g - 2, 2 * g + 2):
                if i < 7:
                    back(i).start()
                else:
                    @pl.when(core == 0)
                    def _():
                        back(7).start()

    for i in range(7):
        back(i).wait_send()
        back_in(i).wait_recv()

    @pl.when(core == 0)
    def _():
        back(7).wait_send()

    @pl.when(core == 1)
    def _():
        back_in(7).wait_recv()
    drain(NM - 1, 0)


def solution(mesh):
    def local_program(ints_blk, c_occ, c_vir):
        v = pl.pallas_call(
            kernel,
            out_shape=pltpu.VMEM((NO, NC, NV), F32),
            in_specs=[pl.BlockSpec(memory_space=pl.ANY)] * 3,
            out_specs=pl.BlockSpec(memory_space=pltpu.VMEM),
            scratch_shapes=[
                pltpu.VMEM((2, 4, NP, 2, NB, NB), BF16),
                pltpu.VMEM((NP, 2, NB, NB), BF16),
                pltpu.VMEM((NP, 4, NB, NB), BF16),
                pltpu.VMEM((NP, 4, NB, NB), BF16),
                pltpu.VMEM((NO, NB), BF16),
                pltpu.VMEM((NV, NB), BF16),
                pltpu.VMEM((16, L), F32),
                pltpu.VMEM((L, L), F32),
                pltpu.VMEM((L, 1024), BF16),
                pltpu.VMEM((4, 512, 256), BF16),
                pltpu.VMEM((2, 512, 256), BF16),
                pltpu.VMEM((L, 256), BF16),
                pltpu.VMEM((64, 256), BF16),
                pltpu.VMEM((32, 256), BF16),
                pltpu.VMEM((L, L), F32),
                pltpu.VMEM((384, 1024), BF16),
                pltpu.VMEM((NO, 256, L), BF16),
                pltpu.VMEM((6, 256, 256), BF16),
                pltpu.VMEM((NM, 4, RW, L), F32),
                pltpu.VMEM((3, 4, 96, L), F32),
                pltpu.VMEM((NM, 4, RW, L), F32),
                pltpu.VMEM((3, 4, 96, L), F32),
                pltpu.VMEM((NM, 4, RW, L), F32),
                pltpu.VMEM((3, 4, 96, L), F32),
                pltpu.VMEM((3, NM, RW, L), F32),
                pltpu.VMEM((3, 3, 96, L), F32),
                pltpu.VMEM((8, LW, L), F32),
                pltpu.VMEM((8, NC, NV), F32),
                pltpu.SemaphoreType.DMA((2, 4)),
                pltpu.SemaphoreType.DMA((3,)),
                pltpu.SemaphoreType.DMA((2,)),
                pltpu.SemaphoreType.DMA((NM + 3, 4)),
                pltpu.SemaphoreType.DMA((NM + 3, 4)),
                pltpu.SemaphoreType.DMA((NM + 3, 3)),
                pltpu.SemaphoreType.DMA((NM + 3, 3)),
                pltpu.SemaphoreType.DMA((8,)),
                pltpu.SemaphoreType.DMA((8,)),
            ],
            compiler_params=pltpu.CompilerParams(
                collective_id=0, has_side_effects=True, vmem_limit_bytes=60 * 1024 * 1024),
            name='four_index',
        )(ints_blk, c_occ.T, c_vir.T)
        return v.transpose(0, 2, 1)

    return jax.shard_map(
        local_program,
        mesh=mesh,
        in_specs=(P(('frag', 'dev'), 'dev2', None, None), P('frag', None), P('frag', None)),
        out_specs=P(None, None, ('frag', 'dev2', 'dev')),
        check_vma=False,
    )
```

```python
import jax
import jax.numpy as jnp
from jax import lax
from jax.experimental import pallas as pl
from jax.experimental.pallas import tpu as pltpu
from jax.sharding import PartitionSpec as P

MESH = pl.DeviceIdType.MESH
F32, BF16, I32 = jnp.float32, jnp.bfloat16, jnp.int32

NP, NQ, NB = 29, 58, 116
NO, NV = 15, 96
QC = 8
NM = 6
SMALL = ((48, 2), (50, 4), (54, 4))
PG = 4
L = 128
LW = 3 * L
SP = 108
PW, NS = L - SP, 6
NC, CH = 180, 184
RW = 184
ROWS = (RW, RW - 24)
N1 = NM - 1


def place_of(i, c):
    return 3 * i - 1 + c if i else c


def cols(k, n=1):
    return slice(L * k, L * (k + n))


def rows8(k, n=1):
    return slice(8 * k, 8 * (k + n))


def iota(shape, dim):
    return lax.broadcasted_iota(I32, shape, dim)


def dot(a, b):
    return jnp.dot(a, b, preferred_element_type=F32)


def parts(w):
    hi = w.astype(BF16)
    rest = w - hi.astype(F32)
    mid = rest.astype(BF16)
    lo = (rest - mid.astype(F32)).astype(BF16)
    return jnp.concatenate([hi, mid, lo], axis=1)


def kernel(a_hbm, cot_hbm, cvt_hbm, out_ref, abuf, as0, as1, as2, cot_in, cvt_in, cot, cvt, s_mat, b_mat, bs_mat, l8, l4, l2,
           f1_mat, f2_mat, x_buf, h_buf, own_m, own_s, ps_m, ps_s, pr_m, pr_s, rb_m, rb_s, v_acc, v_fin,
           a_sem, as_sem, c_sem, d_send, d_recv, ds_sem, r_send, r_recv, rs_send, rs_recv, v_sem):
    y = lax.axis_index('dev2')
    dev = lax.axis_index('dev')
    core = lax.rem(dev, 2)
    x = dev // 2
    partner = (0, y, x * 2 + (1 - core))
    peers = [(0, 1 - y, (1 - x) * 2 + core), (0, y, (1 - x) * 2 + core), (0, 1 - y, x * 2 + core)]
    chip = [2 * (1 - y) + (1 - x), 2 * y + (1 - x), 2 * (1 - y) + x, 2 * y + x]

    def a_copy(n, half, slot):
        return pltpu.make_async_copy(
            a_hbm.at[:, pl.ds(n * QC + 4 * half, 4)], abuf.at[slot, half], a_sem.at[slot, half])

    def all_of(ref, sem):
        return pltpu.make_async_remote_copy(
            src_ref=ref, dst_ref=ref, send_sem=sem, recv_sem=sem, device_id=partner, device_id_type=MESH)

    small = [pltpu.make_async_copy(cot_hbm, cot_in, c_sem.at[0]), pltpu.make_async_copy(cvt_hbm, cvt_in, c_sem.at[1])]
    a_small = (as0, as1, as2)
    small_copy = [pltpu.make_async_copy(a_hbm.at[:, pl.ds(q, nq)], a_small[m], as_sem.at[m])
                  for m, (q, nq) in enumerate(SMALL)]
    for c in small:
        c.start()
    small_copy[0].start()
    small_copy[1].start()

    barrier = pltpu.get_barrier_semaphore()
    for other in [partner] + peers:
        pl.semaphore_signal(barrier, inc=1, device_id=other, device_id_type=MESH)

    cot[...] = jnp.zeros_like(cot)
    cvt[...] = jnp.zeros_like(cvt)
    for c in small:
        c.wait()
    cot[0:NO, 0:NB] = cot_in[...].astype(F32)
    cvt[0:NV, 0:NB] = cvt_in[...].astype(F32)
    sub = iota((8, L), 0)
    zero = jnp.zeros((8, L), F32)
    for jj in range(8):
        for p in range(8):
            two = [jnp.where(sub == p, cot[j:j + 1, :], zero) for j in (2 * jj, 2 * jj + 1)]
            s_mat[rows8(2 * jj, 2), cols(p)] = jnp.concatenate(two, axis=0).astype(BF16)
    cv = cvt[...].T.astype(BF16)
    first = [(15 * c) // 4 for c in chip]
    first_s = [4 * c + 2 - c // 3 for c in chip]
    lane, row = iota((L, 256), 1), iota((L, 256), 0)
    want = jnp.where(lane < NC, lane, jnp.where(lane < CH, -100000, lane - 4)) - row
    lane_s, row_s = iota((L, L), 1), iota((L, L), 0)
    want_s = jnp.where(lane_s < SP, lane_s + 252, -100000) - row_s
    bs_mat[...] = jnp.zeros_like(bs_mat)
    for r in range(4):
        for j in range(4):
            place = jnp.where(want == 96 * (first[r] + j) - 360 * chip[r], 1.0, 0.0).astype(BF16)
            b_mat[r, cols(j), :] = dot(cv, place).astype(BF16)
        for j in range(2):
            place = jnp.where(want_s == 96 * (first_s[r] + j) - 360 * chip[r], 1.0, 0.0).astype(BF16)
            h = r % 2
            bs_mat[r // 2, cols(2 * h + j), cols(h)] = dot(cv, place).astype(BF16)
    low, high = cot[0:8, :], cot[8:16, :]
    mine = jnp.concatenate([jnp.where(core == 0, low, high), jnp.where(core == 0, high, low)], axis=0)
    kk = iota((L, 256), 1)
    ploc = ((kk >> 4) & 3) * 8 + (kk & 7)
    pick = (iota((L, 256), 0) == ploc + NP * dev) & (ploc < NP)
    l0 = dot(mine.astype(BF16), jnp.where(pick, 1.0, 0.0).astype(BF16)).astype(BF16)
    def build_l(l_mat, sh):
        nq = 1 << sh
        rows = 16 * nq
        e = jnp.where((iota((rows, 16), 0) >> sh) == iota((rows, 16), 1), 1.0, 0.0).astype(BF16)
        row, k2 = iota((rows, 256), 0), iota((rows, 256), 1)
        here = (k2 >> 6) * 2 + ((k2 >> 3) & 1) == (row & (nq - 1))
        l_mat[...] = jnp.where(here, dot(e, l0), 0.0).astype(BF16)

    build_l(l2, 1)

    def step1(tile_of, qp):
        zl = jnp.zeros((NB, L - NB), BF16)
        zs = jnp.zeros((L - NB, L), BF16)

        def tile(p, q):
            t = jnp.concatenate([tile_of(p, q), zl], axis=1)
            return jnp.concatenate([t, zs], axis=0)

        for pg in range(PG):
            ps = range(8 * pg, min(NP, 8 * pg + 8))
            rhs = jnp.concatenate([jnp.concatenate([tile(p, 0), tile(p, 1)], axis=1) for p in ps], axis=0)
            t = dot(s_mat[rows8(0, NO), cols(0, len(ps))], rhs)
            r = rows8(8 * qp + 2 * pg, 2)
            for j in range(NO):
                two = jnp.concatenate([t[rows8(j), cols(k)] for k in range(2)], axis=0)
                x_buf[j, r, :] = two.astype(BF16)

    def stage_h(rows, k):
        p, t = k // 3, k % 3
        if t < 2:
            js, weights = [first[2 * p + t] + j for j in range(4)], b_mat[2 * p + t]
        else:
            js, weights = [first_s[r] + j for r in (2 * p, 2 * p + 1) for j in range(2)], bs_mat[p]
        lhs = jnp.concatenate([x_buf[j, 0:rows, :] for j in js], axis=1)
        h_buf[k, 0:rows, :] = dot(lhs, weights).astype(BF16)

    def stage_w(rows, lhs, p):
        w = [dot(lhs, h_buf[3 * p + t, 0:rows, :]) for t in range(3)]
        return [jnp.concatenate([w[k], w[2][:, cols(k)]], axis=1) for k in range(2)]

    lane8 = iota((8, L), 1)
    spare = lane8 >= SP

    def pack(ref, w):
        col = [[w[rows8(i), cols(c)] for c in range(3)] for i in range(8)]
        for i in range(8):
            for c in range(3 if i else 2):
                v = col[i][c]
                if c == 2 and i <= NS:
                    v = jnp.where(spare, pltpu.roll(col[0][c], SP - PW * (i - 1), 1), v)
                ref[rows8(place_of(i, c)), :] = v

    def d2d(n, r):
        return pltpu.make_async_remote_copy(
            src_ref=ps_m.at[n, r], dst_ref=pr_m.at[n, r], send_sem=d_send, recv_sem=d_recv.at[n, r // 2],
            device_id=partner, device_id_type=MESH)

    def d2d_s(m, r):
        part = pl.ds(0, 24 * SMALL[m][1])
        return pltpu.make_async_remote_copy(
            src_ref=ps_s.at[m, r, part], dst_ref=pr_s.at[m, r, part], send_sem=ds_sem.at[0, m],
            recv_sem=ds_sem.at[1, m], device_id=partner, device_id_type=MESH)

    def out_m(n, r, rows):
        return pltpu.make_async_remote_copy(
            src_ref=own_m.at[n, r, pl.ds(0, rows)], dst_ref=rb_m.at[r, n, pl.ds(0, rows)],
            send_sem=r_send, recv_sem=r_recv.at[n // N1], device_id=peers[r], device_id_type=MESH)

    def out_s(m, r):
        part = pl.ds(0, 24 * SMALL[m][1])
        return pltpu.make_async_remote_copy(
            src_ref=own_s.at[m, r, part], dst_ref=rb_s.at[r, m, part], send_sem=rs_send.at[m],
            recv_sem=rs_recv.at[m], device_id=peers[r], device_id_type=MESH)

    def by_core(f):
        for k in range(2):
            @pl.when(core == k)
            def _(k=k):
                f(ROWS[k])

    def finish_m(n, rs):
        all_of(pr_m.at[n, pl.ds(rs[0], 2)], d_recv.at[n, rs[0] // 2]).wait_recv()
        for r in rs:
            own_m[n, r] = own_m[n, r] + pr_m[n, r]

        def go(rows):
            for r in rs:
                if r < 3:
                    out_m(n, r, rows).start()

        by_core(go)

    def finish_s(m):
        part = rows8(0, 3 * SMALL[m][1])
        all_of(pr_s.at[m, :, pl.ds(0, 24 * SMALL[m][1])], ds_sem.at[1, m]).wait_recv()
        for r in range(4):
            own_s[m, r, part, :] = own_s[m, r, part, :] + pr_s[m, r, part, :]
            if r < 3:
                out_s(m, r).start()

    small_copy[2].start()
    for m, (l_mat, a_ref) in enumerate(zip((l2, l4, l4), a_small)):
        nq = SMALL[m][1]
        small_copy[m].wait()
        for qp in range(nq // 2):
            step1(lambda p, q: a_ref[p, 2 * qp + q], qp)
        if m == 0:
            pl.semaphore_wait(barrier, 4)
        else:
            finish_s(m - 1)
        rows = 32 * nq
        for k in range(6):
            stage_h(rows, k)
        for p in range(2):
            pair = (2 * p, 2 * p + 1)
            for r, w in zip(pair, stage_w(rows, l_mat[:, 0:rows], p)):
                for c in range(3):
                    own_s[m, r, rows8(c * nq, nq), :] = w[rows8(0, nq), cols(c)]
                    ps_s[m, r, rows8(c * nq, nq), :] = w[rows8(nq, nq), cols(c)]
            for r in pair:
                d2d_s(m, r).start()
        if m < 2:
            for half in range(2):
                a_copy(m, half, m).start()
        if m == 0:
            build_l(l4, 2)
            build_l(l8, 3)

    def body(n, carry):
        slot = lax.rem(n, 2)
        for half in range(2):
            qps = (2 * half, 2 * half + 1)
            a_copy(n, half, slot).wait()
            for qp in qps:
                step1(lambda p, q: abuf[slot, half, p, 2 * (qp % 2) + q], qp)

            @pl.when(n + 2 < NM)
            def _():
                a_copy(n + 2, half, slot).start()

            if half == 0:
                @pl.when(n == 0)
                def _():
                    finish_s(2)

            @pl.when(n > 0)
            def _():
                finish_m(n - 1, qps)

        for k in range(6):
            stage_h(256, k)
        for p in range(2):
            pair = (2 * p, 2 * p + 1)
            for r, w in zip(pair, stage_w(256, l8[...], p)):
                pack(own_m.at[n, r], w[rows8(0, 8)])
                pack(ps_m.at[n, r], w[rows8(8, 8)])
            for r in pair:
                d2d(n, r).start()
        return carry

    lax.fori_loop(0, NM, body, 0)
    finish_m(NM - 1, (0, 1))
    finish_m(NM - 1, (2, 3))

    def w_rows(i, ns):
        def block(n, b):
            near = own_m[n, 3, rows8(b), :] + rb_m[1, n, rows8(b), :]
            far = rb_m[2, n, rows8(b), :] + rb_m[0, n, rows8(b), :]
            return near, far

        both = []
        for n in ns:
            parts_of = [block(n, place_of(i, c)) for c in range(3 if i else 2)]
            if not i:
                s = [jnp.zeros((8, L), F32)] * 2
                for m in range(NS):
                    piece = block(n, place_of(m + 1, 2))
                    here = (lane8 >= PW * m) & (lane8 < min(SP, PW * m + PW))
                    s = [jnp.where(here, pltpu.roll(v, PW * m + PW, 1), o) for v, o in zip(piece, s)]
                parts_of.append(s)
            both.append([jnp.concatenate(list(c), axis=1) for c in zip(*parts_of)])
        return [b[0] for b in both] + [b[1] for b in both]

    def small_rows(i):
        out = []
        for m, (_, nq) in enumerate(SMALL):
            own, ins = [], []
            for c in range(3):
                t = rows8(c * nq + (i * nq) // 8)
                own.append(own_s[m, 3, t, :] + rb_s[1, m, t, :])
                ins.append(rb_s[2, m, t, :] + rb_s[0, m, t, :])
            out += [jnp.concatenate(own, axis=1), jnp.concatenate(ins, axis=1)]
        return out

    base, other_base = NQ * y, NQ * (1 - y)

    late_cv = cvt[...].T.astype(BF16)

    def f_of(want_q):
        sel = jnp.where(iota((L, L), 1) == want_q, 1.0, 0.0).astype(BF16)
        return dot(sel, late_cv)

    kf = iota((L, L), 0)
    h1 = QC * N1
    kt = kf - 2 * h1
    ks, ku = kt >> 4, kt & 7
    kq = jnp.where(ks == 0, SMALL[0][0] + (ku & 1), jnp.where(ks == 1, SMALL[1][0], SMALL[2][0]) + (ku & 3))
    f1_mat[...] = f_of(jnp.where(kt < 0, jnp.where(kf < h1, base + kf, other_base + kf - h1),
                       jnp.where((kt & 8) == 0, base, other_base) + kq))
    f2 = f_of(jnp.where((kf & 8) == 0, base, other_base) + h1 + (kf & 7))
    for i in range(8):
        mine_f = jnp.where((kf >> 4) == i, f2, 0.0).astype(BF16)
        for k in range(3):
            f2_mat[cols(k), cols(i)] = mine_f

    for m, (_, nq) in enumerate(SMALL):
        all_of(rb_s.at[:, m, pl.ds(0, 24 * nq)], rs_recv.at[m]).wait_recv()
    by_core(lambda rows: all_of(rb_m.at[:, pl.ds(0, N1), pl.ds(0, rows)], r_recv.at[0]).wait_recv())

    def turned(w):
        return parts(jnp.concatenate([w[:, cols(c)].T for c in range(3)], axis=0))

    for i in range(8):
        w = jnp.concatenate(w_rows(i, range(N1)) + small_rows(i), axis=0)
        here = (kt < 0) | ((ks == 0) & (ku >> 1 == i % 4)) | ((ks > 0) & (ku >> 2 == i % 2))
        f1 = jnp.where(here, f1_mat[...], 0.0).astype(BF16)
        v_acc[i] = dot(turned(w), jnp.concatenate([f1] * 3, axis=0))

    for m, (_, nq) in enumerate(SMALL):
        all_of(ps_s.at[m, :, pl.ds(0, 24 * nq)], ds_sem.at[0, m]).wait_send()
        all_of(own_s.at[m, pl.ds(0, 3), pl.ds(0, 24 * nq)], rs_send.at[m]).wait_send()
    all_of(ps_m, d_send).wait_send()
    by_core(lambda rows: all_of(rb_m.at[:, N1, pl.ds(0, rows)], r_recv.at[1]).wait_recv())

    def back(i):
        return pltpu.make_async_remote_copy(
            src_ref=v_fin.at[i], dst_ref=out_ref.at[core * 8 + i], send_sem=v_sem.at[0], recv_sem=v_sem.at[1],
            device_id=partner, device_id_type=MESH)

    rows = [v for i in range(7) for v in w_rows(i, range(N1, NM))]
    rows += [jnp.where(core == 0, v, 0.0) for v in w_rows(7, range(N1, NM))]
    w = turned(jnp.concatenate(rows, axis=0))
    vs = [dot(w, f2_mat[:, cols(2 * g, 2)]) for g in range(4)]
    for g, v in enumerate(vs):
        for i in (2 * g, 2 * g + 1):
            vi = v_acc[i] + v[:, cols(i % 2)]
            low, high = vi[0:NC, 0:NV], vi[CH:CH + NC, 0:NV]
            v_fin[i] = jnp.where(core == 0, high, low)
            if i < 7:
                out_ref[core * 8 + i] = jnp.where(core == 0, low, high)
            else:
                @pl.when(core == 0)
                def _():
                    out_ref[7] = low
        if g % 2:
            for i in range(2 * g - 2, 2 * g + 2):
                if i < 7:
                    back(i).start()
                else:
                    @pl.when(core == 0)
                    def _():
                        back(7).start()

    def close(rows):
        n = 8 if rows == RW else 7
        all_of(own_m.at[:, pl.ds(0, 3), pl.ds(0, rows)], r_send).wait_send()
        all_of(v_fin.at[pl.ds(0, n)], v_sem.at[0]).wait_send()
        all_of(out_ref.at[pl.ds(8 if n == 8 else 0, NO - n)], v_sem.at[1]).wait_recv()

    by_core(close)


def solution(mesh):
    def local_program(ints_blk, c_occ, c_vir):
        v = pl.pallas_call(
            kernel,
            out_shape=pltpu.VMEM((NO, NC, NV), F32),
            in_specs=[pl.BlockSpec(memory_space=pl.ANY)] * 3,
            out_specs=pl.BlockSpec(memory_space=pltpu.VMEM),
            scratch_shapes=[
                pltpu.VMEM((2, 2, NP, 4, NB, NB), BF16),
                pltpu.VMEM((NP, 2, NB, NB), BF16),
                pltpu.VMEM((NP, 4, NB, NB), BF16),
                pltpu.VMEM((NP, 4, NB, NB), BF16),
                pltpu.VMEM((NO, NB), BF16),
                pltpu.VMEM((NV, NB), BF16),
                pltpu.VMEM((16, L), F32),
                pltpu.VMEM((L, L), F32),
                pltpu.VMEM((L, 1024), BF16),
                pltpu.VMEM((4, 512, 256), BF16),
                pltpu.VMEM((2, 512, 256), BF16),
                pltpu.VMEM((L, 256), BF16),
                pltpu.VMEM((64, 256), BF16),
                pltpu.VMEM((32, 256), BF16),
                pltpu.VMEM((L, L), F32),
                pltpu.VMEM((384, 1024), BF16),
                pltpu.VMEM((NO, 256, L), BF16),
                pltpu.VMEM((6, 256, 256), BF16),
                pltpu.VMEM((NM, 4, RW, L), F32),
                pltpu.VMEM((3, 4, 96, L), F32),
                pltpu.VMEM((NM, 4, RW, L), F32),
                pltpu.VMEM((3, 4, 96, L), F32),
                pltpu.VMEM((NM, 4, RW, L), F32),
                pltpu.VMEM((3, 4, 96, L), F32),
                pltpu.VMEM((3, NM, RW, L), F32),
                pltpu.VMEM((3, 3, 96, L), F32),
                pltpu.VMEM((8, LW, L), F32),
                pltpu.VMEM((8, NC, NV), F32),
                pltpu.SemaphoreType.DMA((2, 2)),
                pltpu.SemaphoreType.DMA((3,)),
                pltpu.SemaphoreType.DMA((2,)),
                pltpu.SemaphoreType.DMA,
                pltpu.SemaphoreType.DMA((NM, 2)),
                pltpu.SemaphoreType.DMA((2, 3)),
                pltpu.SemaphoreType.DMA,
                pltpu.SemaphoreType.DMA((2,)),
                pltpu.SemaphoreType.DMA((3,)),
                pltpu.SemaphoreType.DMA((3,)),
                pltpu.SemaphoreType.DMA((2,)),
            ],
            compiler_params=pltpu.CompilerParams(
                collective_id=0, has_side_effects=True, vmem_limit_bytes=60 * 1024 * 1024),
            name='four_index',
        )(ints_blk, c_occ.T, c_vir.T)
        return v.transpose(0, 2, 1)

    return jax.shard_map(
        local_program,
        mesh=mesh,
        in_specs=(P(('frag', 'dev'), 'dev2', None, None), P('frag', None), P('frag', None)),
        out_specs=P(None, None, ('frag', 'dev2', 'dev')),
        check_vma=False,
    )
```

```python
import jax
import jax.numpy as jnp
from jax import lax
from jax.experimental import pallas as pl
from jax.experimental.pallas import tpu as pltpu
from jax.sharding import PartitionSpec as P

MESH = pl.DeviceIdType.MESH
F32, BF16, I32 = jnp.float32, jnp.bfloat16, jnp.int32

NP, NQ, NB = 29, 58, 116
NO, NV = 15, 96
QC = 8
NM = 6
SMALL = ((48, 2), (50, 4), (54, 4))
PG = 4
L = 128
LW = 3 * L
SP = 108
PW, NS = L - SP, 6
NC, CH = 180, 184
RW = 184
ROWS = (RW, RW - 24)
N1 = NM - 1


def place_of(i, c):
    return 3 * i - 1 + c if i else c


def cols(k, n=1):
    return slice(L * k, L * (k + n))


def rows8(k, n=1):
    return slice(8 * k, 8 * (k + n))


def iota(shape, dim):
    return lax.broadcasted_iota(I32, shape, dim)


def dot(a, b):
    return jnp.dot(a, b, preferred_element_type=F32)


def parts(w):
    hi = w.astype(BF16)
    rest = w - hi.astype(F32)
    mid = rest.astype(BF16)
    lo = (rest - mid.astype(F32)).astype(BF16)
    return jnp.concatenate([hi, mid, lo], axis=1)


def kernel(a_hbm, cot_hbm, cvt_hbm, out_ref, abuf, as0, as1, as2, cot_in, cvt_in, cot, cvt, s_mat, b_mat, bs_mat, l8, l4, l2,
           f1_mat, f2_mat, x_buf, h_buf, own_m, own_s, ps_m, ps_s, pr_m, pr_s, rb_m, rb_s, v_acc, v_in, w2, w2_in,
           a_sem, as_sem, c_sem, d_send, d_recv, ds_send, ds_recv, r_send, r_recv, rs_send, rs_recv, v_sem, w_sem):
    y = lax.axis_index('dev2')
    dev = lax.axis_index('dev')
    core = lax.rem(dev, 2)
    x = dev // 2
    partner = (0, y, x * 2 + (1 - core))
    peers = [(0, 1 - y, (1 - x) * 2 + core), (0, y, (1 - x) * 2 + core), (0, 1 - y, x * 2 + core)]
    chip = [2 * (1 - y) + (1 - x), 2 * y + (1 - x), 2 * (1 - y) + x, 2 * y + x]

    def a_copy(n, half, slot):
        return pltpu.make_async_copy(
            a_hbm.at[:, pl.ds(n * QC + 4 * half, 4)], abuf.at[slot, half], a_sem.at[slot, half])

    def all_of(ref, sem):
        return pltpu.make_async_remote_copy(
            src_ref=ref, dst_ref=ref, send_sem=sem, recv_sem=sem, device_id=partner, device_id_type=MESH)

    small = [pltpu.make_async_copy(cot_hbm, cot_in, c_sem.at[0]), pltpu.make_async_copy(cvt_hbm, cvt_in, c_sem.at[1])]
    a_small = (as0, as1, as2)
    small_copy = [[pltpu.make_async_copy(a_hbm.at[:, pl.ds(q + 2 * k, 2)], a_small[m].at[:, pl.ds(2 * k, 2)],
                                         as_sem.at[m, k]) for k in range(nq // 2)]
                  for m, (q, nq) in enumerate(SMALL)]
    for c in small:
        c.start()
    small_copy[0][0].start()

    barrier = pltpu.get_barrier_semaphore()
    for other in [partner] + peers:
        pl.semaphore_signal(barrier, inc=1, device_id=other, device_id_type=MESH)

    cot[...] = jnp.zeros_like(cot)
    cvt[...] = jnp.zeros_like(cvt)
    for c in small:
        c.wait()
    for c in small_copy[1]:
        c.start()
    cot[0:NO, 0:NB] = cot_in[...].astype(F32)
    cvt[0:NV, 0:NB] = cvt_in[...].astype(F32)
    sub = iota((8, L), 0)
    zero = jnp.zeros((8, L), F32)
    for jj in range(8):
        for p in range(8):
            two = [jnp.where(sub == p, cot[j:j + 1, :], zero) for j in (2 * jj, 2 * jj + 1)]
            s_mat[rows8(2 * jj, 2), cols(p)] = jnp.concatenate(two, axis=0).astype(BF16)
    cv = cvt[...].T.astype(BF16)
    first = [(15 * c) // 4 for c in chip]
    first_s = [4 * c + 2 - c // 3 for c in chip]
    lane, row = iota((L, 256), 1), iota((L, 256), 0)
    want = jnp.where(lane < NC, lane, jnp.where(lane < CH, -100000, lane - 4)) - row
    lane_s, row_s = iota((L, L), 1), iota((L, L), 0)
    want_s = jnp.where(lane_s < SP, lane_s + 252, -100000) - row_s
    bs_mat[...] = jnp.zeros_like(bs_mat)
    for r in range(4):
        for j in range(4):
            place = jnp.where(want == 96 * (first[r] + j) - 360 * chip[r], 1.0, 0.0).astype(BF16)
            b_mat[r, cols(j), :] = dot(cv, place).astype(BF16)
        for j in range(2):
            place = jnp.where(want_s == 96 * (first_s[r] + j) - 360 * chip[r], 1.0, 0.0).astype(BF16)
            h = r % 2
            bs_mat[r // 2, cols(2 * h + j), cols(h)] = dot(cv, place).astype(BF16)
    low, high = cot[0:8, :], cot[8:16, :]
    mine = jnp.concatenate([jnp.where(core == 0, low, high), jnp.where(core == 0, high, low)], axis=0)
    kk = iota((L, 256), 1)
    ploc = ((kk >> 4) & 3) * 8 + (kk & 7)
    pick = (iota((L, 256), 0) == ploc + NP * dev) & (ploc < NP)
    l0 = dot(mine.astype(BF16), jnp.where(pick, 1.0, 0.0).astype(BF16)).astype(BF16)
    def build_l(l_mat, sh):
        nq = 1 << sh
        rows = 16 * nq
        e = jnp.where((iota((rows, 16), 0) >> sh) == iota((rows, 16), 1), 1.0, 0.0).astype(BF16)
        row, k2 = iota((rows, 256), 0), iota((rows, 256), 1)
        here = (k2 >> 6) * 2 + ((k2 >> 3) & 1) == (row & (nq - 1))
        l_mat[...] = jnp.where(here, dot(e, l0), 0.0).astype(BF16)

    build_l(l2, 1)

    def step1(tile_of, qp):
        zl = jnp.zeros((NB, L - NB), BF16)
        zs = jnp.zeros((L - NB, L), BF16)

        def tile(p, q):
            t = jnp.concatenate([tile_of(p, q), zl], axis=1)
            return jnp.concatenate([t, zs], axis=0)

        for pg in range(PG):
            ps = range(8 * pg, min(NP, 8 * pg + 8))
            rhs = jnp.concatenate([jnp.concatenate([tile(p, 0), tile(p, 1)], axis=1) for p in ps], axis=0)
            t = dot(s_mat[rows8(0, NO), cols(0, len(ps))], rhs)
            r = rows8(8 * qp + 2 * pg, 2)
            for j in range(NO):
                two = jnp.concatenate([t[rows8(j), cols(k)] for k in range(2)], axis=0)
                x_buf[j, r, :] = two.astype(BF16)

    def stage_h(rows, k):
        p, t = k // 3, k % 3
        if t < 2:
            js, weights = [first[2 * p + t] + j for j in range(4)], b_mat[2 * p + t]
        else:
            js, weights = [first_s[r] + j for r in (2 * p, 2 * p + 1) for j in range(2)], bs_mat[p]
        lhs = jnp.concatenate([x_buf[j, 0:rows, :] for j in js], axis=1)
        h_buf[k, 0:rows, :] = dot(lhs, weights).astype(BF16)

    def stage_w(rows, lhs, p):
        w = [dot(lhs, h_buf[3 * p + t, 0:rows, :]) for t in range(3)]
        return [jnp.concatenate([w[k], w[2][:, cols(k)]], axis=1) for k in range(2)]

    lane8 = iota((8, L), 1)
    spare = lane8 >= SP

    def pack(ref, w):
        col = [[w[rows8(i), cols(c)] for c in range(3)] for i in range(8)]
        for i in range(8):
            for c in range(3 if i else 2):
                v = col[i][c]
                if c == 2 and i <= NS:
                    v = jnp.where(spare, pltpu.roll(col[0][c], SP - PW * (i - 1), 1), v)
                ref[rows8(place_of(i, c)), :] = v

    def d2d(n, r):
        return pltpu.make_async_remote_copy(
            src_ref=ps_m.at[n, r], dst_ref=pr_m.at[n, r], send_sem=d_send, recv_sem=d_recv.at[n, r // 2],
            device_id=partner, device_id_type=MESH)

    def d2d_s(m, r):
        part = pl.ds(0, 24 * SMALL[m][1])
        return pltpu.make_async_remote_copy(
            src_ref=ps_s.at[m, r, part], dst_ref=pr_s.at[m, r, part], send_sem=ds_send.at[m],
            recv_sem=ds_recv.at[m, r // 2], device_id=partner, device_id_type=MESH)

    def out_m(n, r, rows):
        return pltpu.make_async_remote_copy(
            src_ref=own_m.at[n, r, pl.ds(0, rows)], dst_ref=rb_m.at[r, n, pl.ds(0, rows)],
            send_sem=r_send, recv_sem=r_recv.at[n // N1], device_id=peers[r], device_id_type=MESH)

    def out_s(m, r):
        part = pl.ds(0, 24 * SMALL[m][1])
        return pltpu.make_async_remote_copy(
            src_ref=own_s.at[m, r, part], dst_ref=rb_s.at[r, m, part], send_sem=rs_send.at[m],
            recv_sem=rs_recv.at[m], device_id=peers[r], device_id_type=MESH)

    def by_core(f):
        for k in range(2):
            @pl.when(core == k)
            def _(k=k):
                f(ROWS[k])

    def finish_m(n, rs):
        all_of(pr_m.at[n, pl.ds(rs[0], 2)], d_recv.at[n, rs[0] // 2]).wait_recv()
        for r in rs:
            own_m[n, r] = own_m[n, r] + pr_m[n, r]

        def go(rows):
            for r in rs:
                if r < 3:
                    out_m(n, r, rows).start()

        by_core(go)

    def finish_s(m):
        part = rows8(0, 3 * SMALL[m][1])
        for r in range(4):
            if r % 2 == 0:
                all_of(pr_s.at[m, pl.ds(r, 2), pl.ds(0, 24 * SMALL[m][1])], ds_recv.at[m, r // 2]).wait_recv()
            own_s[m, r, part, :] = own_s[m, r, part, :] + pr_s[m, r, part, :]
            if r < 3:
                out_s(m, r).start()

    for c in small_copy[2]:
        c.start()
    for m, (l_mat, a_ref) in enumerate(zip((l2, l4, l4), a_small)):
        nq = SMALL[m][1]
        for qp in range(nq // 2):
            small_copy[m][qp].wait()
            step1(lambda p, q: a_ref[p, 2 * qp + q], qp)
        if m == 0:
            pl.semaphore_wait(barrier, 4)
        else:
            finish_s(m - 1)
        rows = 32 * nq
        for k in range(6):
            stage_h(rows, k)
        for p in range(2):
            pair = (2 * p, 2 * p + 1)
            for r, w in zip(pair, stage_w(rows, l_mat[:, 0:rows], p)):
                for c in range(3):
                    own_s[m, r, rows8(c * nq, nq), :] = w[rows8(0, nq), cols(c)]
                    ps_s[m, r, rows8(c * nq, nq), :] = w[rows8(nq, nq), cols(c)]
            for r in pair:
                d2d_s(m, r).start()
        if m < 2:
            for half in range(2):
                a_copy(m, half, m).start()
        if m == 0:
            build_l(l4, 2)
            build_l(l8, 3)

    def body(n, carry):
        slot = lax.rem(n, 2)
        for half in range(2):
            qps = (2 * half, 2 * half + 1)
            a_copy(n, half, slot).wait()
            for qp in qps:
                step1(lambda p, q: abuf[slot, half, p, 2 * (qp % 2) + q], qp)

            @pl.when(n + 2 < NM)
            def _():
                a_copy(n + 2, half, slot).start()

            if half == 0:
                @pl.when(n == 0)
                def _():
                    finish_s(2)

            @pl.when(n > 0)
            def _():
                finish_m(n - 1, qps)

        for k in range(6):
            stage_h(256, k)
        for p in range(2):
            pair = (2 * p, 2 * p + 1)
            for r, w in zip(pair, stage_w(256, l8[...], p)):
                pack(own_m.at[n, r], w[rows8(0, 8)])
                pack(ps_m.at[n, r], w[rows8(8, 8)])
            for r in pair:
                d2d(n, r).start()
        return carry

    lax.fori_loop(0, NM, body, 0)
    finish_m(NM - 1, (0, 1))
    finish_m(NM - 1, (2, 3))

    def w_rows(i, ns):
        def block(n, b):
            near = own_m[n, 3, rows8(b), :] + rb_m[1, n, rows8(b), :]
            far = rb_m[2, n, rows8(b), :] + rb_m[0, n, rows8(b), :]
            return near, far

        both = []
        for n in ns:
            parts_of = [block(n, place_of(i, c)) for c in range(3 if i else 2)]
            if not i:
                s = [jnp.zeros((8, L), F32)] * 2
                for m in range(NS):
                    piece = block(n, place_of(m + 1, 2))
                    here = (lane8 >= PW * m) & (lane8 < min(SP, PW * m + PW))
                    s = [jnp.where(here, pltpu.roll(v, PW * m + PW, 1), o) for v, o in zip(piece, s)]
                parts_of.append(s)
            both.append([jnp.concatenate(list(c), axis=1) for c in zip(*parts_of)])
        return [b[0] for b in both] + [b[1] for b in both]

    def small_rows(i):
        out = []
        for m, (_, nq) in enumerate(SMALL):
            own, ins = [], []
            for c in range(3):
                t = rows8(c * nq + (i * nq) // 8)
                own.append(own_s[m, 3, t, :] + rb_s[1, m, t, :])
                ins.append(rb_s[2, m, t, :] + rb_s[0, m, t, :])
            out += [jnp.concatenate(own, axis=1), jnp.concatenate(ins, axis=1)]
        return out

    base, other_base = NQ * y, NQ * (1 - y)

    late_cv = cvt[...].T.astype(BF16)

    def f_of(want_q):
        sel = jnp.where(iota((L, L), 1) == want_q, 1.0, 0.0).astype(BF16)
        return dot(sel, late_cv)

    kf = iota((L, L), 0)
    h1 = QC * N1
    kt = kf - 2 * h1
    ks, ku = kt >> 4, kt & 7
    kq = jnp.where(ks == 0, SMALL[0][0] + (ku & 1), jnp.where(ks == 1, SMALL[1][0], SMALL[2][0]) + (ku & 3))
    f1_mat[...] = f_of(jnp.where(kt < 0, jnp.where(kf < h1, base + kf, other_base + kf - h1),
                       jnp.where((kt & 8) == 0, base, other_base) + kq))
    f2 = f_of(jnp.where((kf & 8) == 0, base, other_base) + h1 + (kf & 7))
    for i in range(8):
        mine_f = jnp.where((kf >> 4) == i, f2, 0.0).astype(BF16)
        for k in range(3):
            f2_mat[cols(k), cols(i)] = mine_f

    for m, (_, nq) in enumerate(SMALL):
        all_of(rb_s.at[:, m, pl.ds(0, 24 * nq)], rs_recv.at[m]).wait_recv()
    by_core(lambda rows: all_of(rb_m.at[:, pl.ds(0, N1), pl.ds(0, rows)], r_recv.at[0]).wait_recv())

    def turned(w):
        return jnp.concatenate([w[:, cols(c)].T for c in range(3)], axis=0)

    for i in range(8):
        w = jnp.concatenate(w_rows(i, range(N1)) + small_rows(i), axis=0)
        here = (kt < 0) | ((ks == 0) & (ku >> 1 == i % 4)) | ((ks > 0) & (ku >> 2 == i % 2))
        f1 = jnp.where(here, f1_mat[...], 0.0).astype(BF16)
        v = dot(parts(turned(w)), jnp.concatenate([f1] * 3, axis=0))
        for h in range(2):
            v_acc[h, i] = v[CH * h:CH * h + CH]

    across = pltpu.make_async_remote_copy(
        src_ref=v_acc.at[1 - core], dst_ref=v_in, send_sem=v_sem.at[0], recv_sem=v_sem.at[1],
        device_id=partner, device_id_type=MESH)
    across.start()

    for m, (_, nq) in enumerate(SMALL):
        all_of(ps_s.at[m, :, pl.ds(0, 24 * nq)], ds_send.at[m]).wait_send()
        all_of(own_s.at[m, pl.ds(0, 3), pl.ds(0, 24 * nq)], rs_send.at[m]).wait_send()
    all_of(ps_m, d_send).wait_send()
    by_core(lambda rows: all_of(rb_m.at[:, N1, pl.ds(0, rows)], r_recv.at[1]).wait_recv())

    rows = [v for i in range(7) for v in w_rows(i, range(N1, NM))]
    rows += [jnp.where(core == 0, v, 0.0) for v in w_rows(7, range(N1, NM))]
    w2[...] = jnp.concatenate(rows, axis=0)
    last = pltpu.make_async_remote_copy(
        src_ref=w2, dst_ref=w2_in, send_sem=w_sem.at[0], recv_sem=w_sem.at[1], device_id=partner, device_id_type=MESH)
    last.start()

    def finish_v(w, acc, who):
        t = turned(w)
        t = parts(jnp.where(core == 0, t[0:CH], t[CH:2 * CH]))
        vs = [dot(t, f2_mat[:, cols(2 * g, 2)]) for g in range(4)]
        for i in range(7):
            out_ref[who * 8 + i] = (acc(i) + vs[i // 2][:, cols(i % 2)])[0:NC, 0:NV]

        @pl.when(who == 0)
        def _():
            out_ref[7] = (acc(7) + vs[3][:, cols(1)])[0:NC, 0:NV]

    finish_v(w2[...], lambda i: v_acc[core, i], core)
    across.wait_recv()
    last.wait_recv()
    finish_v(w2_in[...], lambda i: v_in[i], 1 - core)
    across.wait_send()
    last.wait_send()
    by_core(lambda rows: all_of(own_m.at[:, pl.ds(0, 3), pl.ds(0, rows)], r_send).wait_send())


def solution(mesh):
    def local_program(ints_blk, c_occ, c_vir):
        v = pl.pallas_call(
            kernel,
            out_shape=pltpu.VMEM((NO, NC, NV), F32),
            in_specs=[pl.BlockSpec(memory_space=pl.ANY)] * 3,
            out_specs=pl.BlockSpec(memory_space=pltpu.VMEM),
            scratch_shapes=[
                pltpu.VMEM((2, 2, NP, 4, NB, NB), BF16),
                pltpu.VMEM((NP, 2, NB, NB), BF16),
                pltpu.VMEM((NP, 4, NB, NB), BF16),
                pltpu.VMEM((NP, 4, NB, NB), BF16),
                pltpu.VMEM((NO, NB), BF16),
                pltpu.VMEM((NV, NB), BF16),
                pltpu.VMEM((16, L), F32),
                pltpu.VMEM((L, L), F32),
                pltpu.VMEM((L, 1024), BF16),
                pltpu.VMEM((4, 512, 256), BF16),
                pltpu.VMEM((2, 512, 256), BF16),
                pltpu.VMEM((L, 256), BF16),
                pltpu.VMEM((64, 256), BF16),
                pltpu.VMEM((32, 256), BF16),
                pltpu.VMEM((L, L), F32),
                pltpu.VMEM((384, 1024), BF16),
                pltpu.VMEM((NO, 256, L), BF16),
                pltpu.VMEM((6, 256, 256), BF16),
                pltpu.VMEM((NM, 4, RW, L), F32),
                pltpu.VMEM((3, 4, 96, L), F32),
                pltpu.VMEM((NM, 4, RW, L), F32),
                pltpu.VMEM((3, 4, 96, L), F32),
                pltpu.VMEM((NM, 4, RW, L), F32),
                pltpu.VMEM((3, 4, 96, L), F32),
                pltpu.VMEM((3, NM, RW, L), F32),
                pltpu.VMEM((3, 3, 96, L), F32),
                pltpu.VMEM((2, 8, CH, L), F32),
                pltpu.VMEM((8, CH, L), F32),
                pltpu.VMEM((L, LW), F32),
                pltpu.VMEM((L, LW), F32),
                pltpu.SemaphoreType.DMA((2, 2)),
                pltpu.SemaphoreType.DMA((3, 2)),
                pltpu.SemaphoreType.DMA((2,)),
                pltpu.SemaphoreType.DMA,
                pltpu.SemaphoreType.DMA((NM, 2)),
                pltpu.SemaphoreType.DMA((3,)),
                pltpu.SemaphoreType.DMA((3, 2)),
                pltpu.SemaphoreType.DMA,
                pltpu.SemaphoreType.DMA((2,)),
                pltpu.SemaphoreType.DMA((3,)),
                pltpu.SemaphoreType.DMA((3,)),
                pltpu.SemaphoreType.DMA((2,)),
                pltpu.SemaphoreType.DMA((2,)),
            ],
            compiler_params=pltpu.CompilerParams(
                collective_id=0, has_side_effects=True, vmem_limit_bytes=60 * 1024 * 1024),
            name='four_index',
        )(ints_blk, c_occ.T, c_vir.T)
        return v.transpose(0, 2, 1)

    return jax.shard_map(
        local_program,
        mesh=mesh,
        in_specs=(P(('frag', 'dev'), 'dev2', None, None), P('frag', None), P('frag', None)),
        out_specs=P(None, None, ('frag', 'dev2', 'dev')),
        check_vma=False,
    )
```

```python
import jax
import jax.numpy as jnp
from jax import lax
from jax.experimental import pallas as pl
from jax.experimental.pallas import tpu as pltpu
from jax.sharding import PartitionSpec as P

MESH = pl.DeviceIdType.MESH
F32, BF16, I32 = jnp.float32, jnp.bfloat16, jnp.int32

NP, NQ, NB = 29, 58, 116
NO, NV = 15, 96
QC = 8
NM = 6
SMALL = ((48, 2), (50, 4), (54, 4))
PG = 4
L = 128
LW = 3 * L
SP = 108
PW, NS = L - SP, 6
NC, CH = 180, 184
RW = 184
ROWS = (RW, RW - 24)
N1 = NM - 1


def place_of(i, c):
    return 3 * i - 1 + c if i else c


def cols(k, n=1):
    return slice(L * k, L * (k + n))


def rows8(k, n=1):
    return slice(8 * k, 8 * (k + n))


def iota(shape, dim):
    return lax.broadcasted_iota(I32, shape, dim)


def dot(a, b):
    return jnp.dot(a, b, preferred_element_type=F32)


def parts(w):
    hi = w.astype(BF16)
    rest = w - hi.astype(F32)
    mid = rest.astype(BF16)
    lo = (rest - mid.astype(F32)).astype(BF16)
    return jnp.concatenate([hi, mid, lo], axis=1)


def kernel(a_hbm, cot_hbm, cvt_hbm, out_ref, abuf, as0, as1, as2, cot_in, cvt_in, cot, cvt, s_mat, b_mat, bs_mat, l8, l4, l2,
           f1_mat, f2_mat, x_buf, h_buf, own_m, own_s, ps_m, ps_s, pr_m, pr_s, rb_m, rb_s, v_acc, v_in, w2, w2_in,
           a_sem, as_sem, c_sem, d_send, d_recv, ds_send, ds_recv, r_send, r_recv, rs_send, rs_recv, v_sem, w_sem):
    y = lax.axis_index('dev2')
    dev = lax.axis_index('dev')
    core = lax.rem(dev, 2)
    x = dev // 2
    partner = (0, y, x * 2 + (1 - core))
    peers = [(0, 1 - y, (1 - x) * 2 + core), (0, y, (1 - x) * 2 + core), (0, 1 - y, x * 2 + core)]
    chip = [2 * (1 - y) + (1 - x), 2 * y + (1 - x), 2 * (1 - y) + x, 2 * y + x]

    def a_copy(n, half, slot):
        return pltpu.make_async_copy(
            a_hbm.at[:, pl.ds(n * QC + 4 * half, 4)], abuf.at[slot, half], a_sem.at[slot, half])

    def all_of(ref, sem):
        return pltpu.make_async_remote_copy(
            src_ref=ref, dst_ref=ref, send_sem=sem, recv_sem=sem, device_id=partner, device_id_type=MESH)

    small = [pltpu.make_async_copy(cot_hbm, cot_in, c_sem.at[0]), pltpu.make_async_copy(cvt_hbm, cvt_in, c_sem.at[1])]
    a_small = (as0, as1, as2)
    small_copy = [[pltpu.make_async_copy(a_hbm.at[:, pl.ds(q + 2 * k, 2)], a_small[m].at[:, pl.ds(2 * k, 2)],
                                         as_sem.at[m, k]) for k in range(nq // 2)]
                  for m, (q, nq) in enumerate(SMALL)]
    for c in small:
        c.start()
    small_copy[0][0].start()

    barrier = pltpu.get_barrier_semaphore()
    for other in [partner] + peers:
        pl.semaphore_signal(barrier, inc=1, device_id=other, device_id_type=MESH)

    cot[...] = jnp.zeros_like(cot)
    cvt[...] = jnp.zeros_like(cvt)
    for c in small:
        c.wait()
    for c in small_copy[1]:
        c.start()
    cot[0:NO, 0:NB] = cot_in[...].astype(F32)
    cvt[0:NV, 0:NB] = cvt_in[...].astype(F32)
    sub = iota((8, L), 0)
    zero = jnp.zeros((8, L), F32)
    for jj in range(8):
        for p in range(8):
            two = [jnp.where(sub == p, cot[j:j + 1, :], zero) for j in (2 * jj, 2 * jj + 1)]
            s_mat[rows8(2 * jj, 2), cols(p)] = jnp.concatenate(two, axis=0).astype(BF16)
    cv = cvt[...].T.astype(BF16)
    first = [(15 * c) // 4 for c in chip]
    first_s = [4 * c + 2 - c // 3 for c in chip]
    lane, row = iota((1, 256), 1), iota((L, 256), 0)
    bs_mat[...] = jnp.zeros_like(bs_mat)

    def full_of(rel, block, j0, steps):
        c = rel + 360 * block
        step = sum((c >= 96 * (j0 + t)).astype(I32) for t in range(1, steps))
        place = jnp.where(row == c - 96 * (j0 + step), 1.0, 0.0).astype(BF16)
        return dot(cv, place), step

    far = -100000
    rel = jnp.where(lane < NC, lane, jnp.where(lane < CH, far, lane - 4))
    for r in range(4):
        full, step = full_of(rel, chip[r], first[r], 4)
        for t in range(4):
            b_mat[r, cols(t), :] = jnp.where(step == t, full, 0.0).astype(BF16)
    rel = jnp.where((lane & (L - 1)) < SP, (lane & (L - 1)) + 252, far)
    for p in range(2):
        r0, r1 = 2 * p, 2 * p + 1
        full, step = full_of(rel, jnp.where(lane < L, chip[r0], chip[r1]), jnp.where(lane < L, first_s[r0], first_s[r1]), 2)
        for t in range(2):
            some = jnp.where(step == t, full, 0.0).astype(BF16)
            for h in range(2):
                bs_mat[p, cols(2 * h + t), cols(h)] = some[:, cols(h)]
    low, high = cot[0:8, :], cot[8:16, :]
    mine = jnp.concatenate([jnp.where(core == 0, low, high), jnp.where(core == 0, high, low)], axis=0)
    kk = iota((L, 256), 1)
    ploc = ((kk >> 4) & 3) * 8 + (kk & 7)
    pick = (iota((L, 256), 0) == ploc + NP * dev) & (ploc < NP)
    l0 = dot(mine.astype(BF16), jnp.where(pick, 1.0, 0.0).astype(BF16)).astype(BF16)
    def build_l(l_mat, sh):
        nq = 1 << sh
        rows = 16 * nq
        e = jnp.where((iota((rows, 16), 0) >> sh) == iota((rows, 16), 1), 1.0, 0.0).astype(BF16)
        row, k2 = iota((rows, 256), 0), iota((rows, 256), 1)
        here = (k2 >> 6) * 2 + ((k2 >> 3) & 1) == (row & (nq - 1))
        l_mat[...] = jnp.where(here, dot(e, l0), 0.0).astype(BF16)

    build_l(l2, 1)
    build_l(l4, 2)
    build_l(l8, 3)

    def step1(tile_of, qp):
        zl = jnp.zeros((NB, L - NB), BF16)
        zs = jnp.zeros((L - NB, L), BF16)

        def tile(p, q):
            t = jnp.concatenate([tile_of(p, q), zl], axis=1)
            return jnp.concatenate([t, zs], axis=0)

        for pg in range(PG):
            ps = range(8 * pg, min(NP, 8 * pg + 8))
            rhs = jnp.concatenate([jnp.concatenate([tile(p, 0), tile(p, 1)], axis=1) for p in ps], axis=0)
            t = dot(s_mat[rows8(0, NO), cols(0, len(ps))], rhs)
            r = rows8(8 * qp + 2 * pg, 2)
            for j in range(NO):
                two = jnp.concatenate([t[rows8(j), cols(k)] for k in range(2)], axis=0)
                x_buf[j, r, :] = two.astype(BF16)

    def stage_h(rows, k):
        p, t = k // 3, k % 3
        if t < 2:
            js, weights = [first[2 * p + t] + j for j in range(4)], b_mat[2 * p + t]
        else:
            js, weights = [first_s[r] + j for r in (2 * p, 2 * p + 1) for j in range(2)], bs_mat[p]
        lhs = jnp.concatenate([x_buf[j, 0:rows, :] for j in js], axis=1)
        h_buf[k, 0:rows, :] = dot(lhs, weights).astype(BF16)

    def stage_w(rows, lhs, p):
        w = [dot(lhs, h_buf[3 * p + t, 0:rows, :]) for t in range(3)]
        return [jnp.concatenate([w[k], w[2][:, cols(k)]], axis=1) for k in range(2)]

    lane8 = iota((8, L), 1)
    spare = lane8 >= SP

    def pack(ref, w):
        col = [[w[rows8(i), cols(c)] for c in range(3)] for i in range(8)]
        for i in range(8):
            for c in range(3 if i else 2):
                v = col[i][c]
                if c == 2 and i <= NS:
                    v = jnp.where(spare, pltpu.roll(col[0][c], SP - PW * (i - 1), 1), v)
                ref[rows8(place_of(i, c)), :] = v

    def d2d(n, r):
        return pltpu.make_async_remote_copy(
            src_ref=ps_m.at[n, r], dst_ref=pr_m.at[n, r], send_sem=d_send, recv_sem=d_recv.at[n, r // 2],
            device_id=partner, device_id_type=MESH)

    def d2d_s(m, r):
        part = pl.ds(0, 24 * SMALL[m][1])
        return pltpu.make_async_remote_copy(
            src_ref=ps_s.at[m, r, part], dst_ref=pr_s.at[m, r, part], send_sem=ds_send.at[m],
            recv_sem=ds_recv.at[m, r // 2], device_id=partner, device_id_type=MESH)

    def out_m(n, r, rows):
        return pltpu.make_async_remote_copy(
            src_ref=own_m.at[n, r, pl.ds(0, rows)], dst_ref=rb_m.at[r, n, pl.ds(0, rows)],
            send_sem=r_send, recv_sem=r_recv.at[n // N1], device_id=peers[r], device_id_type=MESH)

    def out_s(m, r):
        part = pl.ds(0, 24 * SMALL[m][1])
        return pltpu.make_async_remote_copy(
            src_ref=own_s.at[m, r, part], dst_ref=rb_s.at[r, m, part], send_sem=rs_send.at[m],
            recv_sem=rs_recv.at[m], device_id=peers[r], device_id_type=MESH)

    def by_core(f):
        for k in range(2):
            @pl.when(core == k)
            def _(k=k):
                f(ROWS[k])

    def finish_m(n, rs):
        all_of(pr_m.at[n, pl.ds(rs[0], 2)], d_recv.at[n, rs[0] // 2]).wait_recv()
        for r in rs:
            own_m[n, r] = own_m[n, r] + pr_m[n, r]

        def go(rows):
            for r in rs:
                if r < 3:
                    out_m(n, r, rows).start()

        by_core(go)

    def finish_s(m):
        part = rows8(0, 3 * SMALL[m][1])
        for r in range(4):
            if r % 2 == 0:
                all_of(pr_s.at[m, pl.ds(r, 2), pl.ds(0, 24 * SMALL[m][1])], ds_recv.at[m, r // 2]).wait_recv()
            own_s[m, r, part, :] = own_s[m, r, part, :] + pr_s[m, r, part, :]
            if r < 3:
                out_s(m, r).start()

    for m, (l_mat, a_ref) in enumerate(zip((l2, l4, l4), a_small)):
        nq = SMALL[m][1]
        for qp in range(nq // 2):
            small_copy[m][qp].wait()
            step1(lambda p, q: a_ref[p, 2 * qp + q], qp)
        if m == 0:
            for c in small_copy[2]:
                c.start()
            pl.semaphore_wait(barrier, 4)
        else:
            for half in range(2):
                a_copy(m - 1, half, m - 1).start()
            finish_s(m - 1)
        rows = 32 * nq
        for k in range(6):
            stage_h(rows, k)
        for p in range(2):
            pair = (2 * p, 2 * p + 1)
            for r, w in zip(pair, stage_w(rows, l_mat[:, 0:rows], p)):
                for c in range(3):
                    own_s[m, r, rows8(c * nq, nq), :] = w[rows8(0, nq), cols(c)]
                    ps_s[m, r, rows8(c * nq, nq), :] = w[rows8(nq, nq), cols(c)]
            for r in pair:
                d2d_s(m, r).start()

    def body(n, carry):
        slot = lax.rem(n, 2)
        for half in range(2):
            qps = (2 * half, 2 * half + 1)
            a_copy(n, half, slot).wait()
            for qp in qps:
                step1(lambda p, q: abuf[slot, half, p, 2 * (qp % 2) + q], qp)

            @pl.when(n + 2 < NM)
            def _():
                a_copy(n + 2, half, slot).start()

            if half == 0:
                @pl.when(n == 0)
                def _():
                    finish_s(2)

            @pl.when(n > 0)
            def _():
                finish_m(n - 1, qps)

        for k in range(6):
            stage_h(256, k)
        for p in range(2):
            pair = (2 * p, 2 * p + 1)
            for r, w in zip(pair, stage_w(256, l8[...], p)):
                pack(own_m.at[n, r], w[rows8(0, 8)])
                pack(ps_m.at[n, r], w[rows8(8, 8)])
            for r in pair:
                d2d(n, r).start()
        return carry

    lax.fori_loop(0, NM, body, 0)
    finish_m(NM - 1, (0, 1))
    finish_m(NM - 1, (2, 3))

    def w_rows(i, ns):
        def block(n, b):
            near = own_m[n, 3, rows8(b), :] + rb_m[1, n, rows8(b), :]
            far = rb_m[2, n, rows8(b), :] + rb_m[0, n, rows8(b), :]
            return near, far

        both = []
        for n in ns:
            parts_of = [block(n, place_of(i, c)) for c in range(3 if i else 2)]
            if not i:
                s = [jnp.zeros((8, L), F32)] * 2
                for m in range(NS):
                    piece = block(n, place_of(m + 1, 2))
                    here = (lane8 >= PW * m) & (lane8 < min(SP, PW * m + PW))
                    s = [jnp.where(here, pltpu.roll(v, PW * m + PW, 1), o) for v, o in zip(piece, s)]
                parts_of.append(s)
            both.append([jnp.concatenate(list(c), axis=1) for c in zip(*parts_of)])
        return [b[0] for b in both] + [b[1] for b in both]

    def small_rows(i):
        out = []
        for m, (_, nq) in enumerate(SMALL):
            own, ins = [], []
            for c in range(3):
                t = rows8(c * nq + (i * nq) // 8)
                own.append(own_s[m, 3, t, :] + rb_s[1, m, t, :])
                ins.append(rb_s[2, m, t, :] + rb_s[0, m, t, :])
            out += [jnp.concatenate(own, axis=1), jnp.concatenate(ins, axis=1)]
        return out

    base, other_base = NQ * y, NQ * (1 - y)

    late_cv = cvt[...].T.astype(BF16)

    def f_of(want_q):
        sel = jnp.where(iota((L, L), 1) == want_q, 1.0, 0.0).astype(BF16)
        return dot(sel, late_cv)

    kf = iota((L, L), 0)
    h1 = QC * N1
    kt = kf - 2 * h1
    ks, ku = kt >> 4, kt & 7
    kq = jnp.where(ks == 0, SMALL[0][0] + (ku & 1), jnp.where(ks == 1, SMALL[1][0], SMALL[2][0]) + (ku & 3))
    f1_mat[...] = f_of(jnp.where(kt < 0, jnp.where(kf < h1, base + kf, other_base + kf - h1),
                       jnp.where((kt & 8) == 0, base, other_base) + kq))
    f2 = f_of(jnp.where((kf & 8) == 0, base, other_base) + h1 + (kf & 7))
    for i in range(8):
        mine_f = jnp.where((kf >> 4) == i, f2, 0.0).astype(BF16)
        for k in range(3):
            f2_mat[cols(k), cols(i)] = mine_f

    for m, (_, nq) in enumerate(SMALL):
        all_of(rb_s.at[:, m, pl.ds(0, 24 * nq)], rs_recv.at[m]).wait_recv()
    by_core(lambda rows: all_of(rb_m.at[:, pl.ds(0, N1), pl.ds(0, rows)], r_recv.at[0]).wait_recv())

    def turned(w):
        return jnp.concatenate([w[:, cols(c)].T for c in range(3)], axis=0)

    for i in range(8):
        w = jnp.concatenate(w_rows(i, range(N1)) + small_rows(i), axis=0)
        here = (kt < 0) | ((ks == 0) & (ku >> 1 == i % 4)) | ((ks > 0) & (ku >> 2 == i % 2))
        f1 = jnp.where(here, f1_mat[...], 0.0).astype(BF16)
        v = dot(parts(turned(w)), jnp.concatenate([f1] * 3, axis=0))
        for h in range(2):
            v_acc[h, i] = v[CH * h:CH * h + CH]

    across = pltpu.make_async_remote_copy(
        src_ref=v_acc.at[1 - core], dst_ref=v_in, send_sem=v_sem.at[0], recv_sem=v_sem.at[1],
        device_id=partner, device_id_type=MESH)
    across.start()

    for m, (_, nq) in enumerate(SMALL):
        all_of(ps_s.at[m, :, pl.ds(0, 24 * nq)], ds_send.at[m]).wait_send()
        all_of(own_s.at[m, pl.ds(0, 3), pl.ds(0, 24 * nq)], rs_send.at[m]).wait_send()
    all_of(ps_m, d_send).wait_send()
    by_core(lambda rows: all_of(rb_m.at[:, N1, pl.ds(0, rows)], r_recv.at[1]).wait_recv())

    rows = [v for i in range(7) for v in w_rows(i, range(N1, NM))]
    rows += [jnp.where(core == 0, v, 0.0) for v in w_rows(7, range(N1, NM))]
    w = jnp.concatenate(rows, axis=0)
    for c in range(3):
        w2[c] = w[:, cols(c)]
    last = pltpu.make_async_remote_copy(
        src_ref=w2.at[pl.ds(1 - core, 2)], dst_ref=w2_in, send_sem=w_sem.at[0], recv_sem=w_sem.at[1], device_id=partner, device_id_type=MESH)
    last.start()

    def finish_v(w, acc, who):
        t = jnp.concatenate([v.T for v in w], axis=0)
        t = parts(jnp.where(core == 0, t[0:CH], t[CH - L:2 * CH - L]))
        vs = [dot(t, f2_mat[:, cols(2 * g, 2)]) for g in range(4)]
        for i in range(7):
            out_ref[who * 8 + i] = (acc(i) + vs[i // 2][:, cols(i % 2)])[0:NC, 0:NV]

        @pl.when(who == 0)
        def _():
            out_ref[7] = (acc(7) + vs[3][:, cols(1)])[0:NC, 0:NV]

    finish_v([w2[core], w2[core + 1]], lambda i: v_acc[core, i], core)
    across.wait_recv()
    last.wait_recv()
    finish_v([w2_in[0], w2_in[1]], lambda i: v_in[i], 1 - core)
    across.wait_send()
    last.wait_send()
    by_core(lambda rows: all_of(own_m.at[:, pl.ds(0, 3), pl.ds(0, rows)], r_send).wait_send())


def solution(mesh):
    def local_program(ints_blk, c_occ, c_vir):
        v = pl.pallas_call(
            kernel,
            out_shape=pltpu.VMEM((NO, NC, NV), F32),
            in_specs=[pl.BlockSpec(memory_space=pl.ANY)] * 3,
            out_specs=pl.BlockSpec(memory_space=pltpu.VMEM),
            scratch_shapes=[
                pltpu.VMEM((2, 2, NP, 4, NB, NB), BF16),
                pltpu.VMEM((NP, 2, NB, NB), BF16),
                pltpu.VMEM((NP, 4, NB, NB), BF16),
                pltpu.VMEM((NP, 4, NB, NB), BF16),
                pltpu.VMEM((NO, NB), BF16),
                pltpu.VMEM((NV, NB), BF16),
                pltpu.VMEM((16, L), F32),
                pltpu.VMEM((L, L), F32),
                pltpu.VMEM((L, 1024), BF16),
                pltpu.VMEM((4, 512, 256), BF16),
                pltpu.VMEM((2, 512, 256), BF16),
                pltpu.VMEM((L, 256), BF16),
                pltpu.VMEM((64, 256), BF16),
                pltpu.VMEM((32, 256), BF16),
                pltpu.VMEM((L, L), F32),
                pltpu.VMEM((384, 1024), BF16),
                pltpu.VMEM((NO, 256, L), BF16),
                pltpu.VMEM((6, 256, 256), BF16),
                pltpu.VMEM((NM, 4, RW, L), F32),
                pltpu.VMEM((3, 4, 96, L), F32),
                pltpu.VMEM((NM, 4, RW, L), F32),
                pltpu.VMEM((3, 4, 96, L), F32),
                pltpu.VMEM((NM, 4, RW, L), F32),
                pltpu.VMEM((3, 4, 96, L), F32),
                pltpu.VMEM((3, NM, RW, L), F32),
                pltpu.VMEM((3, 3, 96, L), F32),
                pltpu.VMEM((2, 8, CH, L), F32),
                pltpu.VMEM((8, CH, L), F32),
                pltpu.VMEM((3, L, L), F32),
                pltpu.VMEM((2, L, L), F32),
                pltpu.SemaphoreType.DMA((2, 2)),
                pltpu.SemaphoreType.DMA((3, 2)),
                pltpu.SemaphoreType.DMA((2,)),
                pltpu.SemaphoreType.DMA,
                pltpu.SemaphoreType.DMA((NM, 2)),
                pltpu.SemaphoreType.DMA((3,)),
                pltpu.SemaphoreType.DMA((3, 2)),
                pltpu.SemaphoreType.DMA,
                pltpu.SemaphoreType.DMA((2,)),
                pltpu.SemaphoreType.DMA((3,)),
                pltpu.SemaphoreType.DMA((3,)),
                pltpu.SemaphoreType.DMA((2,)),
                pltpu.SemaphoreType.DMA((2,)),
            ],
            compiler_params=pltpu.CompilerParams(
                collective_id=0, has_side_effects=True, vmem_limit_bytes=60 * 1024 * 1024),
            name='four_index',
        )(ints_blk, c_occ.T, c_vir.T)
        return v.transpose(0, 2, 1)

    return jax.shard_map(
        local_program,
        mesh=mesh,
        in_specs=(P(('frag', 'dev'), 'dev2', None, None), P('frag', None), P('frag', None)),
        out_specs=P(None, None, ('frag', 'dev2', 'dev')),
        check_vma=False,
    )
```

```python
import jax
import jax.numpy as jnp
from jax import lax
from jax.experimental import pallas as pl
from jax.experimental.pallas import tpu as pltpu
from jax.sharding import PartitionSpec as P

MESH = pl.DeviceIdType.MESH
F32, BF16, I32 = jnp.float32, jnp.bfloat16, jnp.int32

NP, NQ, NB = 29, 58, 116
NO, NV = 15, 96
QC = 8
NM = 6
SMALL = ((48, 2), (50, 4), (54, 4))
PG = 4
L = 128
LW = 3 * L
SP = 108
PW, NS = L - SP, 6
NC, CH = 180, 184
RW = 184
ROWS = (RW, RW - 24)
N1 = NM - 1


def place_of(i, c):
    return 3 * i - 1 + c if i else c


def cols(k, n=1):
    return slice(L * k, L * (k + n))


def rows8(k, n=1):
    return slice(8 * k, 8 * (k + n))


def iota(shape, dim):
    return lax.broadcasted_iota(I32, shape, dim)


def dot(a, b):
    return jnp.dot(a, b, preferred_element_type=F32)


def parts(w):
    hi = w.astype(BF16)
    rest = w - hi.astype(F32)
    mid = rest.astype(BF16)
    lo = (rest - mid.astype(F32)).astype(BF16)
    return jnp.concatenate([hi, mid, lo], axis=1)


def kernel(a_hbm, cot_hbm, cvt_hbm, out_ref, abuf, as0, as1, as2, cot_in, cvt_in, cot, cvt, s_mat, b_mat, bs_mat, l8, l4, l2,
           f1_mat, f2_mat, x_buf, h_buf, own_m, own_s, ps_m, ps_s, pr_m, pr_s, rb_m, rb_s, v_acc, v_in, w2, w2_in,
           a_sem, as_sem, c_sem, d_send, d_recv, ds_send, ds_recv, r_send, r_recv, rs_send, rs_recv, v_sem, w_sem):
    y = lax.axis_index('dev2')
    dev = lax.axis_index('dev')
    core = lax.rem(dev, 2)
    x = dev // 2
    partner = (0, y, x * 2 + (1 - core))
    peers = [(0, 1 - y, (1 - x) * 2 + core), (0, 1 - y, x * 2 + core), (0, y, (1 - x) * 2 + core)]
    chip = [2 * (1 - y) + (1 - x), 2 * (1 - y) + x, 2 * y + (1 - x), 2 * y + x]

    def a_copy(n, half, slot):
        return pltpu.make_async_copy(
            a_hbm.at[:, pl.ds(n * QC + 4 * half, 4)], abuf.at[slot, half], a_sem.at[slot, half])

    def all_of(ref, sem):
        return pltpu.make_async_remote_copy(
            src_ref=ref, dst_ref=ref, send_sem=sem, recv_sem=sem, device_id=partner, device_id_type=MESH)

    small = [pltpu.make_async_copy(cot_hbm, cot_in, c_sem.at[0]), pltpu.make_async_copy(cvt_hbm, cvt_in, c_sem.at[1])]
    a_small = (as0, as1, as2)
    small_copy = [[pltpu.make_async_copy(a_hbm.at[:, pl.ds(q + 2 * k, 2)], a_small[m].at[:, pl.ds(2 * k, 2)],
                                         as_sem.at[m, k]) for k in range(nq // 2)]
                  for m, (q, nq) in enumerate(SMALL)]
    for c in small:
        c.start()
    small_copy[0][0].start()

    barrier = pltpu.get_barrier_semaphore()
    for other in [partner] + peers:
        pl.semaphore_signal(barrier, inc=1, device_id=other, device_id_type=MESH)

    cot[...] = jnp.zeros_like(cot)
    cvt[...] = jnp.zeros_like(cvt)
    for c in small:
        c.wait()
    for c in small_copy[1]:
        c.start()
    cot[0:NO, 0:NB] = cot_in[...].astype(F32)
    cvt[0:NV, 0:NB] = cvt_in[...].astype(F32)
    sub = iota((8, L), 0)
    zero = jnp.zeros((8, L), F32)
    for jj in range(8):
        for p in range(8):
            two = [jnp.where(sub == p, cot[j:j + 1, :], zero) for j in (2 * jj, 2 * jj + 1)]
            s_mat[rows8(2 * jj, 2), cols(p)] = jnp.concatenate(two, axis=0).astype(BF16)
    cv = cvt[...].T.astype(BF16)
    first = [(15 * c) // 4 for c in chip]
    first_s = [4 * c + 2 - c // 3 for c in chip]
    lane, row = iota((1, 256), 1), iota((L, 256), 0)
    bs_mat[...] = jnp.zeros_like(bs_mat)

    def full_of(rel, block, j0, steps):
        c = rel + 360 * block
        step = sum((c >= 96 * (j0 + t)).astype(I32) for t in range(1, steps))
        place = jnp.where(row == c - 96 * (j0 + step), 1.0, 0.0).astype(BF16)
        return dot(cv, place), step

    far = -100000
    rel = jnp.where(lane < NC, lane, jnp.where(lane < CH, far, lane - 4))
    for r in range(4):
        full, step = full_of(rel, chip[r], first[r], 4)
        for t in range(4):
            b_mat[r, cols(t), :] = jnp.where(step == t, full, 0.0).astype(BF16)
    rel = jnp.where((lane & (L - 1)) < SP, (lane & (L - 1)) + 252, far)
    for p in range(2):
        r0, r1 = 2 * p, 2 * p + 1
        full, step = full_of(rel, jnp.where(lane < L, chip[r0], chip[r1]), jnp.where(lane < L, first_s[r0], first_s[r1]), 2)
        for t in range(2):
            some = jnp.where(step == t, full, 0.0).astype(BF16)
            for h in range(2):
                bs_mat[p, cols(2 * h + t), cols(h)] = some[:, cols(h)]
    low, high = cot[0:8, :], cot[8:16, :]
    mine = jnp.concatenate([jnp.where(core == 0, low, high), jnp.where(core == 0, high, low)], axis=0)
    kk = iota((L, 256), 1)
    ploc = ((kk >> 4) & 3) * 8 + (kk & 7)
    pick = (iota((L, 256), 0) == ploc + NP * dev) & (ploc < NP)
    l0 = dot(mine.astype(BF16), jnp.where(pick, 1.0, 0.0).astype(BF16)).astype(BF16)
    def build_l(l_mat, sh):
        nq = 1 << sh
        rows = 16 * nq
        e = jnp.where((iota((rows, 16), 0) >> sh) == iota((rows, 16), 1), 1.0, 0.0).astype(BF16)
        row, k2 = iota((rows, 256), 0), iota((rows, 256), 1)
        here = (k2 >> 6) * 2 + ((k2 >> 3) & 1) == (row & (nq - 1))
        l_mat[...] = jnp.where(here, dot(e, l0), 0.0).astype(BF16)

    build_l(l2, 1)
    build_l(l4, 2)
    build_l(l8, 3)

    def step1(tile_of, qp):
        zl = jnp.zeros((NB, L - NB), BF16)
        zs = jnp.zeros((L - NB, L), BF16)

        def tile(p, q):
            t = jnp.concatenate([tile_of(p, q), zl], axis=1)
            return jnp.concatenate([t, zs], axis=0)

        for pg in range(PG):
            ps = range(8 * pg, min(NP, 8 * pg + 8))
            rhs = jnp.concatenate([jnp.concatenate([tile(p, 0), tile(p, 1)], axis=1) for p in ps], axis=0)
            t = dot(s_mat[rows8(0, NO), cols(0, len(ps))], rhs)
            r = rows8(8 * qp + 2 * pg, 2)
            for j in range(NO):
                two = jnp.concatenate([t[rows8(j), cols(k)] for k in range(2)], axis=0)
                x_buf[j, r, :] = two.astype(BF16)

    def stage_h(rows, k):
        p, t = k // 3, k % 3
        if t < 2:
            js, weights = [first[2 * p + t] + j for j in range(4)], b_mat[2 * p + t]
        else:
            js, weights = [first_s[r] + j for r in (2 * p, 2 * p + 1) for j in range(2)], bs_mat[p]
        lhs = jnp.concatenate([x_buf[j, 0:rows, :] for j in js], axis=1)
        h_buf[k, 0:rows, :] = dot(lhs, weights).astype(BF16)

    def stage_w(rows, lhs, p):
        w = [dot(lhs, h_buf[3 * p + t, 0:rows, :]) for t in range(3)]
        return [jnp.concatenate([w[k], w[2][:, cols(k)]], axis=1) for k in range(2)]

    lane8 = iota((8, L), 1)
    spare = lane8 >= SP

    def pack(ref, w):
        col = [[w[rows8(i), cols(c)] for c in range(3)] for i in range(8)]
        for i in range(8):
            for c in range(3 if i else 2):
                v = col[i][c]
                if c == 2 and i <= NS:
                    v = jnp.where(spare, pltpu.roll(col[0][c], SP - PW * (i - 1), 1), v)
                ref[rows8(place_of(i, c)), :] = v

    def d2d(n, r):
        return pltpu.make_async_remote_copy(
            src_ref=ps_m.at[n, r], dst_ref=pr_m.at[n, r], send_sem=d_send, recv_sem=d_recv.at[n, r // 2],
            device_id=partner, device_id_type=MESH)

    def d2d_s(m, r):
        part = pl.ds(0, 24 * SMALL[m][1])
        return pltpu.make_async_remote_copy(
            src_ref=ps_s.at[m, r, part], dst_ref=pr_s.at[m, r, part], send_sem=ds_send.at[m],
            recv_sem=ds_recv.at[m, r // 2], device_id=partner, device_id_type=MESH)

    def out_m(n, r, rows):
        return pltpu.make_async_remote_copy(
            src_ref=own_m.at[n, r, pl.ds(0, rows)], dst_ref=rb_m.at[r, n, pl.ds(0, rows)],
            send_sem=r_send, recv_sem=r_recv.at[n // N1], device_id=peers[r], device_id_type=MESH)

    def out_s(m, r):
        part = pl.ds(0, 24 * SMALL[m][1])
        return pltpu.make_async_remote_copy(
            src_ref=own_s.at[m, r, part], dst_ref=rb_s.at[r, m, part], send_sem=rs_send.at[m],
            recv_sem=rs_recv.at[m], device_id=peers[r], device_id_type=MESH)

    def by_core(f):
        for k in range(2):
            @pl.when(core == k)
            def _(k=k):
                f(ROWS[k])

    def finish_m(n, rs):
        all_of(pr_m.at[n, pl.ds(rs[0], 2)], d_recv.at[n, rs[0] // 2]).wait_recv()
        for r in rs:
            own_m[n, r] = own_m[n, r] + pr_m[n, r]

        def go(rows):
            for r in rs:
                if r < 3:
                    out_m(n, r, rows).start()

        by_core(go)

    def finish_s(m):
        part = rows8(0, 3 * SMALL[m][1])
        for r in range(4):
            if r % 2 == 0:
                all_of(pr_s.at[m, pl.ds(r, 2), pl.ds(0, 24 * SMALL[m][1])], ds_recv.at[m, r // 2]).wait_recv()
            own_s[m, r, part, :] = own_s[m, r, part, :] + pr_s[m, r, part, :]
            if r < 3:
                out_s(m, r).start()

    for m, (l_mat, a_ref) in enumerate(zip((l2, l4, l4), a_small)):
        nq = SMALL[m][1]
        for qp in range(nq // 2):
            small_copy[m][qp].wait()
            step1(lambda p, q: a_ref[p, 2 * qp + q], qp)
        if m == 0:
            for c in small_copy[2]:
                c.start()
            pl.semaphore_wait(barrier, 4)
        else:
            for half in range(2):
                a_copy(m - 1, half, m - 1).start()
            finish_s(m - 1)
        rows = 32 * nq
        for k in range(6):
            stage_h(rows, k)
        for p in range(2):
            pair = (2 * p, 2 * p + 1)
            for r, w in zip(pair, stage_w(rows, l_mat[:, 0:rows], p)):
                for c in range(3):
                    own_s[m, r, rows8(c * nq, nq), :] = w[rows8(0, nq), cols(c)]
                    ps_s[m, r, rows8(c * nq, nq), :] = w[rows8(nq, nq), cols(c)]
            for r in pair:
                d2d_s(m, r).start()

    def body(n, carry):
        slot = lax.rem(n, 2)
        for half in range(2):
            qps = (2 * half, 2 * half + 1)
            a_copy(n, half, slot).wait()
            for qp in qps:
                step1(lambda p, q: abuf[slot, half, p, 2 * (qp % 2) + q], qp)

            @pl.when(n + 2 < NM)
            def _():
                a_copy(n + 2, half, slot).start()

            if half == 0:
                @pl.when(n == 0)
                def _():
                    finish_s(2)

            @pl.when(n > 0)
            def _():
                finish_m(n - 1, qps)

        for k in range(6):
            stage_h(256, k)
        for p in range(2):
            pair = (2 * p, 2 * p + 1)
            for r, w in zip(pair, stage_w(256, l8[...], p)):
                pack(own_m.at[n, r], w[rows8(0, 8)])
                pack(ps_m.at[n, r], w[rows8(8, 8)])
            for r in pair:
                d2d(n, r).start()
        return carry

    lax.fori_loop(0, NM, body, 0)
    finish_m(NM - 1, (0, 1))
    finish_m(NM - 1, (2, 3))

    def w_rows(i, ns):
        def block(n, b):
            near = own_m[n, 3, rows8(b), :] + rb_m[2, n, rows8(b), :]
            far = rb_m[1, n, rows8(b), :] + rb_m[0, n, rows8(b), :]
            return near, far

        both = []
        for n in ns:
            parts_of = [block(n, place_of(i, c)) for c in range(3 if i else 2)]
            if not i:
                s = [jnp.zeros((8, L), F32)] * 2
                for m in range(NS):
                    piece = block(n, place_of(m + 1, 2))
                    here = (lane8 >= PW * m) & (lane8 < min(SP, PW * m + PW))
                    s = [jnp.where(here, pltpu.roll(v, PW * m + PW, 1), o) for v, o in zip(piece, s)]
                parts_of.append(s)
            both.append([jnp.concatenate(list(c), axis=1) for c in zip(*parts_of)])
        return [b[0] for b in both] + [b[1] for b in both]

    def small_rows(i):
        out = []
        for m, (_, nq) in enumerate(SMALL):
            own, ins = [], []
            for c in range(3):
                t = rows8(c * nq + (i * nq) // 8)
                own.append(own_s[m, 3, t, :] + rb_s[2, m, t, :])
                ins.append(rb_s[1, m, t, :] + rb_s[0, m, t, :])
            out += [jnp.concatenate(own, axis=1), jnp.concatenate(ins, axis=1)]
        return out

    base, other_base = NQ * y, NQ * (1 - y)

    late_cv = cvt[...].T.astype(BF16)

    def f_of(want_q):
        sel = jnp.where(iota((L, L), 1) == want_q, 1.0, 0.0).astype(BF16)
        return dot(sel, late_cv)

    kf = iota((L, L), 0)
    h1 = QC * N1
    kt = kf - 2 * h1
    ks, ku = kt >> 4, kt & 7
    kq = jnp.where(ks == 0, SMALL[0][0] + (ku & 1), jnp.where(ks == 1, SMALL[1][0], SMALL[2][0]) + (ku & 3))
    f1_mat[...] = f_of(jnp.where(kt < 0, jnp.where(kf < h1, base + kf, other_base + kf - h1),
                       jnp.where((kt & 8) == 0, base, other_base) + kq))
    f2 = f_of(jnp.where((kf & 8) == 0, base, other_base) + h1 + (kf & 7))
    for i in range(8):
        mine_f = jnp.where((kf >> 4) == i, f2, 0.0).astype(BF16)
        for k in range(3):
            f2_mat[cols(k), cols(i)] = mine_f

    for m, (_, nq) in enumerate(SMALL):
        all_of(rb_s.at[:, m, pl.ds(0, 24 * nq)], rs_recv.at[m]).wait_recv()
    by_core(lambda rows: all_of(rb_m.at[:, pl.ds(0, N1), pl.ds(0, rows)], r_recv.at[0]).wait_recv())

    def turned(w):
        return jnp.concatenate([w[:, cols(c)].T for c in range(3)], axis=0)

    for i in range(8):
        w = jnp.concatenate(w_rows(i, range(N1)) + small_rows(i), axis=0)
        here = (kt < 0) | ((ks == 0) & (ku >> 1 == i % 4)) | ((ks > 0) & (ku >> 2 == i % 2))
        f1 = jnp.where(here, f1_mat[...], 0.0).astype(BF16)
        v = dot(parts(turned(w)), jnp.concatenate([f1] * 3, axis=0))
        for h in range(2):
            v_acc[h, i] = v[CH * h:CH * h + CH]

    across = pltpu.make_async_remote_copy(
        src_ref=v_acc.at[1 - core], dst_ref=v_in, send_sem=v_sem.at[0], recv_sem=v_sem.at[1],
        device_id=partner, device_id_type=MESH)
    across.start()

    for m, (_, nq) in enumerate(SMALL):
        all_of(ps_s.at[m, :, pl.ds(0, 24 * nq)], ds_send.at[m]).wait_send()
        all_of(own_s.at[m, pl.ds(0, 3), pl.ds(0, 24 * nq)], rs_send.at[m]).wait_send()
    all_of(ps_m, d_send).wait_send()
    by_core(lambda rows: all_of(rb_m.at[:, N1, pl.ds(0, rows)], r_recv.at[1]).wait_recv())

    rows = [v for i in range(7) for v in w_rows(i, range(N1, NM))]
    rows += [jnp.where(core == 0, v, 0.0) for v in w_rows(7, range(N1, NM))]
    w = jnp.concatenate(rows, axis=0)
    for c in range(3):
        w2[c] = w[:, cols(c)]
    last = pltpu.make_async_remote_copy(
        src_ref=w2.at[pl.ds(1 - core, 2)], dst_ref=w2_in, send_sem=w_sem.at[0], recv_sem=w_sem.at[1], device_id=partner, device_id_type=MESH)
    last.start()

    def finish_v(w, acc, who):
        t = jnp.concatenate([v.T for v in w], axis=0)
        t = parts(jnp.where(core == 0, t[0:CH], t[CH - L:2 * CH - L]))
        vs = [dot(t, f2_mat[:, cols(2 * g, 2)]) for g in range(4)]
        for i in range(7):
            out_ref[who * 8 + i] = (acc(i) + vs[i // 2][:, cols(i % 2)])[0:NC, 0:NV]

        @pl.when(who == 0)
        def _():
            out_ref[7] = (acc(7) + vs[3][:, cols(1)])[0:NC, 0:NV]

    finish_v([w2[core], w2[core + 1]], lambda i: v_acc[core, i], core)
    across.wait_recv()
    last.wait_recv()
    finish_v([w2_in[0], w2_in[1]], lambda i: v_in[i], 1 - core)
    across.wait_send()
    last.wait_send()
    by_core(lambda rows: all_of(own_m.at[:, pl.ds(0, 3), pl.ds(0, rows)], r_send).wait_send())


def solution(mesh):
    def local_program(ints_blk, c_occ, c_vir):
        v = pl.pallas_call(
            kernel,
            out_shape=pltpu.VMEM((NO, NC, NV), F32),
            in_specs=[pl.BlockSpec(memory_space=pl.ANY)] * 3,
            out_specs=pl.BlockSpec(memory_space=pltpu.VMEM),
            scratch_shapes=[
                pltpu.VMEM((2, 2, NP, 4, NB, NB), BF16),
                pltpu.VMEM((NP, 2, NB, NB), BF16),
                pltpu.VMEM((NP, 4, NB, NB), BF16),
                pltpu.VMEM((NP, 4, NB, NB), BF16),
                pltpu.VMEM((NO, NB), BF16),
                pltpu.VMEM((NV, NB), BF16),
                pltpu.VMEM((16, L), F32),
                pltpu.VMEM((L, L), F32),
                pltpu.VMEM((L, 1024), BF16),
                pltpu.VMEM((4, 512, 256), BF16),
                pltpu.VMEM((2, 512, 256), BF16),
                pltpu.VMEM((L, 256), BF16),
                pltpu.VMEM((64, 256), BF16),
                pltpu.VMEM((32, 256), BF16),
                pltpu.VMEM((L, L), F32),
                pltpu.VMEM((384, 1024), BF16),
                pltpu.VMEM((NO, 256, L), BF16),
                pltpu.VMEM((6, 256, 256), BF16),
                pltpu.VMEM((NM, 4, RW, L), F32),
                pltpu.VMEM((3, 4, 96, L), F32),
                pltpu.VMEM((NM, 4, RW, L), F32),
                pltpu.VMEM((3, 4, 96, L), F32),
                pltpu.VMEM((NM, 4, RW, L), F32),
                pltpu.VMEM((3, 4, 96, L), F32),
                pltpu.VMEM((3, NM, RW, L), F32),
                pltpu.VMEM((3, 3, 96, L), F32),
                pltpu.VMEM((2, 8, CH, L), F32),
                pltpu.VMEM((8, CH, L), F32),
                pltpu.VMEM((3, L, L), F32),
                pltpu.VMEM((2, L, L), F32),
                pltpu.SemaphoreType.DMA((2, 2)),
                pltpu.SemaphoreType.DMA((3, 2)),
                pltpu.SemaphoreType.DMA((2,)),
                pltpu.SemaphoreType.DMA,
                pltpu.SemaphoreType.DMA((NM, 2)),
                pltpu.SemaphoreType.DMA((3,)),
                pltpu.SemaphoreType.DMA((3, 2)),
                pltpu.SemaphoreType.DMA,
                pltpu.SemaphoreType.DMA((2,)),
                pltpu.SemaphoreType.DMA((3,)),
                pltpu.SemaphoreType.DMA((3,)),
                pltpu.SemaphoreType.DMA((2,)),
                pltpu.SemaphoreType.DMA((2,)),
            ],
            compiler_params=pltpu.CompilerParams(
                collective_id=0, has_side_effects=True, vmem_limit_bytes=60 * 1024 * 1024),
            name='four_index',
        )(ints_blk, c_occ.T, c_vir.T)
        return v.transpose(0, 2, 1)

    return jax.shard_map(
        local_program,
        mesh=mesh,
        in_specs=(P(('frag', 'dev'), 'dev2', None, None), P('frag', None), P('frag', None)),
        out_specs=P(None, None, ('frag', 'dev2', 'dev')),
        check_vma=False,
    )
```

```python
import jax
import jax.numpy as jnp
from jax import lax
from jax.experimental import pallas as pl
from jax.experimental.pallas import tpu as pltpu
from jax.sharding import PartitionSpec as P

MESH = pl.DeviceIdType.MESH
F32, BF16, I32 = jnp.float32, jnp.bfloat16, jnp.int32

NP, NQ, NB = 29, 58, 116
NO, NV = 15, 96
QC = 8
NM = 6
SMALL = ((48, 2), (50, 4), (54, 4))
PG = 4
L = 128
LW = 3 * L
SP = 108
PW, NS = L - SP, 6
NC, CH = 180, 184
RW = 184
ROWS = (RW, RW - 24)
N1 = NM - 1


def place_of(i, c):
    return 3 * i - 1 + c if i else c


def cols(k, n=1):
    return slice(L * k, L * (k + n))


def rows8(k, n=1):
    return slice(8 * k, 8 * (k + n))


def iota(shape, dim):
    return lax.broadcasted_iota(I32, shape, dim)


def dot(a, b):
    return jnp.dot(a, b, preferred_element_type=F32)


def parts(w):
    hi = w.astype(BF16)
    rest = w - hi.astype(F32)
    mid = rest.astype(BF16)
    lo = (rest - mid.astype(F32)).astype(BF16)
    return jnp.concatenate([hi, mid, lo], axis=1)


def kernel(a_hbm, cot_hbm, cvt_hbm, out_ref, abuf, as0, as1, as2, cot_in, cvt_in, cot, cvt, s_mat, b_mat, bs_mat, l8, l4, l2,
           f1_mat, f2_mat, x_buf, h_buf, own_m, own_s, ps_m, ps_s, pr_m, pr_s, rb_m, rb_s, v_acc, v_in, w2, w2_in,
           a_sem, as_sem, c_sem, d_send, d_recv, ds_send, ds_recv, r_send, r_recv, rs_send, rs_recv, v_sem, w_sem):
    y = lax.axis_index('dev2')
    dev = lax.axis_index('dev')
    core = lax.rem(dev, 2)
    x = dev // 2
    partner = (0, y, x * 2 + (1 - core))
    peers = [(0, 1 - y, (1 - x) * 2 + core), (0, 1 - y, x * 2 + core), (0, y, (1 - x) * 2 + core)]
    chip = [2 * (1 - y) + (1 - x), 2 * (1 - y) + x, 2 * y + (1 - x), 2 * y + x]

    def a_copy(n, half, slot):
        return pltpu.make_async_copy(
            a_hbm.at[:, pl.ds(n * QC + 4 * half, 4)], abuf.at[slot, half], a_sem.at[slot, half])

    def all_of(ref, sem):
        return pltpu.make_async_remote_copy(
            src_ref=ref, dst_ref=ref, send_sem=sem, recv_sem=sem, device_id=partner, device_id_type=MESH)

    small = [pltpu.make_async_copy(cot_hbm, cot_in, c_sem.at[0]), pltpu.make_async_copy(cvt_hbm, cvt_in, c_sem.at[1])]
    a_small = (as0, as1, as2)
    small_copy = [[pltpu.make_async_copy(a_hbm.at[:, pl.ds(q + 2 * k, 2)], a_small[m].at[:, pl.ds(2 * k, 2)],
                                         as_sem.at[m, k]) for k in range(nq // 2)]
                  for m, (q, nq) in enumerate(SMALL)]
    for c in small:
        c.start()
    small_copy[0][0].start()

    barrier = pltpu.get_barrier_semaphore()
    for other in [partner] + peers:
        pl.semaphore_signal(barrier, inc=1, device_id=other, device_id_type=MESH)

    cot[...] = jnp.zeros_like(cot)
    cvt[...] = jnp.zeros_like(cvt)
    for c in small:
        c.wait()
    for c in small_copy[1]:
        c.start()
    cot[0:NO, 0:NB] = cot_in[...].astype(F32)
    cvt[0:NV, 0:NB] = cvt_in[...].astype(F32)
    sub = iota((8, L), 0)
    zero = jnp.zeros((8, L), F32)
    for jj in range(8):
        for p in range(8):
            two = [jnp.where(sub == p, cot[j:j + 1, :], zero) for j in (2 * jj, 2 * jj + 1)]
            s_mat[rows8(2 * jj, 2), cols(p)] = jnp.concatenate(two, axis=0).astype(BF16)
    cv = cvt[...].T.astype(BF16)
    first = [(15 * c) // 4 for c in chip]
    first_s = [4 * c + 2 - c // 3 for c in chip]
    lane, row = iota((1, 256), 1), iota((L, 256), 0)
    bs_mat[...] = jnp.zeros_like(bs_mat)

    def full_of(rel, block, j0, steps):
        c = rel + 360 * block
        step = sum((c >= 96 * (j0 + t)).astype(I32) for t in range(1, steps))
        place = jnp.where(row == c - 96 * (j0 + step), 1.0, 0.0).astype(BF16)
        return dot(cv, place), step

    far = -100000
    rel = jnp.where(lane < NC, lane, jnp.where(lane < CH, far, lane - 4))
    for r in range(4):
        full, step = full_of(rel, chip[r], first[r], 4)
        for t in range(4):
            b_mat[r, cols(t), :] = jnp.where(step == t, full, 0.0).astype(BF16)
    rel = jnp.where((lane & (L - 1)) < SP, (lane & (L - 1)) + 252, far)
    for p in range(2):
        r0, r1 = 2 * p, 2 * p + 1
        full, step = full_of(rel, jnp.where(lane < L, chip[r0], chip[r1]), jnp.where(lane < L, first_s[r0], first_s[r1]), 2)
        for t in range(2):
            some = jnp.where(step == t, full, 0.0).astype(BF16)
            for h in range(2):
                bs_mat[p, cols(2 * h + t), cols(h)] = some[:, cols(h)]
    low, high = cot[0:8, :], cot[8:16, :]
    mine = jnp.concatenate([jnp.where(core == 0, low, high), jnp.where(core == 0, high, low)], axis=0)
    kk = iota((L, 256), 1)
    ploc = ((kk >> 4) & 3) * 8 + (kk & 7)
    pick = (iota((L, 256), 0) == ploc + NP * dev) & (ploc < NP)
    l0 = dot(mine.astype(BF16), jnp.where(pick, 1.0, 0.0).astype(BF16)).astype(BF16)
    def build_l(l_mat, sh):
        nq = 1 << sh
        rows = 16 * nq
        e = jnp.where((iota((rows, 16), 0) >> sh) == iota((rows, 16), 1), 1.0, 0.0).astype(BF16)
        row, k2 = iota((rows, 256), 0), iota((rows, 256), 1)
        here = (k2 >> 6) * 2 + ((k2 >> 3) & 1) == (row & (nq - 1))
        l_mat[...] = jnp.where(here, dot(e, l0), 0.0).astype(BF16)

    build_l(l2, 1)
    build_l(l4, 2)
    build_l(l8, 3)

    def step1(tile_of, qp):
        zl = jnp.zeros((NB, L - NB), BF16)
        zs = jnp.zeros((L - NB, L), BF16)

        def tile(p, q):
            t = jnp.concatenate([tile_of(p, q), zl], axis=1)
            return jnp.concatenate([t, zs], axis=0)

        for pg in range(PG):
            ps = range(8 * pg, min(NP, 8 * pg + 8))
            rhs = jnp.concatenate([jnp.concatenate([tile(p, 0), tile(p, 1)], axis=1) for p in ps], axis=0)
            t = dot(s_mat[rows8(0, NO), cols(0, len(ps))], rhs)
            r = rows8(8 * qp + 2 * pg, 2)
            for j in range(NO):
                two = jnp.concatenate([t[rows8(j), cols(k)] for k in range(2)], axis=0)
                x_buf[j, r, :] = two.astype(BF16)

    def stage_h(rows, k):
        p, t = k // 3, k % 3
        if t < 2:
            js, weights = [first[2 * p + t] + j for j in range(4)], b_mat[2 * p + t]
        else:
            js, weights = [first_s[r] + j for r in (2 * p, 2 * p + 1) for j in range(2)], bs_mat[p]
        lhs = jnp.concatenate([x_buf[j, 0:rows, :] for j in js], axis=1)
        h_buf[k, 0:rows, :] = dot(lhs, weights).astype(BF16)

    def stage_w(rows, lhs, p):
        w = [dot(lhs, h_buf[3 * p + t, 0:rows, :]) for t in range(3)]
        return [jnp.concatenate([w[k], w[2][:, cols(k)]], axis=1) for k in range(2)]

    lane8 = iota((8, L), 1)
    spare = lane8 >= SP

    def pack(ref, w):
        col = [[w[rows8(i), cols(c)] for c in range(3)] for i in range(8)]
        for i in range(8):
            for c in range(3 if i else 2):
                v = col[i][c]
                if c == 2 and i <= NS:
                    v = jnp.where(spare, pltpu.roll(col[0][c], SP - PW * (i - 1), 1), v)
                ref[rows8(place_of(i, c)), :] = v

    def d2d(n, r):
        return pltpu.make_async_remote_copy(
            src_ref=ps_m.at[n, r], dst_ref=pr_m.at[n, r], send_sem=d_send, recv_sem=d_recv.at[n % 2, r // 2],
            device_id=partner, device_id_type=MESH)

    def d2d_s(m, r):
        part = pl.ds(0, 24 * SMALL[m][1])
        return pltpu.make_async_remote_copy(
            src_ref=ps_s.at[m, r, part], dst_ref=pr_s.at[m, r, part], send_sem=ds_send,
            recv_sem=ds_recv.at[m, r // 2], device_id=partner, device_id_type=MESH)

    def out_m(n, r, rows):
        return pltpu.make_async_remote_copy(
            src_ref=own_m.at[n, r, pl.ds(0, rows)], dst_ref=rb_m.at[r, n, pl.ds(0, rows)],
            send_sem=r_send, recv_sem=r_recv.at[n // N1], device_id=peers[r], device_id_type=MESH)

    def out_s(m, r):
        part = pl.ds(0, 24 * SMALL[m][1])
        return pltpu.make_async_remote_copy(
            src_ref=own_s.at[m, r, part], dst_ref=rb_s.at[r, m, part], send_sem=rs_send,
            recv_sem=rs_recv, device_id=peers[r], device_id_type=MESH)

    def by_core(f):
        for k in range(2):
            @pl.when(core == k)
            def _(k=k):
                f(ROWS[k])

    def finish_m(n, rs):
        all_of(pr_m.at[n, pl.ds(rs[0], 2)], d_recv.at[n % 2, rs[0] // 2]).wait_recv()
        for r in rs:
            own_m[n, r] = own_m[n, r] + pr_m[n, r]

        def go(rows):
            for r in rs:
                if r < 3:
                    out_m(n, r, rows).start()

        by_core(go)

    def finish_s(m):
        part = rows8(0, 3 * SMALL[m][1])
        for r in range(4):
            if r % 2 == 0:
                all_of(pr_s.at[m, pl.ds(r, 2), pl.ds(0, 24 * SMALL[m][1])], ds_recv.at[m, r // 2]).wait_recv()
            own_s[m, r, part, :] = own_s[m, r, part, :] + pr_s[m, r, part, :]
            if r < 3:
                out_s(m, r).start()

    for m, (l_mat, a_ref) in enumerate(zip((l2, l4, l4), a_small)):
        nq = SMALL[m][1]
        for qp in range(nq // 2):
            small_copy[m][qp].wait()
            step1(lambda p, q: a_ref[p, 2 * qp + q], qp)
        if m == 0:
            for c in small_copy[2]:
                c.start()
            pl.semaphore_wait(barrier, 4)
        else:
            for half in range(2):
                a_copy(m - 1, half, m - 1).start()
            finish_s(m - 1)
        rows = 32 * nq
        for k in range(6):
            stage_h(rows, k)
        for p in range(2):
            pair = (2 * p, 2 * p + 1)
            for r, w in zip(pair, stage_w(rows, l_mat[:, 0:rows], p)):
                for c in range(3):
                    own_s[m, r, rows8(c * nq, nq), :] = w[rows8(0, nq), cols(c)]
                    ps_s[m, r, rows8(c * nq, nq), :] = w[rows8(nq, nq), cols(c)]
            for r in pair:
                d2d_s(m, r).start()

    def body(n, carry):
        slot = lax.rem(n, 2)
        for half in range(2):
            qps = (2 * half, 2 * half + 1)
            a_copy(n, half, slot).wait()
            for qp in qps:
                step1(lambda p, q: abuf[slot, half, p, 2 * (qp % 2) + q], qp)

            @pl.when(n + 2 < NM)
            def _():
                a_copy(n + 2, half, slot).start()

            if half == 0:
                @pl.when(n == 0)
                def _():
                    finish_s(2)

            @pl.when(n > 0)
            def _():
                finish_m(n - 1, qps)

        for k in range(6):
            stage_h(256, k)
        for p in range(2):
            pair = (2 * p, 2 * p + 1)
            for r, w in zip(pair, stage_w(256, l8[...], p)):
                pack(own_m.at[n, r], w[rows8(0, 8)])
                pack(ps_m.at[n, r], w[rows8(8, 8)])
            for r in pair:
                d2d(n, r).start()
        return carry

    lax.fori_loop(0, NM, body, 0)
    finish_m(NM - 1, (0, 1))
    finish_m(NM - 1, (2, 3))

    def w_rows(i, ns):
        def block(n, b):
            near = own_m[n, 3, rows8(b), :] + rb_m[2, n, rows8(b), :]
            far = rb_m[1, n, rows8(b), :] + rb_m[0, n, rows8(b), :]
            return near, far

        both = []
        for n in ns:
            parts_of = [block(n, place_of(i, c)) for c in range(3 if i else 2)]
            if not i:
                s = [jnp.zeros((8, L), F32)] * 2
                for m in range(NS):
                    piece = block(n, place_of(m + 1, 2))
                    here = (lane8 >= PW * m) & (lane8 < min(SP, PW * m + PW))
                    s = [jnp.where(here, pltpu.roll(v, PW * m + PW, 1), o) for v, o in zip(piece, s)]
                parts_of.append(s)
            both.append([jnp.concatenate(list(c), axis=1) for c in zip(*parts_of)])
        return [b[0] for b in both] + [b[1] for b in both]

    def small_rows(i):
        out = []
        for m, (_, nq) in enumerate(SMALL):
            own, ins = [], []
            for c in range(3):
                t = rows8(c * nq + (i * nq) // 8)
                own.append(own_s[m, 3, t, :] + rb_s[2, m, t, :])
                ins.append(rb_s[1, m, t, :] + rb_s[0, m, t, :])
            out += [jnp.concatenate(own, axis=1), jnp.concatenate(ins, axis=1)]
        return out

    base, other_base = NQ * y, NQ * (1 - y)

    late_cv = cvt[...].T.astype(BF16)

    def f_of(want_q):
        sel = jnp.where(iota((L, L), 1) == want_q, 1.0, 0.0).astype(BF16)
        return dot(sel, late_cv)

    kf = iota((L, L), 0)
    h1 = QC * N1
    kt = kf - 2 * h1
    ks, ku = kt >> 4, kt & 7
    kq = jnp.where(ks == 0, SMALL[0][0] + (ku & 1), jnp.where(ks == 1, SMALL[1][0], SMALL[2][0]) + (ku & 3))
    f1_mat[...] = f_of(jnp.where(kt < 0, jnp.where(kf < h1, base + kf, other_base + kf - h1),
                       jnp.where((kt & 8) == 0, base, other_base) + kq))
    f2 = f_of(jnp.where((kf & 8) == 0, base, other_base) + h1 + (kf & 7))
    for i in range(8):
        mine_f = jnp.where((kf >> 4) == i, f2, 0.0).astype(BF16)
        for k in range(3):
            f2_mat[cols(k), cols(i)] = mine_f

    all_of(rb_s.at[:, :, pl.ds(0, 80)], rs_recv).wait_recv()
    by_core(lambda rows: all_of(rb_m.at[:, pl.ds(0, N1), pl.ds(0, rows)], r_recv.at[0]).wait_recv())

    def turned(w):
        return jnp.concatenate([w[:, cols(c)].T for c in range(3)], axis=0)

    for i in range(8):
        w = jnp.concatenate(w_rows(i, range(N1)) + small_rows(i), axis=0)
        here = (kt < 0) | ((ks == 0) & (ku >> 1 == i % 4)) | ((ks > 0) & (ku >> 2 == i % 2))
        f1 = jnp.where(here, f1_mat[...], 0.0).astype(BF16)
        v = dot(parts(turned(w)), jnp.concatenate([f1] * 3, axis=0))
        for h in range(2):
            v_acc[h, i] = v[CH * h:CH * h + CH]

    across = pltpu.make_async_remote_copy(
        src_ref=v_acc.at[1 - core], dst_ref=v_in, send_sem=v_sem.at[0], recv_sem=v_sem.at[1],
        device_id=partner, device_id_type=MESH)
    across.start()

    all_of(ps_s.at[:, :, pl.ds(0, 80)], ds_send).wait_send()
    all_of(own_s.at[:, pl.ds(0, 3), pl.ds(0, 80)], rs_send).wait_send()
    all_of(ps_m, d_send).wait_send()
    by_core(lambda rows: all_of(rb_m.at[:, N1, pl.ds(0, rows)], r_recv.at[1]).wait_recv())

    rows = [v for i in range(7) for v in w_rows(i, range(N1, NM))]
    rows += [jnp.where(core == 0, v, 0.0) for v in w_rows(7, range(N1, NM))]
    w = jnp.concatenate(rows, axis=0)
    for c in range(3):
        w2[c] = w[:, cols(c)]
    last = pltpu.make_async_remote_copy(
        src_ref=w2.at[pl.ds(1 - core, 2)], dst_ref=w2_in, send_sem=w_sem.at[0], recv_sem=w_sem.at[1], device_id=partner, device_id_type=MESH)
    last.start()

    def finish_v(w, acc, who):
        t = jnp.concatenate([v.T for v in w], axis=0)
        t = parts(jnp.where(core == 0, t[0:CH], t[CH - L:2 * CH - L]))
        vs = [dot(t, f2_mat[:, cols(2 * g, 2)]) for g in range(4)]
        for i in range(7):
            out_ref[who * 8 + i] = (acc(i) + vs[i // 2][:, cols(i % 2)])[0:NC, 0:NV]

        @pl.when(who == 0)
        def _():
            out_ref[7] = (acc(7) + vs[3][:, cols(1)])[0:NC, 0:NV]

    finish_v([w2[core], w2[core + 1]], lambda i: v_acc[core, i], core)
    across.wait_recv()
    last.wait_recv()
    finish_v([w2_in[0], w2_in[1]], lambda i: v_in[i], 1 - core)
    across.wait_send()
    last.wait_send()
    by_core(lambda rows: all_of(own_m.at[:, pl.ds(0, 3), pl.ds(0, rows)], r_send).wait_send())


def solution(mesh):
    def local_program(ints_blk, c_occ, c_vir):
        v = pl.pallas_call(
            kernel,
            out_shape=pltpu.VMEM((NO, NC, NV), F32),
            in_specs=[pl.BlockSpec(memory_space=pl.ANY)] * 3,
            out_specs=pl.BlockSpec(memory_space=pltpu.VMEM),
            scratch_shapes=[
                pltpu.VMEM((2, 2, NP, 4, NB, NB), BF16),
                pltpu.VMEM((NP, 2, NB, NB), BF16),
                pltpu.VMEM((NP, 4, NB, NB), BF16),
                pltpu.VMEM((NP, 4, NB, NB), BF16),
                pltpu.VMEM((NO, NB), BF16),
                pltpu.VMEM((NV, NB), BF16),
                pltpu.VMEM((16, L), F32),
                pltpu.VMEM((L, L), F32),
                pltpu.VMEM((L, 1024), BF16),
                pltpu.VMEM((4, 512, 256), BF16),
                pltpu.VMEM((2, 512, 256), BF16),
                pltpu.VMEM((L, 256), BF16),
                pltpu.VMEM((64, 256), BF16),
                pltpu.VMEM((32, 256), BF16),
                pltpu.VMEM((L, L), F32),
                pltpu.VMEM((384, 1024), BF16),
                pltpu.VMEM((NO, 256, L), BF16),
                pltpu.VMEM((6, 256, 256), BF16),
                pltpu.VMEM((NM, 4, RW, L), F32),
                pltpu.VMEM((3, 4, 96, L), F32),
                pltpu.VMEM((NM, 4, RW, L), F32),
                pltpu.VMEM((3, 4, 96, L), F32),
                pltpu.VMEM((NM, 4, RW, L), F32),
                pltpu.VMEM((3, 4, 96, L), F32),
                pltpu.VMEM((3, NM, RW, L), F32),
                pltpu.VMEM((3, 3, 96, L), F32),
                pltpu.VMEM((2, 8, CH, L), F32),
                pltpu.VMEM((8, CH, L), F32),
                pltpu.VMEM((3, L, L), F32),
                pltpu.VMEM((2, L, L), F32),
                pltpu.SemaphoreType.DMA((2, 2)),
                pltpu.SemaphoreType.DMA((3, 2)),
                pltpu.SemaphoreType.DMA((2,)),
                pltpu.SemaphoreType.DMA,
                pltpu.SemaphoreType.DMA((2, 2)),
                pltpu.SemaphoreType.DMA,
                pltpu.SemaphoreType.DMA((3, 2)),
                pltpu.SemaphoreType.DMA,
                pltpu.SemaphoreType.DMA((2,)),
                pltpu.SemaphoreType.DMA,
                pltpu.SemaphoreType.DMA,
                pltpu.SemaphoreType.DMA((2,)),
                pltpu.SemaphoreType.DMA((2,)),
            ],
            compiler_params=pltpu.CompilerParams(
                collective_id=0, has_side_effects=True, vmem_limit_bytes=60 * 1024 * 1024),
            name='four_index',
        )(ints_blk, c_occ.T, c_vir.T)
        return v.transpose(0, 2, 1)

    return jax.shard_map(
        local_program,
        mesh=mesh,
        in_specs=(P(('frag', 'dev'), 'dev2', None, None), P('frag', None), P('frag', None)),
        out_specs=P(None, None, ('frag', 'dev2', 'dev')),
        check_vma=False,
    )
```

```python
import jax
import jax.numpy as jnp
from jax import lax
from jax.experimental import pallas as pl
from jax.experimental.pallas import tpu as pltpu
from jax.sharding import PartitionSpec as P

MESH = pl.DeviceIdType.MESH
F32, BF16, I32 = jnp.float32, jnp.bfloat16, jnp.int32

NP, NQ, NB = 29, 58, 116
NO, NV = 15, 96
QC = 8
NM = 6
SMALL = ((48, 2), (50, 4), (54, 4))
PG = 4
L = 128
LW = 3 * L
SP = 108
PW, NS = L - SP, 6
NC, CH = 180, 184
RW = 184
ROWS = (RW, RW - 24)
N1 = NM - 1


def place_of(i, c):
    return 3 * i - 1 + c if i else c


def cols(k, n=1):
    return slice(L * k, L * (k + n))


def rows8(k, n=1):
    return slice(8 * k, 8 * (k + n))


def iota(shape, dim):
    return lax.broadcasted_iota(I32, shape, dim)


def dot(a, b):
    return jnp.dot(a, b, preferred_element_type=F32)


def parts(w):
    hi = w.astype(BF16)
    rest = w - hi.astype(F32)
    mid = rest.astype(BF16)
    lo = (rest - mid.astype(F32)).astype(BF16)
    return jnp.concatenate([hi, mid, lo], axis=1)


def kernel(a_hbm, cot_hbm, cvt_hbm, out_ref, abuf, as0, as1, as2, cot_in, cvt_in, cot, cvt, s_mat, b_mat, bs_mat, l8, l4, l2,
           f1_mat, f2_mat, x_buf, h_buf, own_m, own_s, ps_m, ps_s, pr_m, pr_s, rb_m, rb_s, v_acc, v_in, w2, w2_in,
           a_sem, as_sem, c_sem, d_send, d_recv, ds_send, ds_recv, r_send, r_recv, rs_send, rs_recv, v_sem, w_sem):
    y = lax.axis_index('dev2')
    dev = lax.axis_index('dev')
    core = lax.rem(dev, 2)
    x = dev // 2
    partner = (0, y, x * 2 + (1 - core))
    peers = [(0, 1 - y, (1 - x) * 2 + core), (0, 1 - y, x * 2 + core), (0, y, (1 - x) * 2 + core)]
    chip = [2 * (1 - y) + (1 - x), 2 * (1 - y) + x, 2 * y + (1 - x), 2 * y + x]

    def a_copy(n, half, slot):
        return pltpu.make_async_copy(
            a_hbm.at[:, pl.ds(n * QC + 4 * half, 4)], abuf.at[slot, half], a_sem.at[slot, half])

    def all_of(ref, sem):
        return pltpu.make_async_remote_copy(
            src_ref=ref, dst_ref=ref, send_sem=sem, recv_sem=sem, device_id=partner, device_id_type=MESH)

    small = [pltpu.make_async_copy(cot_hbm, cot_in, c_sem.at[0]), pltpu.make_async_copy(cvt_hbm, cvt_in, c_sem.at[1])]
    a_small = (as0, as1, as2)
    small_copy = [[pltpu.make_async_copy(a_hbm.at[:, pl.ds(q + 2 * k, 2)], a_small[m].at[:, pl.ds(2 * k, 2)],
                                         as_sem.at[max(2 * m - 1, 0) + k]) for k in range(nq // 2)]
                  for m, (q, nq) in enumerate(SMALL)]
    for c in small:
        c.start()
    small_copy[0][0].start()

    barrier = pltpu.get_barrier_semaphore()
    for other in [partner] + peers:
        pl.semaphore_signal(barrier, inc=1, device_id=other, device_id_type=MESH)

    cot[...] = jnp.zeros_like(cot)
    cvt[...] = jnp.zeros_like(cvt)
    for c in small:
        c.wait()
    for c in small_copy[1]:
        c.start()
    cot[0:NO, 0:NB] = cot_in[...].astype(F32)
    cvt[0:NV, 0:NB] = cvt_in[...].astype(F32)
    sub = iota((8, L), 0)
    zero = jnp.zeros((8, L), F32)
    for jj in range(8):
        for p in range(8):
            two = [jnp.where(sub == p, cot[j:j + 1, :], zero) for j in (2 * jj, 2 * jj + 1)]
            s_mat[rows8(2 * jj, 2), cols(p)] = jnp.concatenate(two, axis=0).astype(BF16)
    cv = cvt[...].T.astype(BF16)
    first = [(15 * c) // 4 for c in chip]
    first_s = [4 * c + 2 - c // 3 for c in chip]
    lane, row = iota((1, 256), 1), iota((L, 256), 0)
    bs_mat[...] = jnp.zeros_like(bs_mat)

    def full_of(rel, block, j0, steps):
        c = rel + 360 * block
        step = sum((c >= 96 * (j0 + t)).astype(I32) for t in range(1, steps))
        place = jnp.where(row == c - 96 * (j0 + step), 1.0, 0.0).astype(BF16)
        return dot(cv, place), step

    far = -100000
    rel = jnp.where(lane < NC, lane, jnp.where(lane < CH, far, lane - 4))
    for r in range(4):
        full, step = full_of(rel, chip[r], first[r], 4)
        for t in range(4):
            b_mat[r, cols(t), :] = jnp.where(step == t, full, 0.0).astype(BF16)
    rel = jnp.where((lane & (L - 1)) < SP, (lane & (L - 1)) + 252, far)
    for p in range(2):
        r0, r1 = 2 * p, 2 * p + 1
        full, step = full_of(rel, jnp.where(lane < L, chip[r0], chip[r1]), jnp.where(lane < L, first_s[r0], first_s[r1]), 2)
        for t in range(2):
            some = jnp.where(step == t, full, 0.0).astype(BF16)
            for h in range(2):
                bs_mat[p, cols(2 * h + t), cols(h)] = some[:, cols(h)]
    low, high = cot[0:8, :], cot[8:16, :]
    mine = jnp.concatenate([jnp.where(core == 0, low, high), jnp.where(core == 0, high, low)], axis=0)
    kk = iota((L, 256), 1)
    ploc = ((kk >> 4) & 3) * 8 + (kk & 7)
    pick = (iota((L, 256), 0) == ploc + NP * dev) & (ploc < NP)
    l0 = dot(mine.astype(BF16), jnp.where(pick, 1.0, 0.0).astype(BF16)).astype(BF16)
    def build_l(l_mat, sh):
        nq = 1 << sh
        rows = 16 * nq
        e = jnp.where((iota((rows, 16), 0) >> sh) == iota((rows, 16), 1), 1.0, 0.0).astype(BF16)
        row, k2 = iota((rows, 256), 0), iota((rows, 256), 1)
        here = (k2 >> 6) * 2 + ((k2 >> 3) & 1) == (row & (nq - 1))
        l_mat[...] = jnp.where(here, dot(e, l0), 0.0).astype(BF16)

    build_l(l2, 1)
    build_l(l4, 2)
    build_l(l8, 3)

    def step1(tile_of, qp):
        zl = jnp.zeros((NB, L - NB), BF16)
        zs = jnp.zeros((L - NB, L), BF16)

        def tile(p, q):
            t = jnp.concatenate([tile_of(p, q), zl], axis=1)
            return jnp.concatenate([t, zs], axis=0)

        for pg in range(PG):
            ps = range(8 * pg, min(NP, 8 * pg + 8))
            rhs = jnp.concatenate([jnp.concatenate([tile(p, 0), tile(p, 1)], axis=1) for p in ps], axis=0)
            t = dot(s_mat[rows8(0, NO), cols(0, len(ps))], rhs)
            r = rows8(8 * qp + 2 * pg, 2)
            for j in range(NO):
                two = jnp.concatenate([t[rows8(j), cols(k)] for k in range(2)], axis=0)
                x_buf[j, r, :] = two.astype(BF16)

    def stage_h(rows, k):
        p, t = k // 3, k % 3
        if t < 2:
            js, weights = [first[2 * p + t] + j for j in range(4)], b_mat[2 * p + t]
        else:
            js, weights = [first_s[r] + j for r in (2 * p, 2 * p + 1) for j in range(2)], bs_mat[p]
        lhs = jnp.concatenate([x_buf[j, 0:rows, :] for j in js], axis=1)
        h_buf[k, 0:rows, :] = dot(lhs, weights).astype(BF16)

    def stage_w(rows, lhs, p):
        w = [dot(lhs, h_buf[3 * p + t, 0:rows, :]) for t in range(3)]
        return [jnp.concatenate([w[k], w[2][:, cols(k)]], axis=1) for k in range(2)]

    lane8 = iota((8, L), 1)
    spare = lane8 >= SP

    def pack(ref, w):
        col = [[w[rows8(i), cols(c)] for c in range(3)] for i in range(8)]
        for i in range(8):
            for c in range(3 if i else 2):
                v = col[i][c]
                if c == 2 and i <= NS:
                    v = jnp.where(spare, pltpu.roll(col[0][c], SP - PW * (i - 1), 1), v)
                ref[rows8(place_of(i, c)), :] = v

    def d2d(n, r):
        return pltpu.make_async_remote_copy(
            src_ref=ps_m.at[n, r], dst_ref=pr_m.at[n, r], send_sem=d_send, recv_sem=d_recv.at[n % 2, r // 2],
            device_id=partner, device_id_type=MESH)

    def d2d_s(m, r):
        part = pl.ds(0, 24 * SMALL[m][1])
        return pltpu.make_async_remote_copy(
            src_ref=ps_s.at[m, r, part], dst_ref=pr_s.at[m, r, part], send_sem=ds_send,
            recv_sem=ds_recv.at[m % 2, r // 2], device_id=partner, device_id_type=MESH)

    def out_m(n, r, rows):
        return pltpu.make_async_remote_copy(
            src_ref=own_m.at[n, r, pl.ds(0, rows)], dst_ref=rb_m.at[r, n, pl.ds(0, rows)],
            send_sem=r_send, recv_sem=r_recv.at[n // N1], device_id=peers[r], device_id_type=MESH)

    def out_s(m, r):
        part = pl.ds(0, 24 * SMALL[m][1])
        return pltpu.make_async_remote_copy(
            src_ref=own_s.at[m, r, part], dst_ref=rb_s.at[r, m, part], send_sem=rs_send,
            recv_sem=rs_recv, device_id=peers[r], device_id_type=MESH)

    def by_core(f):
        for k in range(2):
            @pl.when(core == k)
            def _(k=k):
                f(ROWS[k])

    def finish_m(n, rs):
        all_of(pr_m.at[n, pl.ds(rs[0], 2)], d_recv.at[n % 2, rs[0] // 2]).wait_recv()
        for r in rs:
            own_m[n, r] = own_m[n, r] + pr_m[n, r]

        def go(rows):
            for r in rs:
                if r < 3:
                    out_m(n, r, rows).start()

        by_core(go)

    def finish_s(m):
        part = rows8(0, 3 * SMALL[m][1])
        for r in range(4):
            if r % 2 == 0:
                all_of(pr_s.at[m, pl.ds(r, 2), pl.ds(0, 24 * SMALL[m][1])], ds_recv.at[m % 2, r // 2]).wait_recv()
            own_s[m, r, part, :] = own_s[m, r, part, :] + pr_s[m, r, part, :]
            if r < 3:
                out_s(m, r).start()

    for m, (l_mat, a_ref) in enumerate(zip((l2, l4, l4), a_small)):
        nq = SMALL[m][1]
        for qp in range(nq // 2):
            small_copy[m][qp].wait()
            step1(lambda p, q: a_ref[p, 2 * qp + q], qp)
        if m == 0:
            for c in small_copy[2]:
                c.start()
            pl.semaphore_wait(barrier, 4)
        else:
            for half in range(2):
                a_copy(m - 1, half, m - 1).start()
            finish_s(m - 1)
        rows = 32 * nq
        for k in range(6):
            stage_h(rows, k)
        for p in range(2):
            pair = (2 * p, 2 * p + 1)
            for r, w in zip(pair, stage_w(rows, l_mat[:, 0:rows], p)):
                for c in range(3):
                    own_s[m, r, rows8(c * nq, nq), :] = w[rows8(0, nq), cols(c)]
                    ps_s[m, r, rows8(c * nq, nq), :] = w[rows8(nq, nq), cols(c)]
            for r in pair:
                d2d_s(m, r).start()

    def body(n, carry):
        slot = lax.rem(n, 2)
        for half in range(2):
            qps = (2 * half, 2 * half + 1)
            a_copy(n, half, slot).wait()
            for qp in qps:
                step1(lambda p, q: abuf[slot, half, p, 2 * (qp % 2) + q], qp)

            @pl.when(n + 2 < NM)
            def _():
                a_copy(n + 2, half, slot).start()

            if half == 0:
                @pl.when(n == 0)
                def _():
                    finish_s(2)

            @pl.when(n > 0)
            def _():
                finish_m(n - 1, qps)

        for k in range(6):
            stage_h(256, k)
        for p in range(2):
            pair = (2 * p, 2 * p + 1)
            for r, w in zip(pair, stage_w(256, l8[...], p)):
                pack(own_m.at[n, r], w[rows8(0, 8)])
                pack(ps_m.at[n, r], w[rows8(8, 8)])
            for r in pair:
                d2d(n, r).start()
        return carry

    lax.fori_loop(0, NM, body, 0)
    finish_m(NM - 1, (0, 1))
    finish_m(NM - 1, (2, 3))

    def w_rows(i, ns):
        def block(n, b):
            near = own_m[n, 3, rows8(b), :] + rb_m[2, n, rows8(b), :]
            far = rb_m[1, n, rows8(b), :] + rb_m[0, n, rows8(b), :]
            return near, far

        both = []
        for n in ns:
            parts_of = [block(n, place_of(i, c)) for c in range(3 if i else 2)]
            if not i:
                s = [jnp.zeros((8, L), F32)] * 2
                for m in range(NS):
                    piece = block(n, place_of(m + 1, 2))
                    here = (lane8 >= PW * m) & (lane8 < min(SP, PW * m + PW))
                    s = [jnp.where(here, pltpu.roll(v, PW * m + PW, 1), o) for v, o in zip(piece, s)]
                parts_of.append(s)
            both.append([jnp.concatenate(list(c), axis=1) for c in zip(*parts_of)])
        return [b[0] for b in both] + [b[1] for b in both]

    def small_rows(i):
        out = []
        for m, (_, nq) in enumerate(SMALL):
            own, ins = [], []
            for c in range(3):
                t = rows8(c * nq + (i * nq) // 8)
                own.append(own_s[m, 3, t, :] + rb_s[2, m, t, :])
                ins.append(rb_s[1, m, t, :] + rb_s[0, m, t, :])
            out += [jnp.concatenate(own, axis=1), jnp.concatenate(ins, axis=1)]
        return out

    base, other_base = NQ * y, NQ * (1 - y)

    late_cv = cvt[...].T.astype(BF16)

    def f_of(want_q):
        sel = jnp.where(iota((L, L), 1) == want_q, 1.0, 0.0).astype(BF16)
        return dot(sel, late_cv)

    kf = iota((L, L), 0)
    h1 = QC * N1
    kt = kf - 2 * h1
    ks, ku = kt >> 4, kt & 7
    kq = jnp.where(ks == 0, SMALL[0][0] + (ku & 1), jnp.where(ks == 1, SMALL[1][0], SMALL[2][0]) + (ku & 3))
    f1_mat[...] = f_of(jnp.where(kt < 0, jnp.where(kf < h1, base + kf, other_base + kf - h1),
                       jnp.where((kt & 8) == 0, base, other_base) + kq))
    f2 = f_of(jnp.where((kf & 8) == 0, base, other_base) + h1 + (kf & 7))
    for i in range(8):
        mine_f = jnp.where((kf >> 4) == i, f2, 0.0).astype(BF16)
        for k in range(3):
            f2_mat[cols(k), cols(i)] = mine_f

    all_of(rb_s.at[:, :, pl.ds(0, 80)], rs_recv).wait_recv()
    by_core(lambda rows: all_of(rb_m.at[:, pl.ds(0, N1), pl.ds(0, rows)], r_recv.at[0]).wait_recv())

    def turned(w):
        return jnp.concatenate([w[:, cols(c)].T for c in range(3)], axis=0)

    for i in range(8):
        w = jnp.concatenate(w_rows(i, range(N1)) + small_rows(i), axis=0)
        here = (kt < 0) | ((ks == 0) & (ku >> 1 == i % 4)) | ((ks > 0) & (ku >> 2 == i % 2))
        f1 = jnp.where(here, f1_mat[...], 0.0).astype(BF16)
        v = dot(parts(turned(w)), jnp.concatenate([f1] * 3, axis=0))
        for h in range(2):
            v_acc[h, i] = v[CH * h:CH * h + CH]

    across = pltpu.make_async_remote_copy(
        src_ref=v_acc.at[1 - core], dst_ref=v_in, send_sem=v_sem.at[0], recv_sem=v_sem.at[1],
        device_id=partner, device_id_type=MESH)
    across.start()

    all_of(ps_s.at[:, :, pl.ds(0, 80)], ds_send).wait_send()
    all_of(own_s.at[:, pl.ds(0, 3), pl.ds(0, 80)], rs_send).wait_send()
    all_of(ps_m, d_send).wait_send()
    by_core(lambda rows: all_of(rb_m.at[:, N1, pl.ds(0, rows)], r_recv.at[1]).wait_recv())

    rows = [v for i in range(7) for v in w_rows(i, range(N1, NM))]
    rows += [jnp.where(core == 0, v, 0.0) for v in w_rows(7, range(N1, NM))]
    w = jnp.concatenate(rows, axis=0)
    for c in range(3):
        w2[c] = w[:, cols(c)]
    last = pltpu.make_async_remote_copy(
        src_ref=w2.at[pl.ds(1 - core, 2)], dst_ref=w2_in, send_sem=w_sem.at[0], recv_sem=w_sem.at[1], device_id=partner, device_id_type=MESH)
    last.start()

    def finish_v(w, acc, who):
        t = jnp.concatenate([v.T for v in w], axis=0)
        t = parts(jnp.where(core == 0, t[0:CH], t[CH - L:2 * CH - L]))
        vs = [dot(t, f2_mat[:, cols(2 * g, 2)]) for g in range(4)]
        for i in range(7):
            out_ref[who * 8 + i] = (acc(i) + vs[i // 2][:, cols(i % 2)])[0:NC, 0:NV]

        @pl.when(who == 0)
        def _():
            out_ref[7] = (acc(7) + vs[3][:, cols(1)])[0:NC, 0:NV]

    finish_v([w2[core], w2[core + 1]], lambda i: v_acc[core, i], core)
    across.wait_recv()
    last.wait_recv()
    finish_v([w2_in[0], w2_in[1]], lambda i: v_in[i], 1 - core)
    across.wait_send()
    last.wait_send()
    by_core(lambda rows: all_of(own_m.at[:, pl.ds(0, 3), pl.ds(0, rows)], r_send).wait_send())


def solution(mesh):
    def local_program(ints_blk, c_occ, c_vir):
        v = pl.pallas_call(
            kernel,
            out_shape=pltpu.VMEM((NO, NC, NV), F32),
            in_specs=[pl.BlockSpec(memory_space=pl.ANY)] * 3,
            out_specs=pl.BlockSpec(memory_space=pltpu.VMEM),
            scratch_shapes=[
                pltpu.VMEM((2, 2, NP, 4, NB, NB), BF16),
                pltpu.VMEM((NP, 2, NB, NB), BF16),
                pltpu.VMEM((NP, 4, NB, NB), BF16),
                pltpu.VMEM((NP, 4, NB, NB), BF16),
                pltpu.VMEM((NO, NB), BF16),
                pltpu.VMEM((NV, NB), BF16),
                pltpu.VMEM((16, L), F32),
                pltpu.VMEM((L, L), F32),
                pltpu.VMEM((L, 1024), BF16),
                pltpu.VMEM((4, 512, 256), BF16),
                pltpu.VMEM((2, 512, 256), BF16),
                pltpu.VMEM((L, 256), BF16),
                pltpu.VMEM((64, 256), BF16),
                pltpu.VMEM((32, 256), BF16),
                pltpu.VMEM((L, L), F32),
                pltpu.VMEM((384, 1024), BF16),
                pltpu.VMEM((NO, 256, L), BF16),
                pltpu.VMEM((6, 256, 256), BF16),
                pltpu.VMEM((NM, 4, RW, L), F32),
                pltpu.VMEM((3, 4, 96, L), F32),
                pltpu.VMEM((NM, 4, RW, L), F32),
                pltpu.VMEM((3, 4, 96, L), F32),
                pltpu.VMEM((NM, 4, RW, L), F32),
                pltpu.VMEM((3, 4, 96, L), F32),
                pltpu.VMEM((3, NM, RW, L), F32),
                pltpu.VMEM((3, 3, 96, L), F32),
                pltpu.VMEM((2, 8, CH, L), F32),
                pltpu.VMEM((8, CH, L), F32),
                pltpu.VMEM((3, L, L), F32),
                pltpu.VMEM((2, L, L), F32),
                pltpu.SemaphoreType.DMA((2, 2)),
                pltpu.SemaphoreType.DMA((5,)),
                pltpu.SemaphoreType.DMA((2,)),
                pltpu.SemaphoreType.DMA,
                pltpu.SemaphoreType.DMA((2, 2)),
                pltpu.SemaphoreType.DMA,
                pltpu.SemaphoreType.DMA((2, 2)),
                pltpu.SemaphoreType.DMA,
                pltpu.SemaphoreType.DMA((2,)),
                pltpu.SemaphoreType.DMA,
                pltpu.SemaphoreType.DMA,
                pltpu.SemaphoreType.DMA((2,)),
                pltpu.SemaphoreType.DMA((2,)),
            ],
            compiler_params=pltpu.CompilerParams(
                collective_id=0, has_side_effects=True, vmem_limit_bytes=60 * 1024 * 1024),
            name='four_index',
        )(ints_blk, c_occ.T, c_vir.T)
        return v.transpose(0, 2, 1)

    return jax.shard_map(
        local_program,
        mesh=mesh,
        in_specs=(P(('frag', 'dev'), 'dev2', None, None), P('frag', None), P('frag', None)),
        out_specs=P(None, None, ('frag', 'dev2', 'dev')),
        check_vma=False,
    )
```
